32 devices in a mesh: fsdp: 8 (over z, y), dp: 4 (over x, core).
Axes of the slice: x: 2, y: 2, z: 4, core: 2. Of those that a mesh axis runs over, the one named last changes fastest.
Arguments:
- tokens: bfloat16 [32, 128, 3584], P(('fsdp', 'dp')), may hold values from -6 to 6
- lengths: int32 [32], P(('fsdp', 'dp')), may hold values from 32 to 128
- partner: int32 [32], replicated, may hold values from 0 to 31, as said below
- pair_weight: float32 [32], P(('fsdp', 'dp')), may hold values from 0.25 to 27
- norm_gain: float32 [3584], replicated, may hold values from 0.5 to 1.5
- qkv_weight: bfloat16 [3584, 4608], P('fsdp'), may hold values from -0.09375 to 0.09375
- qkv_bias: float32 [4608], replicated, may hold values from -40 to 40
- out_weight: bfloat16 [3584, 3584], P(None, 'fsdp'), may hold values from -0.09375 to 0.09375
- final_gain: float32 [3584], replicated, may hold values from 0.5 to 1.5
- value_head: float32 [3584], replicated, may hold values from -0.09375 to 0.09375
Outputs:
- hidden: bfloat16 [32, 128, 3584], P(('fsdp', 'dp'))
- margins: float32 [32], P(('fsdp', 'dp'))
- loss: float32 [], replicated
The draws below stay inside these ranges and needn't reach their ends.
Inputs may be any that keep to these rules, and one draw needn't show every extreme that they name: partner[partner[i]] = i and partner[i] != i.
All inputs are finite; a program needn't handle non-finite values.
Results may differ from the reference program's by a relative error of at most 0.013.
The reference program's roundings to bfloat16 on the way count: a program that leaves them out, or rounds other values in their place, can miss the bound.
Values may be sent and summed in bfloat16 or wider, within the bound.
A program may use at most 128 MiB of HBM per device.

```python
import jax
import jax.numpy as jnp
from jax import lax

D = 3584
QUERY_HEADS = 28
KEY_VALUE_HEADS = 4
HEAD_SIZE = 128
SEQUENCE_TOKENS = 128
QUERY_FEATURES = 3584
KEY_FEATURES = 512
QKV = 4608
SEQS = 32


def draw_partner(key, part):
    half = SEQS // 2
    anchor = jax.random.randint(jax.random.fold_in(key, 31), (), 0, half - 2).astype(jnp.int32)
    ranks = jax.random.permutation(jax.random.fold_in(key, 32), SEQS).astype(jnp.int32)
    index = jnp.arange(SEQS, dtype=jnp.int32)
    far_end = anchor + half
    near_one = anchor + 1
    near_two = anchor + 2
    used = (index == anchor) | (index == far_end) | (index == near_one) | (index == near_two)
    sort_key = jnp.where(used, SEQS + ranks, ranks)
    order = jnp.argsort(sort_key, stable=True).astype(jnp.int32)
    rest = order[:SEQS - 4]
    first = rest[0::2]
    second = rest[1::2]
    result = jnp.zeros((SEQS,), jnp.int32)
    result = result.at[first].set(second)
    result = result.at[second].set(first)
    result = result.at[anchor].set(far_end)
    result = result.at[far_end].set(anchor)
    result = result.at[near_one].set(near_two)
    result = result.at[near_two].set(near_one)
    return result


def draw_pair_weight(key, part):
    position = jnp.arange(SEQS, dtype=jnp.float32) / jnp.float32(max(SEQS - 1, 1))
    rising = jnp.exp(position * jnp.log(jnp.float32(9.0)))
    rough = jax.random.uniform(jax.random.fold_in(key, 22), (SEQS,), jnp.float32, 0.5, 1.5)
    return jnp.clip(rising * rough, 0.25, 27.0).astype(jnp.float32)


def draw_qkv_bias(key, part):
    key_three = jax.random.fold_in(key, 13)
    result = 0.5 * jax.random.normal(key_three, (QKV,), jnp.float32)
    return jnp.clip(result, -40.0, 40.0).astype(jnp.float32)


def plant(entries, stream_key, smallest, top_value):
    place = [jax.random.randint(jax.random.fold_in(stream_key, axis), (), 0, length) for axis, length in enumerate(entries.shape)]
    main_axis = entries.shape.index(max(entries.shape))
    beside = place[:main_axis] + [(place[main_axis] + 1) % entries.shape[main_axis]] + place[main_axis + 1:]
    return entries.at[tuple(place)].set(smallest).at[tuple(beside)].set(top_value)


def level_of(rng, dims, shards, low, high):
    def one(dim, parts):
        steps = jax.random.uniform(jax.random.fold_in(jax.random.fold_in(rng, 6), dim), (parts,), jnp.float32, low / len(shards), high / len(shards))
        return jnp.repeat(jnp.exp(steps), dims[dim] // parts).reshape((-1,) + (1,) * (len(dims) - dim - 1))

    level = one(*shards[0])
    for cut in shards[1:]:
        level = level * one(*cut)
    return level


def bell_draw(key, dims, scale, limit, split=(), kind=jnp.bfloat16):
    values = jax.random.normal(key, dims, jnp.float32) * scale
    if len(split) > 0:
        values = level_of(key, dims, split, -0.22, 0.18) * values
    return jnp.clip(values, min=-limit, max=limit).astype(kind)


def setup_inputs(seed: int = 0) -> dict:
    streams_of = jax.random.split(jax.random.key(seed), 11)
    return {
        "tokens": bell_draw(streams_of[0], (SEQS, SEQUENCE_TOKENS, D), 1.0, 6.0, ((0, 32),)),
        "lengths": plant(jax.random.randint(streams_of[1], (SEQS,), SEQUENCE_TOKENS // 4, SEQUENCE_TOKENS + 1), jax.random.fold_in(streams_of[1], 1), SEQUENCE_TOKENS // 4, SEQUENCE_TOKENS).astype(jnp.int32),
        "partner": draw_partner(jax.random.fold_in(streams_of[10], 71), 0),
        "pair_weight": draw_pair_weight(jax.random.fold_in(streams_of[10], 71), 0),
        "norm_gain": jnp.clip(1.0 + 0.1 * jax.random.normal(streams_of[4], (D,), jnp.float32), 0.5, 1.5),
        "qkv_weight": bell_draw(streams_of[5], (D, QKV), D ** -0.5, 0.09375, ((0, 8),)),
        "qkv_bias": draw_qkv_bias(jax.random.fold_in(streams_of[10], 71), 0),
        "out_weight": bell_draw(streams_of[7], (QUERY_FEATURES, D), QUERY_FEATURES ** -0.5, 0.09375, ((1, 8),)),
        "final_gain": jnp.clip(1.0 + 0.1 * jax.random.normal(streams_of[8], (D,), jnp.float32), 0.5, 1.5),
        "value_head": bell_draw(streams_of[9], (D,), D ** -0.5, 0.09375, (), jnp.float32),
    }


def rms_scale(value_rows, gain):
    return value_rows * lax.rsqrt(lax.optimization_barrier(jnp.mean(value_rows * value_rows, axis=-1, keepdims=True)) + 1e-06) * gain

def apply_rotary(heads):
    half = HEAD_SIZE // 2
    positions = jnp.arange(SEQUENCE_TOKENS, dtype=jnp.float32)
    freqs = jnp.exp(-(2.0 * jnp.arange(half, dtype=jnp.float32) / HEAD_SIZE) * jnp.log(jnp.float32(1000000.0)))
    angles = positions[:, None] * freqs[None, :]
    cosine = jnp.cos(angles)
    sine = jnp.sin(angles)
    first = heads[..., :half]
    second = heads[..., half:]
    return jnp.concatenate([first * cosine - second * sine, second * cosine + first * sine], axis=-1)

def one_sequence(sequence, length, norm_gain, qkv_weight, qkv_bias, out_weight, final_gain, value_head):
    normed = rms_scale(sequence.astype(jnp.float32), norm_gain).astype(jnp.bfloat16)
    query_key_value = jnp.dot(normed, qkv_weight, preferred_element_type=jnp.float32) + qkv_bias
    query_rows = query_key_value[:, :QUERY_FEATURES].reshape(SEQUENCE_TOKENS, QUERY_HEADS, HEAD_SIZE).transpose(1, 0, 2)
    key_rows = query_key_value[:, QUERY_FEATURES:QUERY_FEATURES + KEY_FEATURES].reshape(SEQUENCE_TOKENS, KEY_VALUE_HEADS, HEAD_SIZE).transpose(1, 0, 2)
    value_rows = query_key_value[:, QUERY_FEATURES + KEY_FEATURES:].reshape(SEQUENCE_TOKENS, KEY_VALUE_HEADS, HEAD_SIZE).transpose(1, 0, 2).astype(jnp.bfloat16)
    query_rows = apply_rotary(query_rows).astype(jnp.bfloat16).reshape(KEY_VALUE_HEADS, QUERY_HEADS // KEY_VALUE_HEADS, SEQUENCE_TOKENS, HEAD_SIZE)
    key_rows = apply_rotary(key_rows).astype(jnp.bfloat16)
    scores = jnp.einsum('gqtd,gsd->gqts', query_rows.astype(jnp.float32), key_rows.astype(jnp.float32)) / jnp.sqrt(jnp.float32(HEAD_SIZE))
    rows = jnp.arange(SEQUENCE_TOKENS, dtype=jnp.int32)
    allowed = (rows[None, :] <= rows[:, None]) & (rows[None, :] < length)
    scores = jnp.where(allowed, scores, jnp.float32(-1e+30))
    top = lax.optimization_barrier(jnp.max(scores, axis=-1, keepdims=True))
    expd = jnp.exp(scores - top)
    probs = (expd / lax.optimization_barrier(jnp.sum(expd, axis=-1, keepdims=True))).astype(jnp.bfloat16)
    attn = jnp.einsum('gqts,gsd->gqtd', probs.astype(jnp.float32), value_rows.astype(jnp.float32))
    attn = attn.reshape(QUERY_HEADS, SEQUENCE_TOKENS, HEAD_SIZE).transpose(1, 0, 2).reshape(SEQUENCE_TOKENS, QUERY_FEATURES).astype(jnp.bfloat16)
    hidden = (sequence.astype(jnp.float32) + jnp.dot(attn, out_weight, preferred_element_type=jnp.float32)).astype(jnp.bfloat16)
    last = lax.dynamic_slice_in_dim(hidden, (length - 1).astype(jnp.int32), 1, 0)[0].astype(jnp.float32)
    score = jnp.sum(rms_scale(last, final_gain) * value_head)
    return (hidden, score)

def reference(tokens, lengths, partner, pair_weight, norm_gain, qkv_weight, qkv_bias, out_weight, final_gain, value_head):

    def step(item):
        return one_sequence(item[0], item[1], norm_gain, qkv_weight, qkv_bias, out_weight, final_gain, value_head)
    hidden, scores = lax.map(step, (tokens, lengths))
    other = scores[partner]
    index = jnp.arange(SEQS, dtype=jnp.int32)
    margins = jnp.where(index < partner, scores - other, other - scores)
    loss = jnp.sum(pair_weight * jax.nn.softplus(-margins)) / SEQS
    return (hidden, margins, loss)
```

```python
import functools

import jax
import jax.numpy as jnp
import numpy as np
from jax import lax
from jax.experimental import pallas as pl
from jax.experimental.pallas import tpu as pltpu
from jax.sharding import PartitionSpec as P

QUERY_HEADS = 28
KEY_VALUE_HEADS = 4
HEAD_SIZE = 128
QUERY_FEATURES = 3584
KEY_FEATURES = 512


def rms_scale(value_rows, gain):
    return (
        value_rows
        * lax.rsqrt(jnp.mean(value_rows * value_rows, axis=-1, keepdims=True) + 1e-06)
        * gain
    )


def apply_rotary(heads, length_rows):
    half = HEAD_SIZE // 2
    positions = jnp.arange(length_rows, dtype=jnp.float32)
    freqs = jnp.exp(
        -(2.0 * jnp.arange(half, dtype=jnp.float32) / HEAD_SIZE) * jnp.log(jnp.float32(1000000.0))
    )
    angles = positions[:, None] * freqs[None, :]
    cosine = jnp.cos(angles)
    sine = jnp.sin(angles)
    first = heads[..., :half]
    second = heads[..., half:]
    return jnp.concatenate(
        [first * cosine - second * sine, second * cosine + first * sine], axis=-1
    )


def attend(query_key_value, group_lengths, query_heads, key_value_heads):
    seq_count, length_rows, _ = query_key_value.shape
    query_width = query_heads * HEAD_SIZE
    key_width = key_value_heads * HEAD_SIZE
    query_rows = (
        query_key_value[..., :query_width]
        .reshape(seq_count, length_rows, query_heads, HEAD_SIZE)
        .transpose(0, 2, 1, 3)
    )
    key_rows = (
        query_key_value[..., query_width : query_width + key_width]
        .reshape(seq_count, length_rows, key_value_heads, HEAD_SIZE)
        .transpose(0, 2, 1, 3)
    )
    value_rows = (
        query_key_value[..., query_width + key_width :]
        .reshape(seq_count, length_rows, key_value_heads, HEAD_SIZE)
        .transpose(0, 2, 1, 3)
        .astype(jnp.bfloat16)
    )
    query_rows = (
        apply_rotary(query_rows, length_rows)
        .astype(jnp.bfloat16)
        .reshape(seq_count, key_value_heads, query_heads // key_value_heads, length_rows, HEAD_SIZE)
    )
    key_rows = apply_rotary(key_rows, length_rows).astype(jnp.bfloat16)
    scores = jnp.einsum(
        "bgqtd,bgsd->bgqts", query_rows, key_rows, preferred_element_type=jnp.float32
    ) / jnp.sqrt(jnp.float32(HEAD_SIZE))
    places = jnp.arange(length_rows, dtype=jnp.int32)
    causal = places[None, :] <= places[:, None]
    usable = places[None, :] < group_lengths[:, None]
    allowed = causal[None, :, :] & usable[:, None, :]
    scores = jnp.where(allowed[:, None, None, :, :], scores, jnp.float32(-1e30))
    highest = jnp.max(scores, axis=-1, keepdims=True)
    expd = jnp.exp(scores - highest)
    probs = (expd / jnp.sum(expd, axis=-1, keepdims=True)).astype(jnp.bfloat16)
    mixed = jnp.einsum("bgqts,bgsd->bgqtd", probs, value_rows, preferred_element_type=jnp.float32)
    mixed = mixed.reshape(seq_count, query_heads, length_rows, HEAD_SIZE).transpose(0, 2, 1, 3)
    return mixed.reshape(seq_count * length_rows, query_width).astype(jnp.bfloat16)


UP, DOWN, PARTNER = 0, 1, 2


def rotary_tables(length_rows):
    half = HEAD_SIZE // 2
    freqs = 1000000.0 ** (-2.0 * np.arange(half) / HEAD_SIZE)
    angles = np.arange(length_rows)[:, None] * freqs[None, :]
    cosine, sine = np.cos(angles), np.sin(angles)
    return (
        np.concatenate([cosine, cosine], axis=1).astype(np.float32),
        np.concatenate([-sine, sine], axis=1).astype(np.float32),
    )


def layer_kernel(
    shards,
    groups,
    tokens,
    qkv_weight,
    out_weight,
    length,
    pair_weight,
    partner,
    norm_gain_flat,
    final_gain_flat,
    value_head_flat,
    qkv_bias_flat,
    cosine,
    sine,
    hidden_out,
    margin_out,
    loss_out,
    qkv_full,
    out_full,
    cross_qkv,
    cross_out,
    tok_own,
    len_tile,
    len_all,
    normed,
    qkv_rows,
    attn,
    own,
    part_out,
    part_in,
    hidden,
    stats,
    score_tile,
    score_all,
    partner_rows,
    norm_gain,
    final_gain,
    value_head,
    qkv_bias,
    local_sem,
    recv_sem,
    send_sem,
    cross_send,
    tok_send,
    tok_recv,
    len_send,
    len_recv,
    part_send,
    part_recv,
    score_send,
    score_recv,
    hidden_sem,
):
    line = shards // 2
    f = lax.axis_index("fsdp")
    g = lax.axis_index("dp")
    z = f // 2
    y = f % 2
    x = g // 2
    core = g % 2
    seq_rows = tokens.shape[0]
    width = tokens.shape[1]
    depth = qkv_weight.shape[0]
    out_cols = out_weight.shape[0]
    query_cols = QUERY_FEATURES // groups
    key_cols = KEY_FEATURES // groups
    heads = query_cols // HEAD_SIZE
    quarter = depth // 4
    out_quarter = out_cols // 4
    has_up = z < line - 1
    has_down = z > 0
    team = 2 * x + y
    across_team = 2 * x + 1 - y
    across = 2 * z + 1 - y
    x_peer = 2 * (1 - x) + core
    team_ids = ({"dp": x_peer}, {"fsdp": across}, {"fsdp": across, "dp": x_peer})
    way_ids = ({"fsdp": f + 2}, {"fsdp": f - 2}, {"dp": 2 * x + 1 - core})

    def slot(m, s, k):
        if m == 0:
            return qkv_full.at[pl.ds(pl.multiple_of(s * depth + k * quarter, 16), quarter)]
        return out_full.at[s, pl.ds(pl.multiple_of(k * out_quarter, 16), out_quarter)]

    count = 0

    def local(source, dest):
        nonlocal count
        copy = pltpu.make_async_copy(source, dest, local_sem.at[count])
        count += 1
        copy.start()
        return copy

    def qkv_parts(k, owner, dest):
        rows = pl.ds(pl.multiple_of(k * quarter, 16), quarter)
        return [
            local(
                qkv_weight.at[rows, pl.ds(pl.multiple_of(start, 128), size)],
                dest.at[:, pl.ds(to, size)],
            )
            for start, size, to in (
                (owner * query_cols, query_cols, 0),
                (QUERY_FEATURES + owner * key_cols, key_cols, query_cols),
                (QUERY_FEATURES + KEY_FEATURES + owner * key_cols, key_cols, query_cols + key_cols),
            )
        ]

    own_loads, cross_loads = [], []
    for j in range(2):
        k = 2 * j + core
        own_loads.append(qkv_parts(k, team, slot(0, f, k)))
        cross_loads.append(qkv_parts(k, across_team, cross_qkv.at[j]))
    tok_local = local(tokens, tok_own)
    vectors = [
        local(flat, row.at[0, pl.ds(0, flat.shape[0])])
        for flat, row in (
            (norm_gain_flat, norm_gain),
            (final_gain_flat, final_gain),
            (value_head_flat, value_head),
            (qkv_bias_flat, qkv_bias),
        )
    ]
    late_loads = []
    for j in range(2):
        k = 2 * j + 1 - core
        late_loads.extend(qkv_parts(k, team, slot(0, f, k)))
    out_own = local(
        out_weight.at[:, pl.ds(pl.multiple_of(team * query_cols, 128), query_cols)], out_full.at[f]
    )
    out_cross = [
        local(
            out_weight.at[
                pl.ds(pl.multiple_of((2 * j + core) * out_quarter, 16), out_quarter),
                pl.ds(pl.multiple_of(across_team * query_cols, 128), query_cols),
            ],
            cross_out.at[j],
        )
        for j in range(2)
    ]
    len_tile[...] = jnp.full(len_tile.shape, length[0], jnp.int32)
    len_all[0] = len_tile[...]

    barrier = pltpu.get_barrier_semaphore()
    everyone = shards * groups
    me = f * groups + g

    @pl.loop(1, everyone)
    def _(i):
        other = lax.rem(me + i, everyone)
        pl.semaphore_signal(
            barrier, inc=1, device_id={"fsdp": other // groups, "dp": lax.rem(other, groups)}
        )

    pl.semaphore_wait(barrier, everyone - 1)

    def way_copy(way, m, s, j):
        k = 2 * j + core
        return pltpu.make_async_remote_copy(
            src_ref=slot(m, s, k),
            dst_ref=slot(m, s, k),
            send_sem=send_sem.at[way, m, s, j],
            recv_sem=recv_sem.at[m, s, k],
            device_id=way_ids[way],
        )

    def cross_copy(m, j):
        return pltpu.make_async_remote_copy(
            src_ref=(cross_qkv, cross_out)[m].at[j],
            dst_ref=slot(m, f, 2 * j + core),
            send_sem=cross_send.at[m, j],
            recv_sem=recv_sem.at[m, f, 2 * j + core],
            device_id=team_ids[1],
        )

    def arrived(m, s, k):
        pltpu.make_async_copy(slot(m, s, k), slot(m, s, k), recv_sem.at[m, s, k]).wait()

    def send_both(m, s, j):
        pl.when(has_up)(way_copy(UP, m, s, j).start)
        pl.when(has_down)(way_copy(DOWN, m, s, j).start)

    def cross_step(m, j):
        arrived(m, across, 2 * j + core)
        send_both(m, across, j)
        way_copy(PARTNER, m, across, j).start()

    def sides(k, o):
        row = y if o == 0 else 1 - y
        below, above = z - k, z + k
        return (
            (below >= 0, 2 * jnp.maximum(below, 0) + row, UP, has_up),
            (above < line, 2 * jnp.minimum(above, line - 1) + row, DOWN, has_down),
        )

    def line_step(m, k, o, j):
        for ok, s, way, onward in sides(k, o):

            @pl.when(ok)
            def _():
                arrived(m, s, 2 * j + core)
                pl.when(onward)(way_copy(way, m, s, j).start)
                way_copy(PARTNER, m, s, j).start()

    def from_partner(m, s):
        for j in range(2):
            arrived(m, s, 2 * j + 1 - core)

    half_rows = seq_rows // 2

    def tok_copy(way, half):
        source = (0, 0, 1 + half)[way]
        target = team_ids[way] if way < 2 else team_ids[1 - half]
        return pltpu.make_async_remote_copy(
            src_ref=normed.at[pl.ds(source * seq_rows + half * half_rows, half_rows)],
            dst_ref=normed.at[pl.ds((1 + way) * seq_rows + half * half_rows, half_rows)],
            send_sem=tok_send.at[way, half],
            recv_sem=tok_recv.at[way, half],
            device_id=target,
        )

    def len_copy(way):
        return pltpu.make_async_remote_copy(
            src_ref=len_tile,
            dst_ref=len_all.at[1 + way],
            send_sem=len_send.at[way],
            recv_sem=len_recv.at[way],
            device_id=team_ids[way],
        )

    for j in range(2):
        for copy in own_loads[j]:
            copy.wait()
        send_both(0, f, j)
        for copy in cross_loads[j]:
            copy.wait()
        cross_copy(0, j).start()

    tok_local.wait()
    for copy in vectors:
        copy.wait()
    norm_rows = 16

    @pl.loop(0, seq_rows // norm_rows)
    def _(i):
        at = pl.ds(pl.multiple_of(i * norm_rows, norm_rows), norm_rows)
        rows = tok_own[at, :].astype(jnp.float32)
        scale = lax.rsqrt(jnp.mean(rows * rows, axis=-1, keepdims=True) + 1e-06)
        normed[at, :] = (rows * scale * norm_gain[...]).astype(jnp.bfloat16)

    tok_copy(0, 0).start()
    tok_copy(1, 1).start()
    tok_copy(0, 1).start()
    tok_copy(1, 0).start()
    for way in range(3):
        len_copy(way).start()

    bias_parts = (
        (team * query_cols, query_cols, 0),
        (QUERY_FEATURES + team * key_cols, key_cols, query_cols),
        (QUERY_FEATURES + KEY_FEATURES + team * key_cols, key_cols, query_cols + key_cols),
    )
    for start, size, to in bias_parts:
        qkv_rows[:, to : to + size] = jnp.broadcast_to(
            qkv_bias[:, pl.ds(pl.multiple_of(start, HEAD_SIZE), size)],
            (groups * seq_rows, size),
        )

    for j in range(2):
        cross_step(0, j)
        line_step(0, 1, 0, j)
    tok_copy(0, 0).wait_recv()
    tok_copy(2, 0).start()
    line_step(0, 1, 1, 0)
    line_step(0, 1, 1, 1)
    tok_copy(1, 1).wait_recv()
    tok_copy(2, 1).start()
    out_own.wait()
    for j in range(2):
        out_cross[j].wait()
        cross_copy(1, j).start()
    for k in range(2, line - 1):
        for o in range(2):
            for j in range(2):
                line_step(0, k, o, j)
    for j in range(2):
        send_both(1, f, j)

    tok_copy(0, 1).wait_recv()
    tok_copy(1, 0).wait_recv()
    tok_copy(2, 0).wait_recv()
    tok_copy(2, 1).wait_recv()
    for way in range(3):
        len_copy(way).wait_recv()
    for copy in late_loads:
        copy.wait()

    tile = 3 * HEAD_SIZE

    def qkv_step(place):
        rows = pl.ds(pl.multiple_of(place * 2 * depth, 128), 2 * depth)

        @pl.loop(0, (query_cols + 2 * key_cols) // tile)
        def _(t):
            cols = pl.ds(pl.multiple_of(t * tile, tile), tile)
            qkv_rows[:, cols] += jnp.dot(
                normed[:, rows], qkv_full[rows, cols], preferred_element_type=jnp.float32
            )

    def qkv_places(first, last):
        @pl.loop(2 * first, 2 * last)
        def _(i):
            k = i // 2
            place = z + (2 * lax.rem(i, 2) - 1) * k

            @pl.when((place >= 0) & (place < line))
            def _():
                from_partner(0, 2 * place)
                from_partner(0, 2 * place + 1)
                qkv_step(place)

    @pl.loop(0, 1)
    def _(i):
        from_partner(0, across)
        qkv_step(z)

    qkv_places(1, line - 1)
    for j in range(2):
        cross_step(1, j)
    for o in range(2):
        for j in range(2):
            line_step(0, line - 1, o, j)
    qkv_places(line - 1, line)

    def head_rows(j, column):
        return qkv_rows[
            pl.ds(pl.multiple_of(j * seq_rows, seq_rows), seq_rows), column : column + HEAD_SIZE
        ]

    def rotate(rows):
        return (
            rows * cosine[...] + pltpu.roll(rows, HEAD_SIZE // 2, 1) * sine[...]
        ).astype(jnp.bfloat16)

    key_heads = key_cols // HEAD_SIZE
    share = heads // key_heads

    @pl.loop(0, groups)
    def _(j):
        query_place = lax.broadcasted_iota(jnp.int32, (seq_rows, seq_rows), 0)
        key_place = lax.broadcasted_iota(jnp.int32, (seq_rows, seq_rows), 1)
        allowed = (key_place <= query_place) & (key_place < len_all[j, 0:1, :])
        at = pl.ds(pl.multiple_of(j * seq_rows, seq_rows), seq_rows)
        for kh in range(key_heads):
            offset = kh * HEAD_SIZE
            key = rotate(head_rows(j, query_cols + offset))
            value = head_rows(j, query_cols + key_cols + offset).astype(jnp.bfloat16)
            for h in range(kh * share, (kh + 1) * share):
                query = rotate(head_rows(j, h * HEAD_SIZE))
                scores = lax.dot_general(
                    query, key, (((1,), (1,)), ((), ())), preferred_element_type=jnp.float32
                ) / np.float32(np.sqrt(HEAD_SIZE))
                scores = jnp.where(allowed, scores, jnp.float32(-1e30))
                expd = jnp.exp(scores - jnp.max(scores, axis=-1, keepdims=True))
                probs = (expd / jnp.sum(expd, axis=-1, keepdims=True)).astype(jnp.bfloat16)
                attn[at, h * HEAD_SIZE : (h + 1) * HEAD_SIZE] = jnp.dot(
                    probs, value, preferred_element_type=jnp.float32
                ).astype(jnp.bfloat16)

    def part_copy(way, s):
        return pltpu.make_async_remote_copy(
            src_ref=part_out.at[s, pl.ds((1 + way) * seq_rows, seq_rows)],
            dst_ref=part_in.at[way, s],
            send_sem=part_send.at[way, s],
            recv_sem=part_recv.at[way, s],
            device_id=team_ids[way],
        )

    def project(s):
        result = lax.dot_general(
            attn[...],
            out_full[s],
            (((1,), (1,)), ((), ())),
            preferred_element_type=jnp.float32,
        )
        part_out[s] = result.astype(jnp.bfloat16)
        own[s] = result[:seq_rows]
        for way in (2, 0, 1):
            part_copy(way, s).start()

    place = lax.broadcasted_iota(jnp.int32, len_tile.shape, 1)
    pick = (place == len_tile[...] - 1).astype(jnp.bfloat16)
    stats[...] = jnp.zeros_like(stats)

    def hidden_copy(place):
        cols = pl.ds(pl.multiple_of(place * 2 * out_cols, 128), 2 * out_cols)
        return pltpu.make_async_copy(
            hidden.at[:, cols], hidden_out.at[:, cols], hidden_sem.at[place]
        )

    def finish(place):
        sums = []
        for s in (2 * place, 2 * place + 1):
            for way in range(3):
                part_copy(way, s).wait_recv()
            total = own[s]
            for way in range(3):
                total += part_in[way, s].astype(jnp.float32)
            sums.append(total)
        cols = pl.ds(pl.multiple_of(place * 2 * out_cols, 128), 2 * out_cols)
        hidden[:, cols] = (
            tok_own[:, cols].astype(jnp.float32) + jnp.concatenate(sums, axis=1)
        ).astype(jnp.bfloat16)
        hidden_copy(place).start()
        last = jnp.dot(pick, hidden[:, cols], preferred_element_type=jnp.float32)
        weighted = last * final_gain[:, cols] * value_head[:, cols]
        squares = last * last
        for t in range(2 * out_cols // HEAD_SIZE):
            lanes = slice(t * HEAD_SIZE, (t + 1) * HEAD_SIZE)
            stats[0] += squares[:, lanes]
            stats[1] += weighted[:, lanes]

    def project_places(k, o):
        @pl.loop(0, 2)
        def _(i):
            place = z + (2 * i - 1) * k
            s = 2 * place + (y if o == 0 else 1 - y)

            @pl.when((place >= 0) & (place < line))
            def _():
                from_partner(1, s)
                project(s)

    def finish_places(k):
        @pl.loop(0, 2)
        def _(i):
            place = z + (2 * i - 1) * k

            @pl.when((place >= 0) & (place < line))
            def _():
                finish(place)

    for j in range(2):
        line_step(1, 1, 0, j)

    @pl.loop(0, 2)
    def _(i):
        @pl.when(i == 1)
        def _():
            from_partner(1, across)

        project(jnp.where(i == 0, f, across))

    for k in range(1, line):
        project_places(k, 0)
        for j in range(2):
            line_step(1, k, 1, j)
        project_places(k, 1)
        if k < line - 1:
            for j in range(2):
                line_step(1, k + 1, 0, j)
        if k == 1:

            @pl.loop(0, 1)
            def _(i):
                finish(z)

        else:
            finish_places(k - 1)
    finish_places(line - 1)

    mean = jnp.sum(stats[0], axis=-1, keepdims=True) / width
    score = jnp.sum(stats[1], axis=-1, keepdims=True) * lax.rsqrt(mean + 1e-06)
    first_row = lax.broadcasted_iota(jnp.int32, score_tile.shape, 0) == 0
    score_tile[...] = jnp.where(first_row, score, jnp.full(score_tile.shape, pair_weight[0]))
    score_all[me] = score_tile[...]

    def score_copy(i):
        other = lax.rem(me + i, everyone)
        return pltpu.make_async_remote_copy(
            src_ref=score_tile,
            dst_ref=score_all.at[me],
            send_sem=score_send.at[other],
            recv_sem=score_recv.at[me],
            device_id={"fsdp": other // groups, "dp": lax.rem(other, groups)},
        )

    @pl.loop(1, everyone)
    def _(i):
        score_copy(i).start()

    @pl.loop(0, everyone)
    def _(i):
        partner_rows[pl.ds(i, 1), :] = jnp.full((1, HEAD_SIZE), partner[i], jnp.int32)

    @pl.loop(0, line)
    def _(place):
        hidden_copy(place).wait()

    for m in range(2):
        for j in range(2):
            cross_copy(m, j).wait_send()

    @pl.loop(0, shards)
    def _(s):
        for way, ok in (
            (UP, has_up & (s // 2 <= z)),
            (DOWN, has_down & (s // 2 >= z)),
            (PARTNER, s != f),
        ):

            @pl.when(ok)
            def _():
                for m in range(2):
                    for j in range(2):
                        way_copy(way, m, s, j).wait_send()

        for way in range(3):
            part_copy(way, s).wait_send()

    for way in range(3):
        len_copy(way).wait_send()
        for half in range(2):
            tok_copy(way, half).wait_send()

    @pl.loop(1, everyone)
    def _(i):
        other = lax.rem(me + i, everyone)
        pltpu.make_async_copy(
            score_all.at[other], score_all.at[other], score_recv.at[other]
        ).wait()

    scores = score_all[:, 0, :]
    weights = score_all[:, 1, :]
    row = lax.broadcasted_iota(jnp.int32, scores.shape, 0)
    lane = lax.broadcasted_iota(jnp.int32, scores.shape, 1)
    partners = partner_rows[...]
    score_row = jnp.sum(jnp.where(row == lane, scores, 0.0), axis=0, keepdims=True)
    others = jnp.sum(jnp.where(partners == lane, score_row, 0.0), axis=1, keepdims=True)
    margins = jnp.where(row < partners, scores - others, others - scores)
    softplus = jnp.maximum(-margins, 0.0) + jnp.log1p(jnp.exp(-jnp.abs(margins)))
    first_lane = lane == 0
    margin_out[0] = jnp.sum(jnp.where(first_lane & (row == me), margins, 0.0))
    loss_out[0] = jnp.sum(jnp.where(first_lane, weights * softplus, 0.0)) / everyone

    @pl.loop(1, everyone)
    def _(i):
        score_copy(i).wait_send()


def layer_fits(shards, groups, tokens, qkv_weight, out_weight):
    return (
        shards % 2 == 0
        and shards >= 8
        and qkv_weight.shape[0] % 64 == 0
        and groups == 4
        and KEY_VALUE_HEADS % groups == 0
        and tokens.shape[1] == HEAD_SIZE
        and shards * groups <= HEAD_SIZE
        and out_weight.shape[1] % 64 == 0
    )


def layer(
    tokens,
    lengths,
    partner,
    pair_weight,
    norm_gain,
    qkv_weight,
    qkv_bias,
    out_weight,
    final_gain,
    value_head,
):
    shards, groups = lax.axis_size("fsdp"), lax.axis_size("dp")
    _, seq_rows, width = tokens.shape
    depth = qkv_weight.shape[0]
    out_cols = out_weight.shape[1]
    query_cols = QUERY_FEATURES // groups
    key_cols = KEY_FEATURES // groups
    all_cols = query_cols + 2 * key_cols
    rows = groups * seq_rows
    cosine, sine = rotary_tables(seq_rows)
    everyone = shards * groups
    dma = pltpu.SemaphoreType.DMA
    vmem = pl.BlockSpec(memory_space=pltpu.VMEM)
    anywhere = pl.BlockSpec(memory_space=pl.ANY)
    bf16, f32 = jnp.bfloat16, jnp.float32
    scalar = pl.BlockSpec(memory_space=pltpu.SMEM)
    hidden, margin, loss = pl.pallas_call(
        functools.partial(layer_kernel, shards, groups),
        out_shape=(
            jax.ShapeDtypeStruct((seq_rows, width), bf16),
            jax.ShapeDtypeStruct((1,), f32),
            jax.ShapeDtypeStruct((1,), f32),
        ),
        in_specs=[anywhere] * 3 + [scalar] * 3 + [anywhere] * 4 + [vmem] * 2,
        out_specs=(anywhere, scalar, scalar),
        scratch_shapes=[
            pltpu.VMEM((shards * depth, all_cols), bf16),
            pltpu.VMEM((shards, out_cols, query_cols), bf16),
            pltpu.VMEM((2, depth // 4, all_cols), bf16),
            pltpu.VMEM((2, out_cols // 4, query_cols), bf16),
            pltpu.VMEM((seq_rows, width), bf16),
            pltpu.VMEM((8, seq_rows), jnp.int32),
            pltpu.VMEM((groups, 8, seq_rows), jnp.int32),
            pltpu.VMEM((rows, width), bf16),
            pltpu.VMEM((rows, all_cols), f32),
            pltpu.VMEM((rows, query_cols), bf16),
            pltpu.VMEM((shards, seq_rows, out_cols), f32),
            pltpu.VMEM((shards, rows, out_cols), bf16),
            pltpu.VMEM((groups - 1, shards, seq_rows, out_cols), bf16),
            pltpu.VMEM((seq_rows, width), bf16),
            pltpu.VMEM((2, 8, HEAD_SIZE), f32),
            pltpu.VMEM((8, HEAD_SIZE), f32),
            pltpu.VMEM((everyone, 8, HEAD_SIZE), f32),
            pltpu.VMEM((everyone, HEAD_SIZE), jnp.int32),
            pltpu.VMEM((1, width), f32),
            pltpu.VMEM((1, width + 8 * HEAD_SIZE), f32),
            pltpu.VMEM((1, width + 8 * HEAD_SIZE), f32),
            pltpu.VMEM((1, qkv_bias.shape[0] + 8 * HEAD_SIZE), f32),
            dma((26,)),
            dma((2, shards, 4)),
            dma((3, 2, shards, 2)),
            dma((2, 2)),
            dma((3, 2)),
            dma((3, 2)),
            dma((3,)),
            dma((3,)),
            dma((3, shards)),
            dma((3, shards)),
            dma((everyone,)),
            dma((everyone,)),
            dma((shards // 2,)),
        ],
        compiler_params=pltpu.CompilerParams(
            collective_id=0, has_side_effects=True, vmem_limit_bytes=60 * 1024 * 1024
        ),
    )(
        tokens[0],
        qkv_weight,
        out_weight.T,
        lengths,
        pair_weight,
        partner,
        norm_gain,
        final_gain,
        value_head,
        qkv_bias,
        jnp.asarray(cosine),
        jnp.asarray(sine),
    )
    return hidden[None], margin, loss.reshape(())


def projected_by_gathers(
    tokens,
    lengths,
    norm_gain,
    qkv_weight,
    qkv_bias,
    out_weight,
):
    sequence = tokens[0]
    length_rows = sequence.shape[0]
    width = sequence.shape[1]
    normed = rms_scale(sequence.astype(jnp.float32), norm_gain).astype(jnp.bfloat16)
    query_group_count = lax.axis_size("dp")
    group_index = lax.axis_index("dp")
    query_heads = QUERY_HEADS // query_group_count
    key_value_heads = KEY_VALUE_HEADS // query_group_count
    query_cols = query_heads * HEAD_SIZE
    key_cols = key_value_heads * HEAD_SIZE
    group_normed, group_lengths = (
        lax.all_gather(normed[None], "dp", axis=0, tiled=True),
        lax.all_gather(lengths, "dp", axis=0, tiled=True),
    )
    seq_count = group_normed.shape[0]
    flat = group_normed.reshape(seq_count * length_rows, width)
    qkv_cols = jnp.concatenate(
        [
            lax.dynamic_slice_in_dim(qkv_weight, group_index * query_cols, query_cols, 1),
            lax.dynamic_slice_in_dim(
                qkv_weight, QUERY_FEATURES + group_index * key_cols, key_cols, 1
            ),
            lax.dynamic_slice_in_dim(
                qkv_weight, QUERY_FEATURES + KEY_FEATURES + group_index * key_cols, key_cols, 1
            ),
        ],
        axis=1,
    )
    bias_cols = jnp.concatenate(
        [
            lax.dynamic_slice_in_dim(qkv_bias, group_index * query_cols, query_cols, 0),
            lax.dynamic_slice_in_dim(
                qkv_bias, QUERY_FEATURES + group_index * key_cols, key_cols, 0
            ),
            lax.dynamic_slice_in_dim(
                qkv_bias, QUERY_FEATURES + KEY_FEATURES + group_index * key_cols, key_cols, 0
            ),
        ],
        axis=0,
    )
    out_rows = lax.dynamic_slice_in_dim(out_weight, group_index * query_cols, query_cols, 0)
    qkv_full, out_full = (
        lax.all_gather(qkv_cols, "fsdp", axis=0, tiled=True),
        lax.all_gather(out_rows, "fsdp", axis=1, tiled=True),
    )
    query_key_value = jnp.dot(flat, qkv_full, preferred_element_type=jnp.float32) + bias_cols
    attn = attend(
        query_key_value.reshape(seq_count, length_rows, -1),
        group_lengths,
        query_heads,
        key_value_heads,
    )
    return lax.psum_scatter(
        jnp.dot(attn, out_full, preferred_element_type=jnp.float32),
        "dp",
        scatter_dimension=0,
        tiled=True,
    )


def per_device(
    tokens,
    lengths,
    partner,
    pair_weight,
    norm_gain,
    qkv_weight,
    qkv_bias,
    out_weight,
    final_gain,
    value_head,
):
    if layer_fits(lax.axis_size("fsdp"), lax.axis_size("dp"), tokens, qkv_weight, out_weight):
        return layer(
            tokens,
            lengths,
            partner,
            pair_weight,
            norm_gain,
            qkv_weight,
            qkv_bias,
            out_weight,
            final_gain,
            value_head,
        )
    sequence = tokens[0]
    length = lengths[0]
    projected = projected_by_gathers(tokens, lengths, norm_gain, qkv_weight, qkv_bias, out_weight)
    hidden = (sequence.astype(jnp.float32) + projected).astype(jnp.bfloat16)
    last = lax.dynamic_slice_in_dim(hidden, length - 1, 1, 0)[0].astype(jnp.float32)
    score = jnp.sum(rms_scale(last, final_gain) * value_head)
    everyone, weights_all = (
        lax.all_gather(score.reshape(1), ("fsdp", "dp"), axis=0, tiled=True),
        lax.all_gather(pair_weight, ("fsdp", "dp"), axis=0, tiled=True),
    )
    total_seqs = everyone.shape[0]
    mine = lax.axis_index(("fsdp", "dp"))
    index_all = jnp.arange(total_seqs, dtype=jnp.int32)
    my_partner = jnp.sum(jnp.where(index_all == mine, partner, 0))
    other = jnp.sum(jnp.where(index_all == my_partner, everyone, jnp.float32(0.0)))
    margin = jnp.where(mine < my_partner, score - other, other - score)
    matches = partner[:, None] == index_all[None, :]
    others_all = jnp.sum(jnp.where(matches, everyone[None, :], jnp.float32(0.0)), axis=1)
    margins_all = jnp.where(index_all < partner, everyone - others_all, others_all - everyone)
    loss = jnp.sum(weights_all * jax.nn.softplus(-margins_all)) / total_seqs
    return (hidden[None], margin.reshape(1), loss)


def solution(mesh):
    return jax.shard_map(
        per_device,
        mesh=mesh,
        in_specs=(
            P(("fsdp", "dp"), None, None),
            P(("fsdp", "dp")),
            P(),
            P(("fsdp", "dp")),
            P(),
            P("fsdp", None),
            P(),
            P(None, "fsdp"),
            P(),
            P(),
        ),
        out_specs=(P(("fsdp", "dp"), None, None), P(("fsdp", "dp")), P()),
        check_vma=False,
    )
```

```python
import functools

import jax
import jax.numpy as jnp
import numpy as np
from jax import lax
from jax.experimental import pallas as pl
from jax.experimental.pallas import tpu as pltpu
from jax.sharding import PartitionSpec as P

QUERY_HEADS = 28
KEY_VALUE_HEADS = 4
HEAD_SIZE = 128
QUERY_FEATURES = 3584
KEY_FEATURES = 512


def rms_scale(value_rows, gain):
    return (
        value_rows
        * lax.rsqrt(jnp.mean(value_rows * value_rows, axis=-1, keepdims=True) + 1e-06)
        * gain
    )


def apply_rotary(heads, length_rows):
    half = HEAD_SIZE // 2
    positions = jnp.arange(length_rows, dtype=jnp.float32)
    freqs = jnp.exp(
        -(2.0 * jnp.arange(half, dtype=jnp.float32) / HEAD_SIZE) * jnp.log(jnp.float32(1000000.0))
    )
    angles = positions[:, None] * freqs[None, :]
    cosine = jnp.cos(angles)
    sine = jnp.sin(angles)
    first = heads[..., :half]
    second = heads[..., half:]
    return jnp.concatenate(
        [first * cosine - second * sine, second * cosine + first * sine], axis=-1
    )


def attend(query_key_value, group_lengths, query_heads, key_value_heads):
    seq_count, length_rows, _ = query_key_value.shape
    query_width = query_heads * HEAD_SIZE
    key_width = key_value_heads * HEAD_SIZE
    query_rows = (
        query_key_value[..., :query_width]
        .reshape(seq_count, length_rows, query_heads, HEAD_SIZE)
        .transpose(0, 2, 1, 3)
    )
    key_rows = (
        query_key_value[..., query_width : query_width + key_width]
        .reshape(seq_count, length_rows, key_value_heads, HEAD_SIZE)
        .transpose(0, 2, 1, 3)
    )
    value_rows = (
        query_key_value[..., query_width + key_width :]
        .reshape(seq_count, length_rows, key_value_heads, HEAD_SIZE)
        .transpose(0, 2, 1, 3)
        .astype(jnp.bfloat16)
    )
    query_rows = (
        apply_rotary(query_rows, length_rows)
        .astype(jnp.bfloat16)
        .reshape(seq_count, key_value_heads, query_heads // key_value_heads, length_rows, HEAD_SIZE)
    )
    key_rows = apply_rotary(key_rows, length_rows).astype(jnp.bfloat16)
    scores = jnp.einsum(
        "bgqtd,bgsd->bgqts", query_rows, key_rows, preferred_element_type=jnp.float32
    ) / jnp.sqrt(jnp.float32(HEAD_SIZE))
    places = jnp.arange(length_rows, dtype=jnp.int32)
    causal = places[None, :] <= places[:, None]
    usable = places[None, :] < group_lengths[:, None]
    allowed = causal[None, :, :] & usable[:, None, :]
    scores = jnp.where(allowed[:, None, None, :, :], scores, jnp.float32(-1e30))
    highest = jnp.max(scores, axis=-1, keepdims=True)
    expd = jnp.exp(scores - highest)
    probs = (expd / jnp.sum(expd, axis=-1, keepdims=True)).astype(jnp.bfloat16)
    mixed = jnp.einsum("bgqts,bgsd->bgqtd", probs, value_rows, preferred_element_type=jnp.float32)
    mixed = mixed.reshape(seq_count, query_heads, length_rows, HEAD_SIZE).transpose(0, 2, 1, 3)
    return mixed.reshape(seq_count * length_rows, query_width).astype(jnp.bfloat16)


UP, DOWN, PARTNER = 0, 1, 2


def rotary_tables(length_rows):
    half = HEAD_SIZE // 2
    freqs = 1000000.0 ** (-2.0 * np.arange(half) / HEAD_SIZE)
    angles = np.arange(length_rows)[:, None] * freqs[None, :]
    cosine, sine = np.cos(angles), np.sin(angles)
    return (
        np.concatenate([cosine, cosine], axis=1).astype(np.float32),
        np.concatenate([-sine, sine], axis=1).astype(np.float32),
    )


def layer_kernel(
    shards,
    groups,
    tokens,
    qkv_weight,
    out_weight,
    length_one,
    pair_weight_one,
    partner_all,
    norm_gain_flat,
    final_gain_flat,
    value_head_flat,
    qkv_bias_flat,
    cosine_table,
    sine_table,
    hidden,
    margin_out,
    loss_out,
    qkv_full,
    out_full,
    cross_qkv,
    cross_out,
    tok_own,
    len_tile,
    len_all,
    normed,
    qkv_rows,
    attn,
    own,
    part_out,
    part_in,
    stats,
    score_tile,
    score_all,
    partner_rows,
    norm_gain,
    final_gain,
    value_head,
    qkv_bias,
    cosine,
    sine,
    length,
    pair_weight,
    partner,
    local_sem,
    recv_sem,
    send_sem,
    cross_send,
    tok_send,
    tok_recv,
    len_send,
    len_recv,
    part_send,
    part_recv,
    score_send,
    score_recv,
):
    line = shards // 2
    f = lax.axis_index("fsdp")
    g = lax.axis_index("dp")
    z = f // 2
    y = f % 2
    x = g // 2
    core = g % 2
    seq_rows = tokens.shape[0]
    width = tokens.shape[1]
    depth = qkv_weight.shape[0]
    out_cols = out_weight.shape[0]
    query_cols = QUERY_FEATURES // groups
    key_cols = KEY_FEATURES // groups
    heads = query_cols // HEAD_SIZE
    quarter = depth // 4
    out_quarter = out_cols // 4
    has_up = z < line - 1
    has_down = z > 0
    team = 2 * x + y
    across_team = 2 * x + 1 - y
    across = 2 * z + 1 - y
    x_peer = 2 * (1 - x) + core
    team_ids = ({"dp": x_peer}, {"fsdp": across}, {"fsdp": across, "dp": x_peer})
    way_ids = ({"fsdp": f + 2}, {"fsdp": f - 2}, {"dp": 2 * x + 1 - core})

    barrier = pltpu.get_barrier_semaphore()
    for target in (*team_ids, way_ids[PARTNER]):
        pl.semaphore_signal(barrier, inc=1, device_id=target)
    for way, ok in ((UP, has_up), (DOWN, has_down)):

        @pl.when(ok)
        def _():
            pl.semaphore_signal(barrier, inc=1, device_id=way_ids[way])

    def slot(m, s, k):
        if m == 0:
            return qkv_full.at[pl.ds(pl.multiple_of(s * depth + k * quarter, 16), quarter)]
        return out_full.at[s, pl.ds(pl.multiple_of(k * out_quarter, 16), out_quarter)]

    count = 0

    def local(source, dest):
        nonlocal count
        copy = pltpu.make_async_copy(source, dest, local_sem.at[count])
        count += 1
        copy.start()
        return copy

    def qkv_parts(k, owner, dest):
        rows = pl.ds(pl.multiple_of(k * quarter, 16), quarter)
        return [
            local(
                qkv_weight.at[rows, pl.ds(pl.multiple_of(start, 128), size)],
                dest.at[:, pl.ds(to, size)],
            )
            for start, size, to in (
                (owner * query_cols, query_cols, 0),
                (QUERY_FEATURES + owner * key_cols, key_cols, query_cols),
                (QUERY_FEATURES + KEY_FEATURES + owner * key_cols, key_cols, query_cols + key_cols),
            )
        ]

    length_load = local(length_one, length)
    own_loads, cross_loads = [], []
    for j in range(2):
        k = 2 * j + core
        own_loads.append(qkv_parts(k, team, slot(0, f, k)))
        cross_loads.append(qkv_parts(k, across_team, cross_qkv.at[j]))
    tok_local = local(tokens, tok_own)
    vectors = [
        local(flat, row.at[0, pl.ds(0, flat.shape[0])])
        for flat, row in (
            (norm_gain_flat, norm_gain),
            (final_gain_flat, final_gain),
            (value_head_flat, value_head),
            (qkv_bias_flat, qkv_bias),
        )
    ]
    late_loads = []
    for j in range(2):
        k = 2 * j + 1 - core
        late_loads.extend(qkv_parts(k, team, slot(0, f, k)))
    out_own = local(
        out_weight.at[:, pl.ds(pl.multiple_of(team * query_cols, 128), query_cols)], out_full.at[f]
    )
    out_cross = [
        local(
            out_weight.at[
                pl.ds(pl.multiple_of((2 * j + core) * out_quarter, 16), out_quarter),
                pl.ds(pl.multiple_of(across_team * query_cols, 128), query_cols),
            ],
            cross_out.at[j],
        )
        for j in range(2)
    ]
    small_loads = [
        local(source, dest)
        for source, dest in (
            (pair_weight_one, pair_weight),
            (partner_all, partner),
            (cosine_table, cosine),
            (sine_table, sine),
        )
    ]
    everyone = shards * groups
    me = f * groups + g

    pl.semaphore_wait(barrier, 4 + has_up.astype(jnp.int32) + has_down.astype(jnp.int32))

    def way_copy(way, m, s, j):
        k = 2 * j + core
        return pltpu.make_async_remote_copy(
            src_ref=slot(m, s, k),
            dst_ref=slot(m, s, k),
            send_sem=send_sem.at[way, m, s, j],
            recv_sem=recv_sem.at[m, s, k],
            device_id=way_ids[way],
        )

    def cross_copy(m, j):
        return pltpu.make_async_remote_copy(
            src_ref=(cross_qkv, cross_out)[m].at[j],
            dst_ref=slot(m, f, 2 * j + core),
            send_sem=cross_send.at[m, j],
            recv_sem=recv_sem.at[m, f, 2 * j + core],
            device_id=team_ids[1],
        )

    def arrived(m, s, k):
        pltpu.make_async_copy(slot(m, s, k), slot(m, s, k), recv_sem.at[m, s, k]).wait()

    def send_both(m, s, j):
        pl.when(has_up)(way_copy(UP, m, s, j).start)
        pl.when(has_down)(way_copy(DOWN, m, s, j).start)

    def cross_step(m, j):
        arrived(m, across, 2 * j + core)
        send_both(m, across, j)
        way_copy(PARTNER, m, across, j).start()

    def sides(k, o):
        row = y if o == 0 else 1 - y
        below, above = z - k, z + k
        return (
            (below >= 0, 2 * jnp.maximum(below, 0) + row, UP, has_up),
            (above < line, 2 * jnp.minimum(above, line - 1) + row, DOWN, has_down),
        )

    def line_step(m, k, o, j):
        for ok, s, way, onward in sides(k, o):

            @pl.when(ok)
            def _():
                arrived(m, s, 2 * j + core)
                pl.when(onward)(way_copy(way, m, s, j).start)
                way_copy(PARTNER, m, s, j).start()

    def from_partner(m, s):
        for j in range(2):
            arrived(m, s, 2 * j + 1 - core)

    half_rows = seq_rows // 2

    def tok_copy(way, half):
        source = (0, 0, 1 + half)[way]
        target = team_ids[way] if way < 2 else team_ids[1 - half]
        return pltpu.make_async_remote_copy(
            src_ref=normed.at[pl.ds(source * seq_rows + half * half_rows, half_rows)],
            dst_ref=normed.at[pl.ds((1 + way) * seq_rows + half * half_rows, half_rows)],
            send_sem=tok_send.at[way, half],
            recv_sem=tok_recv.at[way, half],
            device_id=target,
        )

    def len_copy(way):
        return pltpu.make_async_remote_copy(
            src_ref=len_tile,
            dst_ref=len_all.at[1 + way],
            send_sem=len_send.at[way],
            recv_sem=len_recv.at[way],
            device_id=team_ids[way],
        )

    for j in range(2):
        for copy in own_loads[j]:
            copy.wait()
        send_both(0, f, j)
        for copy in cross_loads[j]:
            copy.wait()
        cross_copy(0, j).start()

    tok_local.wait()
    for copy in vectors:
        copy.wait()
    norm_rows = 16

    @pl.loop(0, seq_rows // norm_rows)
    def _(i):
        at = pl.ds(pl.multiple_of(i * norm_rows, norm_rows), norm_rows)
        rows = tok_own[at, :].astype(jnp.float32)
        scale = lax.rsqrt(jnp.mean(rows * rows, axis=-1, keepdims=True) + 1e-06)
        normed[at, :] = (rows * scale * norm_gain[...]).astype(jnp.bfloat16)

    tok_copy(0, 0).start()
    tok_copy(1, 1).start()
    tok_copy(0, 1).start()
    tok_copy(1, 0).start()
    length_load.wait()
    len_tile[...] = jnp.full(len_tile.shape, length[0], jnp.int32)
    len_all[0] = len_tile[...]
    for way in range(3):
        len_copy(way).start()

    bias_parts = (
        (team * query_cols, query_cols, 0),
        (QUERY_FEATURES + team * key_cols, key_cols, query_cols),
        (QUERY_FEATURES + KEY_FEATURES + team * key_cols, key_cols, query_cols + key_cols),
    )
    for start, size, to in bias_parts:
        qkv_rows[:, to : to + size] = jnp.broadcast_to(
            qkv_bias[:, pl.ds(pl.multiple_of(start, HEAD_SIZE), size)],
            (groups * seq_rows, size),
        )

    for j in range(2):
        cross_step(0, j)
        line_step(0, 1, 0, j)
    tok_copy(0, 0).wait_recv()
    tok_copy(2, 0).start()
    line_step(0, 1, 1, 0)
    line_step(0, 1, 1, 1)
    tok_copy(1, 1).wait_recv()
    tok_copy(2, 1).start()
    out_own.wait()
    for j in range(2):
        out_cross[j].wait()
        cross_copy(1, j).start()
    for k in range(2, line - 1):
        for o in range(2):
            for j in range(2):
                line_step(0, k, o, j)
    for j in range(2):
        send_both(1, f, j)

    tok_copy(0, 1).wait_recv()
    tok_copy(1, 0).wait_recv()
    tok_copy(2, 0).wait_recv()
    tok_copy(2, 1).wait_recv()
    for way in range(3):
        len_copy(way).wait_recv()
    for copy in (*late_loads, *small_loads):
        copy.wait()

    @pl.loop(0, everyone)
    def _(i):
        partner_rows[pl.ds(i, 1), :] = jnp.full((1, HEAD_SIZE), partner[i], jnp.int32)

    tile = 3 * HEAD_SIZE

    def qkv_step(place):
        rows = pl.ds(pl.multiple_of(place * 2 * depth, 128), 2 * depth)

        @pl.loop(0, (query_cols + 2 * key_cols) // tile)
        def _(t):
            cols = pl.ds(pl.multiple_of(t * tile, tile), tile)
            qkv_rows[:, cols] += jnp.dot(
                normed[:, rows], qkv_full[rows, cols], preferred_element_type=jnp.float32
            )

    def qkv_places(first, last):
        @pl.loop(2 * first, 2 * last)
        def _(i):
            k = i // 2
            place = z + (2 * lax.rem(i, 2) - 1) * k

            @pl.when((place >= 0) & (place < line))
            def _():
                from_partner(0, 2 * place)
                from_partner(0, 2 * place + 1)
                qkv_step(place)

    @pl.loop(0, 1)
    def _(i):
        from_partner(0, across)
        qkv_step(z)

    qkv_places(1, line - 1)
    for j in range(2):
        cross_step(1, j)
    for o in range(2):
        for j in range(2):
            line_step(0, line - 1, o, j)
    qkv_places(line - 1, line)

    def head_rows(j, column):
        return qkv_rows[
            pl.ds(pl.multiple_of(j * seq_rows, seq_rows), seq_rows), column : column + HEAD_SIZE
        ]

    def rotate(rows):
        return (
            rows * cosine[...] + pltpu.roll(rows, HEAD_SIZE // 2, 1) * sine[...]
        ).astype(jnp.bfloat16)

    key_heads = key_cols // HEAD_SIZE
    share = heads // key_heads

    @pl.loop(0, groups)
    def _(j):
        query_place = lax.broadcasted_iota(jnp.int32, (seq_rows, seq_rows), 0)
        key_place = lax.broadcasted_iota(jnp.int32, (seq_rows, seq_rows), 1)
        allowed = (key_place <= query_place) & (key_place < len_all[j, 0:1, :])
        at = pl.ds(pl.multiple_of(j * seq_rows, seq_rows), seq_rows)
        for kh in range(key_heads):
            offset = kh * HEAD_SIZE
            key = rotate(head_rows(j, query_cols + offset))
            value = head_rows(j, query_cols + key_cols + offset).astype(jnp.bfloat16)
            for h in range(kh * share, (kh + 1) * share):
                query = rotate(head_rows(j, h * HEAD_SIZE))
                scores = lax.dot_general(
                    query, key, (((1,), (1,)), ((), ())), preferred_element_type=jnp.float32
                ) / np.float32(np.sqrt(HEAD_SIZE))
                scores = jnp.where(allowed, scores, jnp.float32(-1e30))
                expd = jnp.exp(scores - jnp.max(scores, axis=-1, keepdims=True))
                probs = (expd / jnp.sum(expd, axis=-1, keepdims=True)).astype(jnp.bfloat16)
                attn[at, h * HEAD_SIZE : (h + 1) * HEAD_SIZE] = jnp.dot(
                    probs, value, preferred_element_type=jnp.float32
                ).astype(jnp.bfloat16)

    def part_copy(way, s):
        return pltpu.make_async_remote_copy(
            src_ref=part_out.at[s, pl.ds((1 + way) * seq_rows, seq_rows)],
            dst_ref=part_in.at[way, s],
            send_sem=part_send.at[way, s],
            recv_sem=part_recv.at[way, s],
            device_id=team_ids[way],
        )

    def project(s):
        result = lax.dot_general(
            attn[...],
            out_full[s],
            (((1,), (1,)), ((), ())),
            preferred_element_type=jnp.float32,
        )
        part_out[s] = result.astype(jnp.bfloat16)
        own[s] = result[:seq_rows]
        for way in (2, 0, 1):
            part_copy(way, s).start()

    place = lax.broadcasted_iota(jnp.int32, len_tile.shape, 1)
    pick = (place == len_tile[...] - 1).astype(jnp.bfloat16)
    stats[...] = jnp.zeros_like(stats)

    def finish(place):
        sums = []
        for s in (2 * place, 2 * place + 1):
            for way in range(3):
                part_copy(way, s).wait_recv()
            total = own[s]
            for way in range(3):
                total += part_in[way, s].astype(jnp.float32)
            sums.append(total)
        cols = pl.ds(pl.multiple_of(place * 2 * out_cols, 128), 2 * out_cols)
        hidden[:, cols] = (
            tok_own[:, cols].astype(jnp.float32) + jnp.concatenate(sums, axis=1)
        ).astype(jnp.bfloat16)
        last = jnp.dot(pick, hidden[:, cols], preferred_element_type=jnp.float32)
        weighted = last * final_gain[:, cols] * value_head[:, cols]
        squares = last * last
        for t in range(2 * out_cols // HEAD_SIZE):
            lanes = slice(t * HEAD_SIZE, (t + 1) * HEAD_SIZE)
            stats[0] += squares[:, lanes]
            stats[1] += weighted[:, lanes]

    def project_places(k, o):
        @pl.loop(0, 2)
        def _(i):
            place = z + (2 * i - 1) * k
            s = 2 * place + (y if o == 0 else 1 - y)

            @pl.when((place >= 0) & (place < line))
            def _():
                from_partner(1, s)
                project(s)

    def finish_places(k):
        @pl.loop(0, 2)
        def _(i):
            place = z + (2 * i - 1) * k

            @pl.when((place >= 0) & (place < line))
            def _():
                finish(place)

    for j in range(2):
        line_step(1, 1, 0, j)

    @pl.loop(0, 2)
    def _(i):
        @pl.when(i == 1)
        def _():
            from_partner(1, across)

        project(jnp.where(i == 0, f, across))

    for k in range(1, line):
        project_places(k, 0)
        for j in range(2):
            line_step(1, k, 1, j)
        project_places(k, 1)
        if k < line - 1:
            for j in range(2):
                line_step(1, k + 1, 0, j)
        if k == 1:

            @pl.loop(0, 1)
            def _(i):
                finish(z)

        else:
            finish_places(k - 1)
    finish_places(line - 1)

    mean = jnp.sum(stats[0], axis=-1, keepdims=True) / width
    score = jnp.sum(stats[1], axis=-1, keepdims=True) * lax.rsqrt(mean + 1e-06)
    first_row = lax.broadcasted_iota(jnp.int32, score_tile.shape, 0) == 0
    score_tile[...] = jnp.where(first_row, score, jnp.full(score_tile.shape, pair_weight[0]))
    score_all[me] = score_tile[...]

    def score_copy(i):
        other = lax.rem(me + i, everyone)
        return pltpu.make_async_remote_copy(
            src_ref=score_tile,
            dst_ref=score_all.at[me],
            send_sem=score_send.at[other],
            recv_sem=score_recv.at[me],
            device_id={"fsdp": other // groups, "dp": lax.rem(other, groups)},
        )

    @pl.loop(1, everyone)
    def _(i):
        score_copy(i).start()

    for m in range(2):
        for j in range(2):
            cross_copy(m, j).wait_send()

    @pl.loop(0, shards)
    def _(s):
        for way, ok in (
            (UP, has_up & (s // 2 <= z)),
            (DOWN, has_down & (s // 2 >= z)),
            (PARTNER, s != f),
        ):

            @pl.when(ok)
            def _():
                for m in range(2):
                    for j in range(2):
                        way_copy(way, m, s, j).wait_send()

        for way in range(3):
            part_copy(way, s).wait_send()

    for way in range(3):
        len_copy(way).wait_send()
        for half in range(2):
            tok_copy(way, half).wait_send()

    @pl.loop(1, everyone)
    def _(i):
        other = lax.rem(me + i, everyone)
        pltpu.make_async_copy(
            score_all.at[other], score_all.at[other], score_recv.at[other]
        ).wait()

    scores = score_all[:, 0, :]
    weights = score_all[:, 1, :]
    row = lax.broadcasted_iota(jnp.int32, scores.shape, 0)
    lane = lax.broadcasted_iota(jnp.int32, scores.shape, 1)
    partners = partner_rows[...]
    score_row = jnp.sum(jnp.where(row == lane, scores, 0.0), axis=0, keepdims=True)
    others = jnp.sum(jnp.where(partners == lane, score_row, 0.0), axis=1, keepdims=True)
    margins = jnp.where(row < partners, scores - others, others - scores)
    softplus = jnp.maximum(-margins, 0.0) + jnp.log1p(jnp.exp(-jnp.abs(margins)))
    first_lane = lane == 0
    margin = jnp.sum(jnp.where(first_lane & (row == me), margins, 0.0))
    loss = jnp.sum(jnp.where(first_lane, weights * softplus, 0.0)) / everyone
    margin_out[0] = margin
    loss_out[0] = loss

    @pl.loop(1, everyone)
    def _(i):
        score_copy(i).wait_send()


def layer_fits(shards, groups, tokens, qkv_weight, out_weight):
    return (
        shards % 2 == 0
        and shards >= 8
        and qkv_weight.shape[0] % 64 == 0
        and groups == 4
        and KEY_VALUE_HEADS % groups == 0
        and tokens.shape[1] == HEAD_SIZE
        and shards * groups <= HEAD_SIZE
        and out_weight.shape[1] % 64 == 0
    )


def layer(
    tokens,
    lengths,
    partner,
    pair_weight,
    norm_gain,
    qkv_weight,
    qkv_bias,
    out_weight,
    final_gain,
    value_head,
):
    shards, groups = lax.axis_size("fsdp"), lax.axis_size("dp")
    _, seq_rows, width = tokens.shape
    depth = qkv_weight.shape[0]
    out_cols = out_weight.shape[1]
    query_cols = QUERY_FEATURES // groups
    key_cols = KEY_FEATURES // groups
    all_cols = query_cols + 2 * key_cols
    rows = groups * seq_rows
    cosine, sine = rotary_tables(seq_rows)
    everyone = shards * groups
    dma = pltpu.SemaphoreType.DMA
    vmem = pl.BlockSpec(memory_space=pltpu.VMEM)
    scalar = pl.BlockSpec(memory_space=pltpu.SMEM)
    bf16, f32 = jnp.bfloat16, jnp.float32
    hidden, margin, loss = pl.pallas_call(
        functools.partial(layer_kernel, shards, groups),
        out_shape=(
            pltpu.VMEM((seq_rows, width), bf16),
            pltpu.SMEM((1,), f32),
            pltpu.SMEM((1,), f32),
        ),
        in_specs=[pl.BlockSpec(memory_space=pltpu.HBM)] * 12,
        out_specs=(vmem, scalar, scalar),
        scratch_shapes=[
            pltpu.VMEM((shards * depth, all_cols), bf16),
            pltpu.VMEM((shards, out_cols, query_cols), bf16),
            pltpu.VMEM((2, depth // 4, all_cols), bf16),
            pltpu.VMEM((2, out_cols // 4, query_cols), bf16),
            pltpu.VMEM((seq_rows, width), bf16),
            pltpu.VMEM((8, seq_rows), jnp.int32),
            pltpu.VMEM((groups, 8, seq_rows), jnp.int32),
            pltpu.VMEM((rows, width), bf16),
            pltpu.VMEM((rows, all_cols), f32),
            pltpu.VMEM((rows, query_cols), bf16),
            pltpu.VMEM((shards, seq_rows, out_cols), f32),
            pltpu.VMEM((shards, rows, out_cols), bf16),
            pltpu.VMEM((groups - 1, shards, seq_rows, out_cols), bf16),
            pltpu.VMEM((2, 8, HEAD_SIZE), f32),
            pltpu.VMEM((8, HEAD_SIZE), f32),
            pltpu.VMEM((everyone, 8, HEAD_SIZE), f32),
            pltpu.VMEM((everyone, HEAD_SIZE), jnp.int32),
            pltpu.VMEM((1, width), f32),
            pltpu.VMEM((1, width + 8 * HEAD_SIZE), f32),
            pltpu.VMEM((1, width + 8 * HEAD_SIZE), f32),
            pltpu.VMEM((1, qkv_bias.shape[0] + 8 * HEAD_SIZE), f32),
            pltpu.VMEM((seq_rows, HEAD_SIZE), f32),
            pltpu.VMEM((seq_rows, HEAD_SIZE), f32),
            pltpu.SMEM((1,), jnp.int32),
            pltpu.SMEM((1,), f32),
            pltpu.SMEM((everyone,), jnp.int32),
            dma((31,)),
            dma((2, shards, 4)),
            dma((3, 2, shards, 2)),
            dma((2, 2)),
            dma((3, 2)),
            dma((3, 2)),
            dma((3,)),
            dma((3,)),
            dma((3, shards)),
            dma((3, shards)),
            dma((everyone,)),
            dma((everyone,)),
        ],
        compiler_params=pltpu.CompilerParams(
            collective_id=0, has_side_effects=True, vmem_limit_bytes=56 * 1024 * 1024
        ),
    )(
        tokens[0],
        qkv_weight,
        out_weight.T,
        lengths,
        pair_weight,
        partner,
        norm_gain,
        final_gain,
        value_head,
        qkv_bias,
        jnp.asarray(cosine),
        jnp.asarray(sine),
    )
    return hidden[None], margin, loss.reshape(())


def projected_by_gathers(
    tokens,
    lengths,
    norm_gain,
    qkv_weight,
    qkv_bias,
    out_weight,
):
    sequence = tokens[0]
    length_rows = sequence.shape[0]
    width = sequence.shape[1]
    normed = rms_scale(sequence.astype(jnp.float32), norm_gain).astype(jnp.bfloat16)
    query_group_count = lax.axis_size("dp")
    group_index = lax.axis_index("dp")
    query_heads = QUERY_HEADS // query_group_count
    key_value_heads = KEY_VALUE_HEADS // query_group_count
    query_cols = query_heads * HEAD_SIZE
    key_cols = key_value_heads * HEAD_SIZE
    group_normed, group_lengths = (
        lax.all_gather(normed[None], "dp", axis=0, tiled=True),
        lax.all_gather(lengths, "dp", axis=0, tiled=True),
    )
    seq_count = group_normed.shape[0]
    flat = group_normed.reshape(seq_count * length_rows, width)
    qkv_cols = jnp.concatenate(
        [
            lax.dynamic_slice_in_dim(qkv_weight, group_index * query_cols, query_cols, 1),
            lax.dynamic_slice_in_dim(
                qkv_weight, QUERY_FEATURES + group_index * key_cols, key_cols, 1
            ),
            lax.dynamic_slice_in_dim(
                qkv_weight, QUERY_FEATURES + KEY_FEATURES + group_index * key_cols, key_cols, 1
            ),
        ],
        axis=1,
    )
    bias_cols = jnp.concatenate(
        [
            lax.dynamic_slice_in_dim(qkv_bias, group_index * query_cols, query_cols, 0),
            lax.dynamic_slice_in_dim(
                qkv_bias, QUERY_FEATURES + group_index * key_cols, key_cols, 0
            ),
            lax.dynamic_slice_in_dim(
                qkv_bias, QUERY_FEATURES + KEY_FEATURES + group_index * key_cols, key_cols, 0
            ),
        ],
        axis=0,
    )
    out_rows = lax.dynamic_slice_in_dim(out_weight, group_index * query_cols, query_cols, 0)
    qkv_full, out_full = (
        lax.all_gather(qkv_cols, "fsdp", axis=0, tiled=True),
        lax.all_gather(out_rows, "fsdp", axis=1, tiled=True),
    )
    query_key_value = jnp.dot(flat, qkv_full, preferred_element_type=jnp.float32) + bias_cols
    attn = attend(
        query_key_value.reshape(seq_count, length_rows, -1),
        group_lengths,
        query_heads,
        key_value_heads,
    )
    return lax.psum_scatter(
        jnp.dot(attn, out_full, preferred_element_type=jnp.float32),
        "dp",
        scatter_dimension=0,
        tiled=True,
    )


def per_device(
    tokens,
    lengths,
    partner,
    pair_weight,
    norm_gain,
    qkv_weight,
    qkv_bias,
    out_weight,
    final_gain,
    value_head,
):
    if layer_fits(lax.axis_size("fsdp"), lax.axis_size("dp"), tokens, qkv_weight, out_weight):
        return layer(
            tokens,
            lengths,
            partner,
            pair_weight,
            norm_gain,
            qkv_weight,
            qkv_bias,
            out_weight,
            final_gain,
            value_head,
        )
    sequence = tokens[0]
    length = lengths[0]
    projected = projected_by_gathers(tokens, lengths, norm_gain, qkv_weight, qkv_bias, out_weight)
    hidden = (sequence.astype(jnp.float32) + projected).astype(jnp.bfloat16)
    last = lax.dynamic_slice_in_dim(hidden, length - 1, 1, 0)[0].astype(jnp.float32)
    score = jnp.sum(rms_scale(last, final_gain) * value_head)
    everyone, weights_all = (
        lax.all_gather(score.reshape(1), ("fsdp", "dp"), axis=0, tiled=True),
        lax.all_gather(pair_weight, ("fsdp", "dp"), axis=0, tiled=True),
    )
    total_seqs = everyone.shape[0]
    mine = lax.axis_index(("fsdp", "dp"))
    index_all = jnp.arange(total_seqs, dtype=jnp.int32)
    my_partner = jnp.sum(jnp.where(index_all == mine, partner, 0))
    other = jnp.sum(jnp.where(index_all == my_partner, everyone, jnp.float32(0.0)))
    margin = jnp.where(mine < my_partner, score - other, other - score)
    matches = partner[:, None] == index_all[None, :]
    others_all = jnp.sum(jnp.where(matches, everyone[None, :], jnp.float32(0.0)), axis=1)
    margins_all = jnp.where(index_all < partner, everyone - others_all, others_all - everyone)
    loss = jnp.sum(weights_all * jax.nn.softplus(-margins_all)) / total_seqs
    return (hidden[None], margin.reshape(1), loss)


def solution(mesh):
    return jax.shard_map(
        per_device,
        mesh=mesh,
        in_specs=(
            P(("fsdp", "dp"), None, None),
            P(("fsdp", "dp")),
            P(),
            P(("fsdp", "dp")),
            P(),
            P("fsdp", None),
            P(),
            P(None, "fsdp"),
            P(),
            P(),
        ),
        out_specs=(P(("fsdp", "dp"), None, None), P(("fsdp", "dp")), P()),
        check_vma=False,
    )
```

```python
import functools

import jax
import jax.numpy as jnp
import numpy as np
from jax import lax
from jax.experimental import pallas as pl
from jax.experimental.pallas import tpu as pltpu
from jax.sharding import PartitionSpec as P

QUERY_HEADS = 28
KEY_VALUE_HEADS = 4
HEAD_SIZE = 128
QUERY_FEATURES = 3584
KEY_FEATURES = 512


def rms_scale(value_rows, gain):
    return (
        value_rows
        * lax.rsqrt(jnp.mean(value_rows * value_rows, axis=-1, keepdims=True) + 1e-06)
        * gain
    )


def apply_rotary(heads, length_rows):
    half = HEAD_SIZE // 2
    positions = jnp.arange(length_rows, dtype=jnp.float32)
    freqs = jnp.exp(
        -(2.0 * jnp.arange(half, dtype=jnp.float32) / HEAD_SIZE) * jnp.log(jnp.float32(1000000.0))
    )
    angles = positions[:, None] * freqs[None, :]
    cosine = jnp.cos(angles)
    sine = jnp.sin(angles)
    first = heads[..., :half]
    second = heads[..., half:]
    return jnp.concatenate(
        [first * cosine - second * sine, second * cosine + first * sine], axis=-1
    )


def attend(query_key_value, group_lengths, query_heads, key_value_heads):
    seq_count, length_rows, _ = query_key_value.shape
    query_width = query_heads * HEAD_SIZE
    key_width = key_value_heads * HEAD_SIZE
    query_rows = (
        query_key_value[..., :query_width]
        .reshape(seq_count, length_rows, query_heads, HEAD_SIZE)
        .transpose(0, 2, 1, 3)
    )
    key_rows = (
        query_key_value[..., query_width : query_width + key_width]
        .reshape(seq_count, length_rows, key_value_heads, HEAD_SIZE)
        .transpose(0, 2, 1, 3)
    )
    value_rows = (
        query_key_value[..., query_width + key_width :]
        .reshape(seq_count, length_rows, key_value_heads, HEAD_SIZE)
        .transpose(0, 2, 1, 3)
        .astype(jnp.bfloat16)
    )
    query_rows = (
        apply_rotary(query_rows, length_rows)
        .astype(jnp.bfloat16)
        .reshape(seq_count, key_value_heads, query_heads // key_value_heads, length_rows, HEAD_SIZE)
    )
    key_rows = apply_rotary(key_rows, length_rows).astype(jnp.bfloat16)
    scores = jnp.einsum(
        "bgqtd,bgsd->bgqts", query_rows, key_rows, preferred_element_type=jnp.float32
    ) / jnp.sqrt(jnp.float32(HEAD_SIZE))
    places = jnp.arange(length_rows, dtype=jnp.int32)
    causal = places[None, :] <= places[:, None]
    usable = places[None, :] < group_lengths[:, None]
    allowed = causal[None, :, :] & usable[:, None, :]
    scores = jnp.where(allowed[:, None, None, :, :], scores, jnp.float32(-1e30))
    highest = jnp.max(scores, axis=-1, keepdims=True)
    expd = jnp.exp(scores - highest)
    probs = (expd / jnp.sum(expd, axis=-1, keepdims=True)).astype(jnp.bfloat16)
    mixed = jnp.einsum("bgqts,bgsd->bgqtd", probs, value_rows, preferred_element_type=jnp.float32)
    mixed = mixed.reshape(seq_count, query_heads, length_rows, HEAD_SIZE).transpose(0, 2, 1, 3)
    return mixed.reshape(seq_count * length_rows, query_width).astype(jnp.bfloat16)


UP, DOWN, PARTNER = 0, 1, 2


def rotary_tables(length_rows):
    half = HEAD_SIZE // 2
    freqs = 1000000.0 ** (-2.0 * np.arange(half) / HEAD_SIZE)
    angles = np.arange(length_rows)[:, None] * freqs[None, :]
    cosine, sine = np.cos(angles), np.sin(angles)
    return (
        np.concatenate([cosine, cosine], axis=1).astype(np.float32),
        np.concatenate([-sine, sine], axis=1).astype(np.float32),
    )


def out_pieces(out_cols):
    big = (out_cols // 2 + HEAD_SIZE - 1) // HEAD_SIZE * HEAD_SIZE
    return big, out_cols - big


def layer_kernel(
    shards,
    groups,
    tokens,
    qkv_weight,
    out_weight,
    length_one,
    pair_weight_one,
    partner_all,
    norm_gain_flat,
    final_gain_flat,
    value_head_flat,
    qkv_bias_flat,
    cosine_table,
    sine_table,
    hidden,
    margin_out,
    loss_out,
    qkv_full,
    out_full,
    cross_qkv,
    cross_out,
    tok_own,
    len_tile,
    len_all,
    normed,
    qkv_rows,
    attn,
    own,
    part_out,
    part_in,
    attn_help,
    help_own,
    help_out,
    help_in,
    help_sum,
    help_done,
    stats,
    score_tile,
    score_all,
    partner_rows,
    norm_gain,
    final_gain,
    value_head,
    qkv_bias,
    cosine,
    sine,
    length,
    pair_weight,
    partner,
    local_sem,
    recv_sem,
    send_sem,
    cross_send,
    tok_send,
    tok_recv,
    len_send,
    len_recv,
    part_send,
    part_recv,
    attn_send,
    attn_recv,
    help_send,
    help_recv,
    done_sem,
    score_send,
    score_recv,
):
    line = shards // 2
    f = lax.axis_index("fsdp")
    g = lax.axis_index("dp")
    z = f // 2
    y = f % 2
    x = g // 2
    core = g % 2
    seq_rows = tokens.shape[0]
    width = tokens.shape[1]
    depth = qkv_weight.shape[0]
    out_cols = out_weight.shape[0]
    query_cols = QUERY_FEATURES // groups
    key_cols = KEY_FEATURES // groups
    heads = query_cols // HEAD_SIZE
    quarter = depth // 4
    pair = 2 * out_cols
    big, small = out_pieces(out_cols)
    is_end = (z == 0) | (z == line - 1)
    is_helper = (z == 1) | (z == line - 2)
    far = jnp.where((z == 0) | (z == 1), line - 1, 0)
    end_to_helper = {"fsdp": jnp.where(z == 0, f + 2, f - 2)}
    helper_to_end = {"fsdp": jnp.where(z == 1, f - 2, f + 2)}
    has_up = z < line - 1
    has_down = z > 0
    team = 2 * x + y
    across_team = 2 * x + 1 - y
    across = 2 * z + 1 - y
    x_peer = 2 * (1 - x) + core
    team_ids = ({"dp": x_peer}, {"fsdp": across}, {"fsdp": across, "dp": x_peer})
    way_ids = ({"fsdp": f + 2}, {"fsdp": f - 2}, {"dp": 2 * x + 1 - core})

    barrier = pltpu.get_barrier_semaphore()
    for target in (*team_ids, way_ids[PARTNER]):
        pl.semaphore_signal(barrier, inc=1, device_id=target)
    for way, ok in ((UP, has_up), (DOWN, has_down)):

        @pl.when(ok)
        def _():
            pl.semaphore_signal(barrier, inc=1, device_id=way_ids[way])

    def out_rows(side, piece, half):
        size = (big, small)[piece] // 2
        start = (side * small, (1 - side) * big)[piece]
        return start + half * size, size

    def slot(m, s, piece, half):
        if m == 0:
            start = s * depth + (2 * piece + half) * quarter
            return qkv_full.at[pl.ds(pl.multiple_of(start, 16), quarter)]
        start, size = out_rows(lax.rem(s, 2), piece, half)
        return out_full.at[pl.ds(pl.multiple_of(s * out_cols + start, 16), size)]

    count = 0

    def local(source, dest):
        nonlocal count
        copy = pltpu.make_async_copy(source, dest, local_sem.at[count])
        count += 1
        copy.start()
        return copy

    def qkv_parts(piece, half, owner, dest):
        rows = pl.ds(pl.multiple_of((2 * piece + half) * quarter, 16), quarter)
        return [
            local(
                qkv_weight.at[rows, pl.ds(pl.multiple_of(start, 128), size)],
                dest.at[:, pl.ds(to, size)],
            )
            for start, size, to in (
                (owner * query_cols, query_cols, 0),
                (QUERY_FEATURES + owner * key_cols, key_cols, query_cols),
                (QUERY_FEATURES + KEY_FEATURES + owner * key_cols, key_cols, query_cols + key_cols),
            )
        ]

    length_load = local(length_one, length)
    own_loads, cross_loads = [], []
    for j in range(2):
        own_loads.append(qkv_parts(j, core, team, slot(0, f, j, core)))
        cross_loads.append(qkv_parts(j, core, across_team, cross_qkv.at[j]))
    tok_local = local(tokens, tok_own)
    vectors = [
        local(flat, row.at[0, pl.ds(0, flat.shape[0])])
        for flat, row in (
            (norm_gain_flat, norm_gain),
            (final_gain_flat, final_gain),
            (value_head_flat, value_head),
            (qkv_bias_flat, qkv_bias),
        )
    ]
    late_loads = []
    for j in range(2):
        late_loads.extend(qkv_parts(j, 1 - core, team, slot(0, f, j, 1 - core)))
    out_own = local(
        out_weight.at[:, pl.ds(pl.multiple_of(team * query_cols, 128), query_cols)],
        out_full.at[pl.ds(pl.multiple_of(f * out_cols, 16), out_cols)],
    )

    def cross_part(m, j):
        if m == 0:
            return cross_qkv.at[j]
        return cross_out.at[j, pl.ds(0, (small, big)[j] // 2)]

    out_cross = []
    for j in range(2):
        start, size = out_rows(y, 1 - j, core)
        out_cross.append(
            local(
                out_weight.at[
                    pl.ds(pl.multiple_of(start, 16), size),
                    pl.ds(pl.multiple_of(across_team * query_cols, 128), query_cols),
                ],
                cross_part(1, j),
            )
        )
    small_loads = [
        local(source, dest)
        for source, dest in (
            (pair_weight_one, pair_weight),
            (partner_all, partner),
            (cosine_table, cosine),
            (sine_table, sine),
        )
    ]
    everyone = shards * groups
    me = f * groups + g

    pl.semaphore_wait(barrier, 4 + has_up.astype(jnp.int32) + has_down.astype(jnp.int32))

    def way_copy(way, m, s, piece):
        return pltpu.make_async_remote_copy(
            src_ref=slot(m, s, piece, core),
            dst_ref=slot(m, s, piece, core),
            send_sem=send_sem.at[way, m, s, piece],
            recv_sem=recv_sem.at[m, s, piece, core],
            device_id=way_ids[way],
        )

    def piece_of(m, o, j):
        return 1 - j if m == 1 and o == 1 else j

    def cross_copy(m, j):
        piece = piece_of(m, 1, j)
        return pltpu.make_async_remote_copy(
            src_ref=cross_part(m, j),
            dst_ref=slot(m, f, piece, core),
            send_sem=cross_send.at[m, j],
            recv_sem=recv_sem.at[m, f, piece, core],
            device_id=team_ids[1],
        )

    def arrived(m, s, piece, half):
        there = slot(m, s, piece, half)
        pltpu.make_async_copy(there, there, recv_sem.at[m, s, piece, half]).wait()

    def send_both(m, s, piece):
        pl.when(has_up)(way_copy(UP, m, s, piece).start)
        pl.when(has_down)(way_copy(DOWN, m, s, piece).start)

    def cross_step(m, j):
        piece = piece_of(m, 1, j)
        arrived(m, across, piece, core)
        send_both(m, across, piece)
        way_copy(PARTNER, m, across, piece).start()

    def sides(k, o):
        row = y if o == 0 else 1 - y
        below, above = z - k, z + k
        return (
            (below >= 0, 2 * jnp.maximum(below, 0) + row, UP, has_up),
            (above < line, 2 * jnp.minimum(above, line - 1) + row, DOWN, has_down),
        )

    def line_step(m, k, o, j):
        piece = piece_of(m, o, j)
        for ok, s, way, onward in sides(k, o):
            if m == 1:
                onward = onward & (k < line - 2)

            @pl.when(ok)
            def _():
                arrived(m, s, piece, core)
                pl.when(onward)(way_copy(way, m, s, piece).start)
                way_copy(PARTNER, m, s, piece).start()

    def from_partner(m, s):
        for piece in range(2):
            arrived(m, s, piece, 1 - core)

    half_rows = seq_rows // 2

    def tok_copy(way, half):
        source = (0, 0, 1 + half)[way]
        target = team_ids[way] if way < 2 else team_ids[1 - half]
        return pltpu.make_async_remote_copy(
            src_ref=normed.at[pl.ds(source * seq_rows + half * half_rows, half_rows)],
            dst_ref=normed.at[pl.ds((1 + way) * seq_rows + half * half_rows, half_rows)],
            send_sem=tok_send.at[way, half],
            recv_sem=tok_recv.at[way, half],
            device_id=target,
        )

    def len_copy(way):
        return pltpu.make_async_remote_copy(
            src_ref=len_tile,
            dst_ref=len_all.at[1 + way],
            send_sem=len_send.at[way],
            recv_sem=len_recv.at[way],
            device_id=team_ids[way],
        )

    for j in range(2):
        for copy in own_loads[j]:
            copy.wait()
        send_both(0, f, j)
        for copy in cross_loads[j]:
            copy.wait()
        cross_copy(0, j).start()

    tok_local.wait()
    for copy in vectors:
        copy.wait()
    norm_rows = 16

    @pl.loop(0, seq_rows // norm_rows)
    def _(i):
        at = pl.ds(pl.multiple_of(i * norm_rows, norm_rows), norm_rows)
        rows = tok_own[at, :].astype(jnp.float32)
        scale = lax.rsqrt(jnp.mean(rows * rows, axis=-1, keepdims=True) + 1e-06)
        normed[at, :] = (rows * scale * norm_gain[...]).astype(jnp.bfloat16)

    tok_copy(0, 0).start()
    tok_copy(1, 1).start()
    tok_copy(0, 1).start()
    tok_copy(1, 0).start()
    length_load.wait()
    len_tile[...] = jnp.full(len_tile.shape, length[0], jnp.int32)
    len_all[0] = len_tile[...]
    for way in range(3):
        len_copy(way).start()

    bias_parts = (
        (team * query_cols, query_cols, 0),
        (QUERY_FEATURES + team * key_cols, key_cols, query_cols),
        (QUERY_FEATURES + KEY_FEATURES + team * key_cols, key_cols, query_cols + key_cols),
    )
    for start, size, to in bias_parts:
        qkv_rows[:, to : to + size] = jnp.broadcast_to(
            qkv_bias[:, pl.ds(pl.multiple_of(start, HEAD_SIZE), size)],
            (groups * seq_rows, size),
        )

    for j in range(2):
        cross_step(0, j)
        line_step(0, 1, 0, j)
    tok_copy(0, 0).wait_recv()
    tok_copy(2, 0).start()
    line_step(0, 1, 1, 0)
    line_step(0, 1, 1, 1)
    tok_copy(1, 1).wait_recv()
    tok_copy(2, 1).start()
    out_own.wait()
    for j in range(2):
        out_cross[j].wait()
        cross_copy(1, j).start()
    for k in range(2, line - 1):
        for o in range(2):
            for j in range(2):
                line_step(0, k, o, j)
    for j in range(2):
        send_both(1, f, j)

    tok_copy(0, 1).wait_recv()
    tok_copy(1, 0).wait_recv()
    tok_copy(2, 0).wait_recv()
    tok_copy(2, 1).wait_recv()
    for way in range(3):
        len_copy(way).wait_recv()
    for copy in (*late_loads, *small_loads):
        copy.wait()

    @pl.loop(0, everyone)
    def _(i):
        partner_rows[pl.ds(i, 1), :] = jnp.full((1, HEAD_SIZE), partner[i], jnp.int32)

    tile = 3 * HEAD_SIZE

    def qkv_step(place):
        rows = pl.ds(pl.multiple_of(place * 2 * depth, 128), 2 * depth)

        @pl.loop(0, (query_cols + 2 * key_cols) // tile)
        def _(t):
            cols = pl.ds(pl.multiple_of(t * tile, tile), tile)
            qkv_rows[:, cols] += jnp.dot(
                normed[:, rows], qkv_full[rows, cols], preferred_element_type=jnp.float32
            )

    def qkv_places(first, last):
        @pl.loop(2 * first, 2 * last)
        def _(i):
            k = i // 2
            place = z + (2 * lax.rem(i, 2) - 1) * k

            @pl.when((place >= 0) & (place < line))
            def _():
                from_partner(0, 2 * place)
                from_partner(0, 2 * place + 1)
                qkv_step(place)

    @pl.loop(0, 1)
    def _(i):
        from_partner(0, across)
        qkv_step(z)

    qkv_places(1, line - 1)
    for j in range(2):
        cross_step(1, j)
    for o in range(2):
        for j in range(2):
            line_step(0, line - 1, o, j)
    qkv_places(line - 1, line)

    def head_rows(j, column):
        return qkv_rows[
            pl.ds(pl.multiple_of(j * seq_rows, seq_rows), seq_rows), column : column + HEAD_SIZE
        ]

    def rotate(rows):
        return (
            rows * cosine[...] + pltpu.roll(rows, HEAD_SIZE // 2, 1) * sine[...]
        ).astype(jnp.bfloat16)

    key_heads = key_cols // HEAD_SIZE
    share = heads // key_heads

    def attn_copy(j):
        rows = pl.ds(pl.multiple_of(j * seq_rows, seq_rows), seq_rows)
        return pltpu.make_async_remote_copy(
            src_ref=attn.at[rows],
            dst_ref=attn_help.at[rows],
            send_sem=attn_send.at[j],
            recv_sem=attn_recv.at[j],
            device_id=end_to_helper,
        )

    @pl.loop(0, groups)
    def _(i):
        j = groups - 1 - i
        query_place = lax.broadcasted_iota(jnp.int32, (seq_rows, seq_rows), 0)
        key_place = lax.broadcasted_iota(jnp.int32, (seq_rows, seq_rows), 1)
        allowed = (key_place <= query_place) & (key_place < len_all[j, 0:1, :])
        at = pl.ds(pl.multiple_of(j * seq_rows, seq_rows), seq_rows)
        for kh in range(key_heads):
            offset = kh * HEAD_SIZE
            key = rotate(head_rows(j, query_cols + offset))
            value = head_rows(j, query_cols + key_cols + offset).astype(jnp.bfloat16)
            for h in range(kh * share, (kh + 1) * share):
                query = rotate(head_rows(j, h * HEAD_SIZE))
                scores = lax.dot_general(
                    query, key, (((1,), (1,)), ((), ())), preferred_element_type=jnp.float32
                ) / np.float32(np.sqrt(HEAD_SIZE))
                scores = jnp.where(allowed, scores, jnp.float32(-1e30))
                expd = jnp.exp(scores - jnp.max(scores, axis=-1, keepdims=True))
                probs = (expd / jnp.sum(expd, axis=-1, keepdims=True)).astype(jnp.bfloat16)
                attn[at, h * HEAD_SIZE : (h + 1) * HEAD_SIZE] = jnp.dot(
                    probs, value, preferred_element_type=jnp.float32
                ).astype(jnp.bfloat16)
        pl.when(is_end)(attn_copy(j).start)

    def lanes_of(at, size):
        return pl.ds(pl.multiple_of(at, HEAD_SIZE), size)

    units = ((0, big), (big, 2 * small), (pair - big, big))

    def part_copy(way, place, at, size, unit):
        cols = lanes_of(at, size)
        return pltpu.make_async_remote_copy(
            src_ref=part_out.at[place, pl.ds((1 + way) * seq_rows, seq_rows), cols],
            dst_ref=part_in.at[way, place, :, cols],
            send_sem=part_send.at[way, place, unit],
            recv_sem=part_recv.at[way, place, unit],
            device_id=team_ids[way],
        )

    def project(place, at, size, unit):
        cols = lanes_of(at, size)
        result = lax.dot_general(
            attn[...],
            out_full[lanes_of(place * pair + at, size), :],
            (((1,), (1,)), ((), ())),
            preferred_element_type=jnp.float32,
        )
        part_out[place, :, cols] = result.astype(jnp.bfloat16)
        own[place, :, cols] = result[:seq_rows]
        for way in (2, 0, 1):
            part_copy(way, place, at, size, unit).start()

    def project_pair(place):
        @pl.loop(0, 2)
        def _(i):
            project(place, i * (pair - big), big, 2 * i)

        project(place, big, 2 * small, 1)

    place = lax.broadcasted_iota(jnp.int32, len_tile.shape, 1)
    pick = (place == len_tile[...] - 1).astype(jnp.bfloat16)
    stats[...] = jnp.zeros_like(stats)

    def finish(place, sums):
        cols = lanes_of(place * pair, pair)
        hidden[:, cols] = (tok_own[:, cols].astype(jnp.float32) + sums).astype(jnp.bfloat16)
        last = jnp.dot(pick, hidden[:, cols], preferred_element_type=jnp.float32)
        weighted = last * final_gain[:, cols] * value_head[:, cols]
        squares = last * last
        for t in range(pair // HEAD_SIZE):
            lanes = slice(t * HEAD_SIZE, (t + 1) * HEAD_SIZE)
            stats[0] += squares[:, lanes]
            stats[1] += weighted[:, lanes]

    def finish_parts(place):
        for unit, (at, size) in enumerate(units):
            for way in range(3):
                part_copy(way, place, at, size, unit).wait_recv()
        total = own[place]
        for way in range(3):
            total += part_in[way, place].astype(jnp.float32)
        finish(place, total)

    def at_sides(k, body):
        @pl.loop(0, 2)
        def _(i):
            place = z + (2 * i - 1) * k

            @pl.when((place >= 0) & (place < line) & ((k > 0) | (i == 0)))
            def _():
                body(place)

    def own_unit(place):
        arrived(1, 2 * place + y, 0, 1 - core)
        project(place, y * (pair - big), big, 2 * y)

    def mid_unit(place):
        arrived(1, 2 * place + y, 1, 1 - core)
        arrived(1, 2 * place + 1 - y, 1, 1 - core)
        project(place, big, 2 * small, 1)

    def cross_unit(place):
        arrived(1, 2 * place + 1 - y, 0, 1 - core)
        project(place, (1 - y) * (pair - big), big, 2 * (1 - y))

    from_partner(1, across)
    project_pair(z)

    @pl.loop(1, line - 1)
    def _(k):
        mine = jnp.logical_not(is_helper) | (k < line - 2)
        line_step(1, k, 0, 0)
        line_step(1, k, 0, 1)

        @pl.when(mine)
        def _():
            at_sides(k, own_unit)

        @pl.when(jnp.logical_not(is_helper))
        def _():
            at_sides(k - 1, finish_parts)

        line_step(1, k, 1, 0)

        @pl.when(mine)
        def _():
            at_sides(k, mid_unit)

        line_step(1, k, 1, 1)

        @pl.when(mine)
        def _():
            at_sides(k, cross_unit)

    def help_part(way):
        return pltpu.make_async_remote_copy(
            src_ref=help_out.at[1 + way],
            dst_ref=help_in.at[way],
            send_sem=help_send.at[way],
            recv_sem=help_recv.at[way],
            device_id=team_ids[way],
        )

    done_copy = pltpu.make_async_remote_copy(
        src_ref=help_sum,
        dst_ref=help_done,
        send_sem=done_sem.at[0],
        recv_sem=done_sem.at[1],
        device_id=helper_to_end,
    )

    @pl.when(is_helper)
    def _():
        for o in range(2):
            from_partner(1, 2 * far + o)

        @pl.loop(0, groups)
        def _(i):
            j = groups - 1 - i
            rows = pl.ds(pl.multiple_of(j * seq_rows, seq_rows), seq_rows)
            pltpu.make_async_copy(attn_help.at[rows], attn_help.at[rows], attn_recv.at[j]).wait()
            result = lax.dot_general(
                attn_help[rows, :],
                out_full[lanes_of(far * pair, pair), :],
                (((1,), (1,)), ((), ())),
                preferred_element_type=jnp.float32,
            )
            help_own[...] = result
            help_out[j] = result.astype(jnp.bfloat16)
            for way in range(3):
                pl.when(j == way + 1)(help_part(way).start)

        project_pair(far)

        @pl.loop(0, line)
        def _(place):
            pl.when(place != far)(lambda: finish_parts(place))

        for way in range(3):
            help_part(way).wait_recv()
        total = help_own[...]
        for way in range(3):
            total += help_in[way].astype(jnp.float32)
        help_sum[...] = total.astype(jnp.bfloat16)
        done_copy.start()

    @pl.when(is_end)
    def _():
        at_sides(line - 2, finish_parts)
        done_copy.wait_recv()
        finish(far, help_done[...].astype(jnp.float32))

    @pl.when(is_helper)
    def _():
        finish_parts(far)

    mean = jnp.sum(stats[0], axis=-1, keepdims=True) / width
    score = jnp.sum(stats[1], axis=-1, keepdims=True) * lax.rsqrt(mean + 1e-06)
    first_row = lax.broadcasted_iota(jnp.int32, score_tile.shape, 0) == 0
    score_tile[...] = jnp.where(first_row, score, jnp.full(score_tile.shape, pair_weight[0]))
    score_all[me] = score_tile[...]

    def score_copy(i):
        other = lax.rem(me + i, everyone)
        return pltpu.make_async_remote_copy(
            src_ref=score_tile,
            dst_ref=score_all.at[me],
            send_sem=score_send.at[other],
            recv_sem=score_recv.at[me],
            device_id={"fsdp": other // groups, "dp": lax.rem(other, groups)},
        )

    @pl.loop(1, everyone)
    def _(i):
        score_copy(i).start()

    for m in range(2):
        for j in range(2):
            cross_copy(m, j).wait_send()

    @pl.loop(0, shards)
    def _(s):
        place = s // 2
        skipped = (place == far) & is_end
        for way, ok, ok_out in (
            (UP, has_up & (place <= z), (place > 0) | (z < line - 2)),
            (DOWN, has_down & (place >= z), (place < line - 1) | (z > 1)),
            (PARTNER, s != f, jnp.logical_not(skipped)),
        ):
            for m in range(2):

                @pl.when(ok & ok_out if m == 1 else ok)
                def _():
                    for piece in range(2):
                        way_copy(way, m, s, piece).wait_send()

    @pl.loop(0, line)
    def _(place):
        @pl.when(jnp.logical_not(is_end & (place == far)))
        def _():
            for unit, (at, size) in enumerate(units):
                for way in range(3):
                    part_copy(way, place, at, size, unit).wait_send()

    @pl.when(is_helper)
    def _():
        for way in range(3):
            help_part(way).wait_send()
        done_copy.wait_send()

    @pl.when(is_end)
    def _():
        @pl.loop(0, groups)
        def _(j):
            attn_copy(j).wait_send()

    for way in range(3):
        len_copy(way).wait_send()
        for half in range(2):
            tok_copy(way, half).wait_send()

    @pl.loop(1, everyone)
    def _(i):
        other = lax.rem(me + i, everyone)
        pltpu.make_async_copy(
            score_all.at[other], score_all.at[other], score_recv.at[other]
        ).wait()

    scores = score_all[:, 0, :]
    weights = score_all[:, 1, :]
    row = lax.broadcasted_iota(jnp.int32, scores.shape, 0)
    lane = lax.broadcasted_iota(jnp.int32, scores.shape, 1)
    partners = partner_rows[...]
    score_row = jnp.sum(jnp.where(row == lane, scores, 0.0), axis=0, keepdims=True)
    others = jnp.sum(jnp.where(partners == lane, score_row, 0.0), axis=1, keepdims=True)
    margins = jnp.where(row < partners, scores - others, others - scores)
    softplus = jnp.maximum(-margins, 0.0) + jnp.log1p(jnp.exp(-jnp.abs(margins)))
    first_lane = lane == 0
    margin = jnp.sum(jnp.where(first_lane & (row == me), margins, 0.0))
    loss = jnp.sum(jnp.where(first_lane, weights * softplus, 0.0)) / everyone
    margin_out[0] = margin
    loss_out[0] = loss

    @pl.loop(1, everyone)
    def _(i):
        score_copy(i).wait_send()


def layer_fits(shards, groups, tokens, qkv_weight, out_weight):
    return (
        shards % 2 == 0
        and shards >= 8
        and qkv_weight.shape[0] % 64 == 0
        and groups == 4
        and KEY_VALUE_HEADS % groups == 0
        and tokens.shape[1] == HEAD_SIZE
        and shards * groups <= HEAD_SIZE
        and out_weight.shape[1] % 64 == 0
        and out_weight.shape[1] > HEAD_SIZE
    )


def layer(
    tokens,
    lengths,
    partner,
    pair_weight,
    norm_gain,
    qkv_weight,
    qkv_bias,
    out_weight,
    final_gain,
    value_head,
):
    shards, groups = lax.axis_size("fsdp"), lax.axis_size("dp")
    _, seq_rows, width = tokens.shape
    depth = qkv_weight.shape[0]
    out_cols = out_weight.shape[1]
    query_cols = QUERY_FEATURES // groups
    key_cols = KEY_FEATURES // groups
    all_cols = query_cols + 2 * key_cols
    rows = groups * seq_rows
    line, pair = shards // 2, 2 * out_cols
    cosine, sine = rotary_tables(seq_rows)
    everyone = shards * groups
    dma = pltpu.SemaphoreType.DMA
    vmem = pl.BlockSpec(memory_space=pltpu.VMEM)
    scalar = pl.BlockSpec(memory_space=pltpu.SMEM)
    bf16, f32 = jnp.bfloat16, jnp.float32
    hidden, margin, loss = pl.pallas_call(
        functools.partial(layer_kernel, shards, groups),
        out_shape=(
            pltpu.VMEM((seq_rows, width), bf16),
            pltpu.SMEM((1,), f32),
            pltpu.SMEM((1,), f32),
        ),
        in_specs=[pl.BlockSpec(memory_space=pltpu.HBM)] * 12,
        out_specs=(vmem, scalar, scalar),
        scratch_shapes=[
            pltpu.VMEM((shards * depth, all_cols), bf16),
            pltpu.VMEM((shards * out_cols, query_cols), bf16),
            pltpu.VMEM((2, depth // 4, all_cols), bf16),
            pltpu.VMEM((2, out_pieces(out_cols)[0] // 2, query_cols), bf16),
            pltpu.VMEM((seq_rows, width), bf16),
            pltpu.VMEM((8, seq_rows), jnp.int32),
            pltpu.VMEM((groups, 8, seq_rows), jnp.int32),
            pltpu.VMEM((rows, width), bf16),
            pltpu.VMEM((rows, all_cols), f32),
            pltpu.VMEM((rows, query_cols), bf16),
            pltpu.VMEM((line, seq_rows, pair), f32),
            pltpu.VMEM((line, rows, pair), bf16),
            pltpu.VMEM((groups - 1, line, seq_rows, pair), bf16),
            pltpu.VMEM((rows, query_cols), bf16),
            pltpu.VMEM((seq_rows, pair), f32),
            pltpu.VMEM((groups, seq_rows, pair), bf16),
            pltpu.VMEM((groups - 1, seq_rows, pair), bf16),
            pltpu.VMEM((seq_rows, pair), bf16),
            pltpu.VMEM((seq_rows, pair), bf16),
            pltpu.VMEM((2, 8, HEAD_SIZE), f32),
            pltpu.VMEM((8, HEAD_SIZE), f32),
            pltpu.VMEM((everyone, 8, HEAD_SIZE), f32),
            pltpu.VMEM((everyone, HEAD_SIZE), jnp.int32),
            pltpu.VMEM((1, width), f32),
            pltpu.VMEM((1, width + 8 * HEAD_SIZE), f32),
            pltpu.VMEM((1, width + 8 * HEAD_SIZE), f32),
            pltpu.VMEM((1, qkv_bias.shape[0] + 8 * HEAD_SIZE), f32),
            pltpu.VMEM((seq_rows, HEAD_SIZE), f32),
            pltpu.VMEM((seq_rows, HEAD_SIZE), f32),
            pltpu.SMEM((1,), jnp.int32),
            pltpu.SMEM((1,), f32),
            pltpu.SMEM((everyone,), jnp.int32),
            dma((31,)),
            dma((2, shards, 2, 2)),
            dma((3, 2, shards, 2)),
            dma((2, 2)),
            dma((3, 2)),
            dma((3, 2)),
            dma((3,)),
            dma((3,)),
            dma((3, line, 3)),
            dma((3, line, 3)),
            dma((groups,)),
            dma((groups,)),
            dma((3,)),
            dma((3,)),
            dma((2,)),
            dma((everyone,)),
            dma((everyone,)),
        ],
        compiler_params=pltpu.CompilerParams(
            collective_id=0, has_side_effects=True, vmem_limit_bytes=56 * 1024 * 1024
        ),
    )(
        tokens[0],
        qkv_weight,
        out_weight.T,
        lengths,
        pair_weight,
        partner,
        norm_gain,
        final_gain,
        value_head,
        qkv_bias,
        jnp.asarray(cosine),
        jnp.asarray(sine),
    )
    return hidden[None], margin, loss.reshape(())


def projected_by_gathers(
    tokens,
    lengths,
    norm_gain,
    qkv_weight,
    qkv_bias,
    out_weight,
):
    sequence = tokens[0]
    length_rows = sequence.shape[0]
    width = sequence.shape[1]
    normed = rms_scale(sequence.astype(jnp.float32), norm_gain).astype(jnp.bfloat16)
    query_group_count = lax.axis_size("dp")
    group_index = lax.axis_index("dp")
    query_heads = QUERY_HEADS // query_group_count
    key_value_heads = KEY_VALUE_HEADS // query_group_count
    query_cols = query_heads * HEAD_SIZE
    key_cols = key_value_heads * HEAD_SIZE
    group_normed, group_lengths = (
        lax.all_gather(normed[None], "dp", axis=0, tiled=True),
        lax.all_gather(lengths, "dp", axis=0, tiled=True),
    )
    seq_count = group_normed.shape[0]
    flat = group_normed.reshape(seq_count * length_rows, width)
    qkv_cols = jnp.concatenate(
        [
            lax.dynamic_slice_in_dim(qkv_weight, group_index * query_cols, query_cols, 1),
            lax.dynamic_slice_in_dim(
                qkv_weight, QUERY_FEATURES + group_index * key_cols, key_cols, 1
            ),
            lax.dynamic_slice_in_dim(
                qkv_weight, QUERY_FEATURES + KEY_FEATURES + group_index * key_cols, key_cols, 1
            ),
        ],
        axis=1,
    )
    bias_cols = jnp.concatenate(
        [
            lax.dynamic_slice_in_dim(qkv_bias, group_index * query_cols, query_cols, 0),
            lax.dynamic_slice_in_dim(
                qkv_bias, QUERY_FEATURES + group_index * key_cols, key_cols, 0
            ),
            lax.dynamic_slice_in_dim(
                qkv_bias, QUERY_FEATURES + KEY_FEATURES + group_index * key_cols, key_cols, 0
            ),
        ],
        axis=0,
    )
    out_rows = lax.dynamic_slice_in_dim(out_weight, group_index * query_cols, query_cols, 0)
    qkv_full, out_full = (
        lax.all_gather(qkv_cols, "fsdp", axis=0, tiled=True),
        lax.all_gather(out_rows, "fsdp", axis=1, tiled=True),
    )
    query_key_value = jnp.dot(flat, qkv_full, preferred_element_type=jnp.float32) + bias_cols
    attn = attend(
        query_key_value.reshape(seq_count, length_rows, -1),
        group_lengths,
        query_heads,
        key_value_heads,
    )
    return lax.psum_scatter(
        jnp.dot(attn, out_full, preferred_element_type=jnp.float32),
        "dp",
        scatter_dimension=0,
        tiled=True,
    )


def per_device(
    tokens,
    lengths,
    partner,
    pair_weight,
    norm_gain,
    qkv_weight,
    qkv_bias,
    out_weight,
    final_gain,
    value_head,
):
    if layer_fits(lax.axis_size("fsdp"), lax.axis_size("dp"), tokens, qkv_weight, out_weight):
        return layer(
            tokens,
            lengths,
            partner,
            pair_weight,
            norm_gain,
            qkv_weight,
            qkv_bias,
            out_weight,
            final_gain,
            value_head,
        )
    sequence = tokens[0]
    length = lengths[0]
    projected = projected_by_gathers(tokens, lengths, norm_gain, qkv_weight, qkv_bias, out_weight)
    hidden = (sequence.astype(jnp.float32) + projected).astype(jnp.bfloat16)
    last = lax.dynamic_slice_in_dim(hidden, length - 1, 1, 0)[0].astype(jnp.float32)
    score = jnp.sum(rms_scale(last, final_gain) * value_head)
    everyone, weights_all = (
        lax.all_gather(score.reshape(1), ("fsdp", "dp"), axis=0, tiled=True),
        lax.all_gather(pair_weight, ("fsdp", "dp"), axis=0, tiled=True),
    )
    total_seqs = everyone.shape[0]
    mine = lax.axis_index(("fsdp", "dp"))
    index_all = jnp.arange(total_seqs, dtype=jnp.int32)
    my_partner = jnp.sum(jnp.where(index_all == mine, partner, 0))
    other = jnp.sum(jnp.where(index_all == my_partner, everyone, jnp.float32(0.0)))
    margin = jnp.where(mine < my_partner, score - other, other - score)
    matches = partner[:, None] == index_all[None, :]
    others_all = jnp.sum(jnp.where(matches, everyone[None, :], jnp.float32(0.0)), axis=1)
    margins_all = jnp.where(index_all < partner, everyone - others_all, others_all - everyone)
    loss = jnp.sum(weights_all * jax.nn.softplus(-margins_all)) / total_seqs
    return (hidden[None], margin.reshape(1), loss)


def solution(mesh):
    return jax.shard_map(
        per_device,
        mesh=mesh,
        in_specs=(
            P(("fsdp", "dp"), None, None),
            P(("fsdp", "dp")),
            P(),
            P(("fsdp", "dp")),
            P(),
            P("fsdp", None),
            P(),
            P(None, "fsdp"),
            P(),
            P(),
        ),
        out_specs=(P(("fsdp", "dp"), None, None), P(("fsdp", "dp")), P()),
        check_vma=False,
    )
```

```python
import functools

import jax
import jax.numpy as jnp
import numpy as np
from jax import lax
from jax.experimental import pallas as pl
from jax.experimental.pallas import tpu as pltpu
from jax.sharding import PartitionSpec as P

QUERY_HEADS = 28
KEY_VALUE_HEADS = 4
HEAD_SIZE = 128
QUERY_FEATURES = 3584
KEY_FEATURES = 512


def rms_scale(value_rows, gain):
    return (
        value_rows
        * lax.rsqrt(jnp.mean(value_rows * value_rows, axis=-1, keepdims=True) + 1e-06)
        * gain
    )


def apply_rotary(heads, length_rows):
    half = HEAD_SIZE // 2
    positions = jnp.arange(length_rows, dtype=jnp.float32)
    freqs = jnp.exp(
        -(2.0 * jnp.arange(half, dtype=jnp.float32) / HEAD_SIZE) * jnp.log(jnp.float32(1000000.0))
    )
    angles = positions[:, None] * freqs[None, :]
    cosine = jnp.cos(angles)
    sine = jnp.sin(angles)
    first = heads[..., :half]
    second = heads[..., half:]
    return jnp.concatenate(
        [first * cosine - second * sine, second * cosine + first * sine], axis=-1
    )


def attend(query_key_value, group_lengths, query_heads, key_value_heads):
    seq_count, length_rows, _ = query_key_value.shape
    query_width = query_heads * HEAD_SIZE
    key_width = key_value_heads * HEAD_SIZE
    query_rows = (
        query_key_value[..., :query_width]
        .reshape(seq_count, length_rows, query_heads, HEAD_SIZE)
        .transpose(0, 2, 1, 3)
    )
    key_rows = (
        query_key_value[..., query_width : query_width + key_width]
        .reshape(seq_count, length_rows, key_value_heads, HEAD_SIZE)
        .transpose(0, 2, 1, 3)
    )
    value_rows = (
        query_key_value[..., query_width + key_width :]
        .reshape(seq_count, length_rows, key_value_heads, HEAD_SIZE)
        .transpose(0, 2, 1, 3)
        .astype(jnp.bfloat16)
    )
    query_rows = (
        apply_rotary(query_rows, length_rows)
        .astype(jnp.bfloat16)
        .reshape(seq_count, key_value_heads, query_heads // key_value_heads, length_rows, HEAD_SIZE)
    )
    key_rows = apply_rotary(key_rows, length_rows).astype(jnp.bfloat16)
    scores = jnp.einsum(
        "bgqtd,bgsd->bgqts", query_rows, key_rows, preferred_element_type=jnp.float32
    ) / jnp.sqrt(jnp.float32(HEAD_SIZE))
    places = jnp.arange(length_rows, dtype=jnp.int32)
    causal = places[None, :] <= places[:, None]
    usable = places[None, :] < group_lengths[:, None]
    allowed = causal[None, :, :] & usable[:, None, :]
    scores = jnp.where(allowed[:, None, None, :, :], scores, jnp.float32(-1e30))
    highest = jnp.max(scores, axis=-1, keepdims=True)
    expd = jnp.exp(scores - highest)
    probs = (expd / jnp.sum(expd, axis=-1, keepdims=True)).astype(jnp.bfloat16)
    mixed = jnp.einsum("bgqts,bgsd->bgqtd", probs, value_rows, preferred_element_type=jnp.float32)
    mixed = mixed.reshape(seq_count, query_heads, length_rows, HEAD_SIZE).transpose(0, 2, 1, 3)
    return mixed.reshape(seq_count * length_rows, query_width).astype(jnp.bfloat16)


UP, DOWN, PARTNER = 0, 1, 2


def rotary_tables(length_rows):
    half = HEAD_SIZE // 2
    freqs = 1000000.0 ** (-2.0 * np.arange(half) / HEAD_SIZE)
    angles = np.arange(length_rows)[:, None] * freqs[None, :]
    cosine, sine = np.cos(angles), np.sin(angles)
    return (
        np.concatenate([cosine, cosine], axis=1).astype(np.float32),
        np.concatenate([-sine, sine], axis=1).astype(np.float32),
    )


def out_pieces(out_cols):
    big = (out_cols // 2 + HEAD_SIZE - 1) // HEAD_SIZE * HEAD_SIZE
    return big, out_cols - big


def layer_kernel(
    shards,
    groups,
    tokens,
    qkv_weight,
    out_weight,
    length_one,
    pair_weight_one,
    partner_all,
    norm_gain_flat,
    final_gain_flat,
    value_head_flat,
    qkv_bias_flat,
    cosine_table,
    sine_table,
    hidden,
    results,
    qkv_full,
    out_full,
    cross_qkv,
    cross_out,
    tok_own,
    len_tile,
    len_all,
    normed,
    qkv_rows,
    attn,
    own,
    part_out,
    part_in,
    attn_help,
    help_own,
    help_out,
    help_in,
    help_sum,
    help_done,
    stats,
    score_tile,
    score_all,
    partner_rows,
    norm_gain,
    final_gain,
    value_head,
    qkv_bias,
    cosine,
    sine,
    length,
    pair_weight,
    partner,
    local_sem,
    recv_sem,
    send_sem,
    cross_send,
    tok_send,
    tok_recv,
    len_send,
    len_recv,
    part_send,
    part_recv,
    attn_send,
    attn_recv,
    help_send,
    help_recv,
    done_sem,
    score_send,
    score_recv,
):
    line = shards // 2
    f = lax.axis_index("fsdp")
    g = lax.axis_index("dp")
    z = f // 2
    y = f % 2
    x = g // 2
    core = g % 2
    seq_rows = tokens.shape[0]
    width = tokens.shape[1]
    depth = qkv_weight.shape[0]
    out_cols = out_weight.shape[0]
    query_cols = QUERY_FEATURES // groups
    key_cols = KEY_FEATURES // groups
    heads = query_cols // HEAD_SIZE
    quarter = depth // 4
    pair = 2 * out_cols
    big, small = out_pieces(out_cols)
    is_end = (z == 0) | (z == line - 1)
    is_helper = (z == 1) | (z == line - 2)
    far = jnp.where((z == 0) | (z == 1), line - 1, 0)
    end_to_helper = {"fsdp": jnp.where(z == 0, f + 2, f - 2)}
    helper_to_end = {"fsdp": jnp.where(z == 1, f - 2, f + 2)}
    has_up = z < line - 1
    has_down = z > 0
    team = 2 * x + y
    across_team = 2 * x + 1 - y
    across = 2 * z + 1 - y
    x_peer = 2 * (1 - x) + core
    team_ids = ({"dp": x_peer}, {"fsdp": across}, {"fsdp": across, "dp": x_peer})
    way_ids = ({"fsdp": f + 2}, {"fsdp": f - 2}, {"dp": 2 * x + 1 - core})

    barrier = pltpu.get_barrier_semaphore()
    for target in (*team_ids, way_ids[PARTNER]):
        pl.semaphore_signal(barrier, inc=1, device_id=target)
    for way, ok in ((UP, has_up), (DOWN, has_down)):

        @pl.when(ok)
        def _():
            pl.semaphore_signal(barrier, inc=1, device_id=way_ids[way])

    def out_rows(side, piece, half):
        size = (big, small)[piece] // 2
        start = (side * small, (1 - side) * big)[piece]
        return start + half * size, size

    def slot(m, s, piece, half):
        if m == 0:
            start = s * depth + (2 * piece + half) * quarter
            return qkv_full.at[pl.ds(pl.multiple_of(start, 16), quarter)]
        start, size = out_rows(lax.rem(s, 2), piece, half)
        return out_full.at[pl.ds(pl.multiple_of(s * out_cols + start, 16), size)]

    count = 0

    def local(source, dest):
        nonlocal count
        copy = pltpu.make_async_copy(source, dest, local_sem.at[count])
        count += 1
        copy.start()
        return copy

    def qkv_parts(piece, half, owner, dest):
        rows = pl.ds(pl.multiple_of((2 * piece + half) * quarter, 16), quarter)
        return [
            local(
                qkv_weight.at[rows, pl.ds(pl.multiple_of(start, 128), size)],
                dest.at[:, pl.ds(to, size)],
            )
            for start, size, to in (
                (owner * query_cols, query_cols, 0),
                (QUERY_FEATURES + owner * key_cols, key_cols, query_cols),
                (QUERY_FEATURES + KEY_FEATURES + owner * key_cols, key_cols, query_cols + key_cols),
            )
        ]

    length_load = local(length_one, length)
    own_loads, cross_loads = [], []
    for j in range(2):
        own_loads.append(qkv_parts(j, core, team, slot(0, f, j, core)))
        cross_loads.append(qkv_parts(j, core, across_team, cross_qkv.at[j]))
    tok_local = local(tokens, tok_own)
    vectors = [
        local(flat, row.at[0, pl.ds(0, flat.shape[0])])
        for flat, row in (
            (norm_gain_flat, norm_gain),
            (final_gain_flat, final_gain),
            (value_head_flat, value_head),
            (qkv_bias_flat, qkv_bias),
        )
    ]
    late_loads = []
    for j in range(2):
        late_loads.extend(qkv_parts(j, 1 - core, team, slot(0, f, j, 1 - core)))
    out_own = local(
        out_weight.at[:, pl.ds(pl.multiple_of(team * query_cols, 128), query_cols)],
        out_full.at[pl.ds(pl.multiple_of(f * out_cols, 16), out_cols)],
    )

    def cross_part(m, j):
        if m == 0:
            return cross_qkv.at[j]
        return cross_out.at[j, pl.ds(0, (small, big)[j] // 2)]

    out_cross = []
    for j in range(2):
        start, size = out_rows(y, 1 - j, core)
        out_cross.append(
            local(
                out_weight.at[
                    pl.ds(pl.multiple_of(start, 16), size),
                    pl.ds(pl.multiple_of(across_team * query_cols, 128), query_cols),
                ],
                cross_part(1, j),
            )
        )
    small_loads = [
        local(source, dest)
        for source, dest in (
            (pair_weight_one, pair_weight),
            (partner_all, partner),
            (cosine_table, cosine),
            (sine_table, sine),
        )
    ]
    everyone = shards * groups
    me = f * groups + g

    pl.semaphore_wait(barrier, 4 + has_up.astype(jnp.int32) + has_down.astype(jnp.int32))

    def way_copy(way, m, s, piece):
        return pltpu.make_async_remote_copy(
            src_ref=slot(m, s, piece, core),
            dst_ref=slot(m, s, piece, core),
            send_sem=send_sem.at[way, m, s, piece],
            recv_sem=recv_sem.at[m, s, piece, core],
            device_id=way_ids[way],
        )

    def piece_of(m, o, j):
        return 1 - j if m == 1 and o == 1 else j

    def cross_copy(m, j):
        piece = piece_of(m, 1, j)
        return pltpu.make_async_remote_copy(
            src_ref=cross_part(m, j),
            dst_ref=slot(m, f, piece, core),
            send_sem=cross_send.at[m, j],
            recv_sem=recv_sem.at[m, f, piece, core],
            device_id=team_ids[1],
        )

    def arrived(m, s, piece, half):
        there = slot(m, s, piece, half)
        pltpu.make_async_copy(there, there, recv_sem.at[m, s, piece, half]).wait()

    def send_both(m, s, piece):
        pl.when(has_up)(way_copy(UP, m, s, piece).start)
        pl.when(has_down)(way_copy(DOWN, m, s, piece).start)

    def cross_step(m, j):
        piece = piece_of(m, 1, j)
        arrived(m, across, piece, core)
        send_both(m, across, piece)
        way_copy(PARTNER, m, across, piece).start()

    def sides(k, o):
        row = y if o == 0 else 1 - y
        below, above = z - k, z + k
        return (
            (below >= 0, 2 * jnp.maximum(below, 0) + row, UP, has_up),
            (above < line, 2 * jnp.minimum(above, line - 1) + row, DOWN, has_down),
        )

    def line_step(m, k, o, j):
        piece = piece_of(m, o, j)
        for ok, s, way, onward in sides(k, o):
            if m == 1:
                onward = onward & (k < line - 2)

            @pl.when(ok)
            def _():
                arrived(m, s, piece, core)
                pl.when(onward)(way_copy(way, m, s, piece).start)
                way_copy(PARTNER, m, s, piece).start()

    def from_partner(m, s):
        for piece in range(2):
            arrived(m, s, piece, 1 - core)

    half_rows = seq_rows // 2

    def tok_copy(way, half):
        source = (0, 0, 1 + half)[way]
        target = team_ids[way] if way < 2 else team_ids[1 - half]
        return pltpu.make_async_remote_copy(
            src_ref=normed.at[pl.ds(source * seq_rows + half * half_rows, half_rows)],
            dst_ref=normed.at[pl.ds((1 + way) * seq_rows + half * half_rows, half_rows)],
            send_sem=tok_send.at[way, half],
            recv_sem=tok_recv.at[way, half],
            device_id=target,
        )

    def len_copy(way):
        return pltpu.make_async_remote_copy(
            src_ref=len_tile,
            dst_ref=len_all.at[1 + way],
            send_sem=len_send.at[way],
            recv_sem=len_recv.at[way],
            device_id=team_ids[way],
        )

    for j in range(2):
        for copy in own_loads[j]:
            copy.wait()
        send_both(0, f, j)
        for copy in cross_loads[j]:
            copy.wait()
        cross_copy(0, j).start()

    tok_local.wait()
    for copy in vectors:
        copy.wait()
    norm_rows = 16

    @pl.loop(0, seq_rows // norm_rows)
    def _(i):
        at = pl.ds(pl.multiple_of(i * norm_rows, norm_rows), norm_rows)
        rows = tok_own[at, :].astype(jnp.float32)
        scale = lax.rsqrt(jnp.mean(rows * rows, axis=-1, keepdims=True) + 1e-06)
        normed[at, :] = (rows * scale * norm_gain[...]).astype(jnp.bfloat16)

    tok_copy(0, 0).start()
    tok_copy(1, 1).start()
    tok_copy(0, 1).start()
    tok_copy(1, 0).start()
    length_load.wait()
    len_tile[...] = jnp.full(len_tile.shape, length[0, 0], jnp.int32)
    len_all[0] = len_tile[...]
    for way in range(3):
        len_copy(way).start()

    bias_parts = (
        (team * query_cols, query_cols, 0),
        (QUERY_FEATURES + team * key_cols, key_cols, query_cols),
        (QUERY_FEATURES + KEY_FEATURES + team * key_cols, key_cols, query_cols + key_cols),
    )
    for start, size, to in bias_parts:
        qkv_rows[:, to : to + size] = jnp.broadcast_to(
            qkv_bias[:, pl.ds(pl.multiple_of(start, HEAD_SIZE), size)],
            (groups * seq_rows, size),
        )

    for j in range(2):
        cross_step(0, j)
        line_step(0, 1, 0, j)
    tok_copy(0, 0).wait_recv()
    tok_copy(2, 0).start()
    line_step(0, 1, 1, 0)
    line_step(0, 1, 1, 1)
    tok_copy(1, 1).wait_recv()
    tok_copy(2, 1).start()
    out_own.wait()
    for j in range(2):
        out_cross[j].wait()
        cross_copy(1, j).start()
    for k in range(2, line - 1):
        for o in range(2):
            for j in range(2):
                line_step(0, k, o, j)
    for j in range(2):
        send_both(1, f, j)

    tok_copy(0, 1).wait_recv()
    tok_copy(1, 0).wait_recv()
    tok_copy(2, 0).wait_recv()
    tok_copy(2, 1).wait_recv()
    for way in range(3):
        len_copy(way).wait_recv()
    for copy in (*late_loads, *small_loads):
        copy.wait()

    @pl.loop(0, everyone)
    def _(i):
        partner_rows[pl.ds(i, 1), :] = jnp.full((1, HEAD_SIZE), partner[i], jnp.int32)

    tile = 3 * HEAD_SIZE

    def qkv_step(place):
        rows = pl.ds(pl.multiple_of(place * 2 * depth, 128), 2 * depth)

        @pl.loop(0, (query_cols + 2 * key_cols) // tile)
        def _(t):
            cols = pl.ds(pl.multiple_of(t * tile, tile), tile)
            qkv_rows[:, cols] += jnp.dot(
                normed[:, rows], qkv_full[rows, cols], preferred_element_type=jnp.float32
            )

    def qkv_places(first, last):
        @pl.loop(2 * first, 2 * last)
        def _(i):
            k = i // 2
            place = z + (2 * lax.rem(i, 2) - 1) * k

            @pl.when((place >= 0) & (place < line))
            def _():
                from_partner(0, 2 * place)
                from_partner(0, 2 * place + 1)
                qkv_step(place)

    @pl.loop(0, 1)
    def _(i):
        from_partner(0, across)
        qkv_step(z)

    qkv_places(1, line - 1)
    for j in range(2):
        cross_step(1, j)
    for o in range(2):
        for j in range(2):
            line_step(0, line - 1, o, j)
    qkv_places(line - 1, line)

    def head_rows(j, column):
        return qkv_rows[
            pl.ds(pl.multiple_of(j * seq_rows, seq_rows), seq_rows), column : column + HEAD_SIZE
        ]

    def rotate(rows):
        return (
            rows * cosine[...] + pltpu.roll(rows, HEAD_SIZE // 2, 1) * sine[...]
        ).astype(jnp.bfloat16)

    key_heads = key_cols // HEAD_SIZE
    share = heads // key_heads

    def lanes_of(at, size):
        return pl.ds(pl.multiple_of(at, HEAD_SIZE), size)

    units = ((0, big), (big, 2 * small), (pair - big, big))

    def part_copy(way, place, at, size, unit):
        cols = lanes_of(at, size)
        return pltpu.make_async_remote_copy(
            src_ref=part_out.at[place, pl.ds((1 + way) * seq_rows, seq_rows), cols],
            dst_ref=part_in.at[way, place, :, cols],
            send_sem=part_send.at[way, place, unit],
            recv_sem=part_recv.at[way, place, unit],
            device_id=team_ids[way],
        )

    def project(place, at, size, unit):
        cols = lanes_of(at, size)
        result = lax.dot_general(
            attn[...],
            out_full[lanes_of(place * pair + at, size), :],
            (((1,), (1,)), ((), ())),
            preferred_element_type=jnp.float32,
        )
        part_out[place, :, cols] = result.astype(jnp.bfloat16)
        own[place, :, cols] = result[:seq_rows]
        for way in (2, 0, 1):
            part_copy(way, place, at, size, unit).start()

    def attn_copy(j):
        rows = pl.ds(pl.multiple_of(j * seq_rows, seq_rows), seq_rows)
        return pltpu.make_async_remote_copy(
            src_ref=attn.at[rows],
            dst_ref=attn_help.at[rows],
            send_sem=attn_send.at[j],
            recv_sem=attn_recv.at[j],
            device_id=end_to_helper,
        )

    from_partner(1, across)

    @pl.loop(0, groups)
    def _(i):
        j = groups - 1 - i
        query_place = lax.broadcasted_iota(jnp.int32, (seq_rows, seq_rows), 0)
        key_place = lax.broadcasted_iota(jnp.int32, (seq_rows, seq_rows), 1)
        allowed = (key_place <= query_place) & (key_place < len_all[j, 0:1, :])
        at = pl.ds(pl.multiple_of(j * seq_rows, seq_rows), seq_rows)
        for kh in range(key_heads):
            offset = kh * HEAD_SIZE
            key = rotate(head_rows(j, query_cols + offset))
            value = head_rows(j, query_cols + key_cols + offset).astype(jnp.bfloat16)
            for h in range(kh * share, (kh + 1) * share):
                query = rotate(head_rows(j, h * HEAD_SIZE))
                scores = lax.dot_general(
                    query, key, (((1,), (1,)), ((), ())), preferred_element_type=jnp.float32
                ) * np.float32(1 / np.sqrt(HEAD_SIZE))
                scores = jnp.where(allowed, scores, jnp.float32(-1e30))
                expd = jnp.exp(scores - jnp.max(scores, axis=-1, keepdims=True))
                inverse = 1.0 / jnp.sum(expd, axis=-1, keepdims=True)
                probs = (expd * inverse).astype(jnp.bfloat16)
                attn[at, h * HEAD_SIZE : (h + 1) * HEAD_SIZE] = jnp.dot(
                    probs, value, preferred_element_type=jnp.float32
                ).astype(jnp.bfloat16)
        pl.when(is_end)(attn_copy(j).start)
        result = lax.dot_general(
            attn[at, :],
            out_full[lanes_of(z * pair, pair), :],
            (((1,), (1,)), ((), ())),
            preferred_element_type=jnp.float32,
        )
        part_out[z, at, :] = result.astype(jnp.bfloat16)
        own[z] = result
        for way in range(3):
            pl.when(j == way + 1)(part_copy(way, z, 0, pair, 0).start)

    def project_pair(place):
        @pl.loop(0, 2)
        def _(i):
            project(place, i * (pair - big), big, 2 * i)

        project(place, big, 2 * small, 1)

    place = lax.broadcasted_iota(jnp.int32, len_tile.shape, 1)
    pick = (place == len_tile[...] - 1).astype(jnp.bfloat16)
    stats[...] = jnp.zeros_like(stats)

    def finish(place, sums):
        cols = lanes_of(place * pair, pair)
        hidden[:, cols] = (tok_own[:, cols].astype(jnp.float32) + sums).astype(jnp.bfloat16)
        last = jnp.dot(pick, hidden[:, cols], preferred_element_type=jnp.float32)
        weighted = last * final_gain[:, cols] * value_head[:, cols]
        squares = last * last
        for t in range(pair // HEAD_SIZE):
            lanes = slice(t * HEAD_SIZE, (t + 1) * HEAD_SIZE)
            stats[0] += squares[:, lanes]
            stats[1] += weighted[:, lanes]

    def each_part(place, body):
        @pl.when(place == z)
        def _():
            for way in range(3):
                body(part_copy(way, place, 0, pair, 0))

        @pl.when(place != z)
        def _():
            for unit, (at, size) in enumerate(units):
                for way in range(3):
                    body(part_copy(way, place, at, size, unit))

    def finish_parts(place):
        each_part(place, lambda copy: copy.wait_recv())
        total = own[place]
        for way in range(3):
            total += part_in[way, place].astype(jnp.float32)
        finish(place, total)

    def at_sides(k, body):
        @pl.loop(0, 2)
        def _(i):
            place = z + (2 * i - 1) * k

            @pl.when((place >= 0) & (place < line) & ((k > 0) | (i == 0)))
            def _():
                body(place)

    def own_unit(place):
        arrived(1, 2 * place + y, 0, 1 - core)
        project(place, y * (pair - big), big, 2 * y)

    def mid_unit(place):
        arrived(1, 2 * place + y, 1, 1 - core)
        arrived(1, 2 * place + 1 - y, 1, 1 - core)
        project(place, big, 2 * small, 1)

    def cross_unit(place):
        arrived(1, 2 * place + 1 - y, 0, 1 - core)
        project(place, (1 - y) * (pair - big), big, 2 * (1 - y))

    @pl.loop(1, line - 1)
    def _(k):
        mine = jnp.logical_not(is_helper) | (k < line - 2)
        line_step(1, k, 0, 0)
        line_step(1, k, 0, 1)

        @pl.when(mine)
        def _():
            at_sides(k, own_unit)

        @pl.when(jnp.logical_not(is_helper))
        def _():
            at_sides(k - 1, finish_parts)

        line_step(1, k, 1, 0)

        @pl.when(mine)
        def _():
            at_sides(k, mid_unit)

        line_step(1, k, 1, 1)

        @pl.when(mine)
        def _():
            at_sides(k, cross_unit)

    def help_part(way):
        return pltpu.make_async_remote_copy(
            src_ref=help_out.at[1 + way],
            dst_ref=help_in.at[way],
            send_sem=help_send.at[way],
            recv_sem=help_recv.at[way],
            device_id=team_ids[way],
        )

    done_copy = pltpu.make_async_remote_copy(
        src_ref=help_sum,
        dst_ref=help_done,
        send_sem=done_sem.at[0],
        recv_sem=done_sem.at[1],
        device_id=helper_to_end,
    )

    @pl.when(is_helper)
    def _():
        for o in range(2):
            from_partner(1, 2 * far + o)

        @pl.loop(0, groups)
        def _(i):
            j = groups - 1 - i
            rows = pl.ds(pl.multiple_of(j * seq_rows, seq_rows), seq_rows)
            pltpu.make_async_copy(attn_help.at[rows], attn_help.at[rows], attn_recv.at[j]).wait()
            result = lax.dot_general(
                attn_help[rows, :],
                out_full[lanes_of(far * pair, pair), :],
                (((1,), (1,)), ((), ())),
                preferred_element_type=jnp.float32,
            )
            help_own[...] = result
            help_out[j] = result.astype(jnp.bfloat16)
            for way in range(3):
                pl.when(j == way + 1)(help_part(way).start)

        project_pair(far)

        @pl.loop(0, line)
        def _(place):
            pl.when(place != far)(lambda: finish_parts(place))

        for way in range(3):
            help_part(way).wait_recv()
        total = help_own[...]
        for way in range(3):
            total += help_in[way].astype(jnp.float32)
        help_sum[...] = total.astype(jnp.bfloat16)
        done_copy.start()

    @pl.when(is_end)
    def _():
        at_sides(line - 2, finish_parts)
        done_copy.wait_recv()
        finish(far, help_done[...].astype(jnp.float32))

    @pl.when(is_helper)
    def _():
        finish_parts(far)

    mean = jnp.sum(stats[0], axis=-1, keepdims=True) / width
    score = jnp.sum(stats[1], axis=-1, keepdims=True) * lax.rsqrt(mean + 1e-06)
    first_row = lax.broadcasted_iota(jnp.int32, score_tile.shape, 0) == 0
    score_tile[...] = jnp.where(first_row, score, jnp.full(score_tile.shape, pair_weight[0, 0]))
    score_all[me] = score_tile[...]

    def score_copy(i):
        other = lax.rem(me + i, everyone)
        return pltpu.make_async_remote_copy(
            src_ref=score_tile,
            dst_ref=score_all.at[me],
            send_sem=score_send.at[other],
            recv_sem=score_recv.at[me],
            device_id={"fsdp": other // groups, "dp": lax.rem(other, groups)},
        )

    @pl.loop(1, everyone)
    def _(i):
        score_copy(i).start()

    for m in range(2):
        for j in range(2):
            cross_copy(m, j).wait_send()

    @pl.loop(0, shards)
    def _(s):
        place = s // 2
        skipped = (place == far) & is_end
        for way, ok, ok_out in (
            (UP, has_up & (place <= z), (place > 0) | (z < line - 2)),
            (DOWN, has_down & (place >= z), (place < line - 1) | (z > 1)),
            (PARTNER, s != f, jnp.logical_not(skipped)),
        ):
            for m in range(2):

                @pl.when(ok & ok_out if m == 1 else ok)
                def _():
                    for piece in range(2):
                        way_copy(way, m, s, piece).wait_send()

    @pl.loop(0, line)
    def _(place):
        @pl.when(jnp.logical_not(is_end & (place == far)))
        def _():
            each_part(place, lambda copy: copy.wait_send())

    @pl.when(is_helper)
    def _():
        for way in range(3):
            help_part(way).wait_send()
        done_copy.wait_send()

    @pl.when(is_end)
    def _():
        @pl.loop(0, groups)
        def _(j):
            attn_copy(j).wait_send()

    for way in range(3):
        len_copy(way).wait_send()
        for half in range(2):
            tok_copy(way, half).wait_send()

    @pl.loop(1, everyone)
    def _(i):
        other = lax.rem(me + i, everyone)
        pltpu.make_async_copy(
            score_all.at[other], score_all.at[other], score_recv.at[other]
        ).wait()

    scores = score_all[:, 0, :]
    weights = score_all[:, 1, :]
    row = lax.broadcasted_iota(jnp.int32, scores.shape, 0)
    lane = lax.broadcasted_iota(jnp.int32, scores.shape, 1)
    partners = partner_rows[...]
    score_row = jnp.sum(jnp.where(row == lane, scores, 0.0), axis=0, keepdims=True)
    others = jnp.sum(jnp.where(partners == lane, score_row, 0.0), axis=1, keepdims=True)
    margins = jnp.where(row < partners, scores - others, others - scores)
    softplus = jnp.maximum(-margins, 0.0) + jnp.log1p(jnp.exp(-jnp.abs(margins)))
    first_lane = lane == 0
    margin = jnp.sum(jnp.where(first_lane & (row == me), margins, 0.0))
    loss = jnp.sum(jnp.where(first_lane, weights * softplus, 0.0)) / everyone
    results[...] = jnp.where(first_row, jnp.full(results.shape, margin), loss)

    @pl.loop(1, everyone)
    def _(i):
        score_copy(i).wait_send()


def layer_fits(shards, groups, tokens, qkv_weight, out_weight):
    return (
        shards % 2 == 0
        and shards >= 8
        and qkv_weight.shape[0] % 64 == 0
        and groups == 4
        and KEY_VALUE_HEADS % groups == 0
        and tokens.shape[1] == HEAD_SIZE
        and shards * groups <= HEAD_SIZE
        and out_weight.shape[1] % 64 == 0
        and out_weight.shape[1] > HEAD_SIZE
    )


def layer(
    tokens,
    lengths,
    partner,
    pair_weight,
    norm_gain,
    qkv_weight,
    qkv_bias,
    out_weight,
    final_gain,
    value_head,
):
    shards, groups = lax.axis_size("fsdp"), lax.axis_size("dp")
    _, seq_rows, width = tokens.shape
    depth = qkv_weight.shape[0]
    out_cols = out_weight.shape[1]
    query_cols = QUERY_FEATURES // groups
    key_cols = KEY_FEATURES // groups
    all_cols = query_cols + 2 * key_cols
    rows = groups * seq_rows
    line, pair = shards // 2, 2 * out_cols
    cosine, sine = rotary_tables(seq_rows)
    everyone = shards * groups
    dma = pltpu.SemaphoreType.DMA
    vmem = pl.BlockSpec(memory_space=pltpu.VMEM)
    bf16, f32 = jnp.bfloat16, jnp.float32
    hidden, results = pl.pallas_call(
        functools.partial(layer_kernel, shards, groups),
        out_shape=(
            pltpu.VMEM((seq_rows, width), bf16),
            pltpu.VMEM((8, HEAD_SIZE), f32),
        ),
        in_specs=[pl.BlockSpec(memory_space=pltpu.HBM)] * 12,
        out_specs=(vmem, vmem),
        scratch_shapes=[
            pltpu.VMEM((shards * depth, all_cols), bf16),
            pltpu.VMEM((shards * out_cols, query_cols), bf16),
            pltpu.VMEM((2, depth // 4, all_cols), bf16),
            pltpu.VMEM((2, out_pieces(out_cols)[0] // 2, query_cols), bf16),
            pltpu.VMEM((seq_rows, width), bf16),
            pltpu.VMEM((8, seq_rows), jnp.int32),
            pltpu.VMEM((groups, 8, seq_rows), jnp.int32),
            pltpu.VMEM((rows, width), bf16),
            pltpu.VMEM((rows, all_cols), f32),
            pltpu.VMEM((rows, query_cols), bf16),
            pltpu.VMEM((line, seq_rows, pair), f32),
            pltpu.VMEM((line, rows, pair), bf16),
            pltpu.VMEM((groups - 1, line, seq_rows, pair), bf16),
            pltpu.VMEM((rows, query_cols), bf16),
            pltpu.VMEM((seq_rows, pair), f32),
            pltpu.VMEM((groups, seq_rows, pair), bf16),
            pltpu.VMEM((groups - 1, seq_rows, pair), bf16),
            pltpu.VMEM((seq_rows, pair), bf16),
            pltpu.VMEM((seq_rows, pair), bf16),
            pltpu.VMEM((2, 8, HEAD_SIZE), f32),
            pltpu.VMEM((8, HEAD_SIZE), f32),
            pltpu.VMEM((everyone, 8, HEAD_SIZE), f32),
            pltpu.VMEM((everyone, HEAD_SIZE), jnp.int32),
            pltpu.VMEM((1, width), f32),
            pltpu.VMEM((1, width + 8 * HEAD_SIZE), f32),
            pltpu.VMEM((1, width + 8 * HEAD_SIZE), f32),
            pltpu.VMEM((1, qkv_bias.shape[0] + 8 * HEAD_SIZE), f32),
            pltpu.VMEM((seq_rows, HEAD_SIZE), f32),
            pltpu.VMEM((seq_rows, HEAD_SIZE), f32),
            pltpu.SMEM((1, 1), jnp.int32),
            pltpu.SMEM((1, 1), f32),
            pltpu.SMEM((everyone,), jnp.int32),
            dma((31,)),
            dma((2, shards, 2, 2)),
            dma((3, 2, shards, 2)),
            dma((2, 2)),
            dma((3, 2)),
            dma((3, 2)),
            dma((3,)),
            dma((3,)),
            dma((3, line, 3)),
            dma((3, line, 3)),
            dma((groups,)),
            dma((groups,)),
            dma((3,)),
            dma((3,)),
            dma((2,)),
            dma((everyone,)),
            dma((everyone,)),
        ],
        compiler_params=pltpu.CompilerParams(
            collective_id=0, has_side_effects=True, vmem_limit_bytes=56 * 1024 * 1024
        ),
    )(
        tokens[0],
        qkv_weight,
        out_weight.T,
        lengths[None],
        pair_weight[None],
        partner,
        norm_gain,
        final_gain,
        value_head,
        qkv_bias,
        jnp.asarray(cosine),
        jnp.asarray(sine),
    )
    return hidden[None], results[0, :1], results[1, 0]


def projected_by_gathers(
    tokens,
    lengths,
    norm_gain,
    qkv_weight,
    qkv_bias,
    out_weight,
):
    sequence = tokens[0]
    length_rows = sequence.shape[0]
    width = sequence.shape[1]
    normed = rms_scale(sequence.astype(jnp.float32), norm_gain).astype(jnp.bfloat16)
    query_group_count = lax.axis_size("dp")
    group_index = lax.axis_index("dp")
    query_heads = QUERY_HEADS // query_group_count
    key_value_heads = KEY_VALUE_HEADS // query_group_count
    query_cols = query_heads * HEAD_SIZE
    key_cols = key_value_heads * HEAD_SIZE
    group_normed, group_lengths = (
        lax.all_gather(normed[None], "dp", axis=0, tiled=True),
        lax.all_gather(lengths, "dp", axis=0, tiled=True),
    )
    seq_count = group_normed.shape[0]
    flat = group_normed.reshape(seq_count * length_rows, width)
    qkv_cols = jnp.concatenate(
        [
            lax.dynamic_slice_in_dim(qkv_weight, group_index * query_cols, query_cols, 1),
            lax.dynamic_slice_in_dim(
                qkv_weight, QUERY_FEATURES + group_index * key_cols, key_cols, 1
            ),
            lax.dynamic_slice_in_dim(
                qkv_weight, QUERY_FEATURES + KEY_FEATURES + group_index * key_cols, key_cols, 1
            ),
        ],
        axis=1,
    )
    bias_cols = jnp.concatenate(
        [
            lax.dynamic_slice_in_dim(qkv_bias, group_index * query_cols, query_cols, 0),
            lax.dynamic_slice_in_dim(
                qkv_bias, QUERY_FEATURES + group_index * key_cols, key_cols, 0
            ),
            lax.dynamic_slice_in_dim(
                qkv_bias, QUERY_FEATURES + KEY_FEATURES + group_index * key_cols, key_cols, 0
            ),
        ],
        axis=0,
    )
    out_rows = lax.dynamic_slice_in_dim(out_weight, group_index * query_cols, query_cols, 0)
    qkv_full, out_full = (
        lax.all_gather(qkv_cols, "fsdp", axis=0, tiled=True),
        lax.all_gather(out_rows, "fsdp", axis=1, tiled=True),
    )
    query_key_value = jnp.dot(flat, qkv_full, preferred_element_type=jnp.float32) + bias_cols
    attn = attend(
        query_key_value.reshape(seq_count, length_rows, -1),
        group_lengths,
        query_heads,
        key_value_heads,
    )
    return lax.psum_scatter(
        jnp.dot(attn, out_full, preferred_element_type=jnp.float32),
        "dp",
        scatter_dimension=0,
        tiled=True,
    )


def per_device(
    tokens,
    lengths,
    partner,
    pair_weight,
    norm_gain,
    qkv_weight,
    qkv_bias,
    out_weight,
    final_gain,
    value_head,
):
    if layer_fits(lax.axis_size("fsdp"), lax.axis_size("dp"), tokens, qkv_weight, out_weight):
        return layer(
            tokens,
            lengths,
            partner,
            pair_weight,
            norm_gain,
            qkv_weight,
            qkv_bias,
            out_weight,
            final_gain,
            value_head,
        )
    sequence = tokens[0]
    length = lengths[0]
    projected = projected_by_gathers(tokens, lengths, norm_gain, qkv_weight, qkv_bias, out_weight)
    hidden = (sequence.astype(jnp.float32) + projected).astype(jnp.bfloat16)
    last = lax.dynamic_slice_in_dim(hidden, length - 1, 1, 0)[0].astype(jnp.float32)
    score = jnp.sum(rms_scale(last, final_gain) * value_head)
    everyone, weights_all = (
        lax.all_gather(score.reshape(1), ("fsdp", "dp"), axis=0, tiled=True),
        lax.all_gather(pair_weight, ("fsdp", "dp"), axis=0, tiled=True),
    )
    total_seqs = everyone.shape[0]
    mine = lax.axis_index(("fsdp", "dp"))
    index_all = jnp.arange(total_seqs, dtype=jnp.int32)
    my_partner = jnp.sum(jnp.where(index_all == mine, partner, 0))
    other = jnp.sum(jnp.where(index_all == my_partner, everyone, jnp.float32(0.0)))
    margin = jnp.where(mine < my_partner, score - other, other - score)
    matches = partner[:, None] == index_all[None, :]
    others_all = jnp.sum(jnp.where(matches, everyone[None, :], jnp.float32(0.0)), axis=1)
    margins_all = jnp.where(index_all < partner, everyone - others_all, others_all - everyone)
    loss = jnp.sum(weights_all * jax.nn.softplus(-margins_all)) / total_seqs
    return (hidden[None], margin.reshape(1), loss)


def solution(mesh):
    return jax.shard_map(
        per_device,
        mesh=mesh,
        in_specs=(
            P(("fsdp", "dp"), None, None),
            P(("fsdp", "dp")),
            P(),
            P(("fsdp", "dp")),
            P(),
            P("fsdp", None),
            P(),
            P(None, "fsdp"),
            P(),
            P(),
        ),
        out_specs=(P(("fsdp", "dp"), None, None), P(("fsdp", "dp")), P()),
        check_vma=False,
    )
```

```python
import functools

import jax
import jax.numpy as jnp
import numpy as np
from jax import lax
from jax.experimental import pallas as pl
from jax.experimental.pallas import tpu as pltpu
from jax.sharding import PartitionSpec as P

QUERY_HEADS = 28
KEY_VALUE_HEADS = 4
HEAD_SIZE = 128
QUERY_FEATURES = 3584
KEY_FEATURES = 512


def rms_scale(value_rows, gain):
    return (
        value_rows
        * lax.rsqrt(jnp.mean(value_rows * value_rows, axis=-1, keepdims=True) + 1e-06)
        * gain
    )


def apply_rotary(heads, length_rows):
    half = HEAD_SIZE // 2
    positions = jnp.arange(length_rows, dtype=jnp.float32)
    freqs = jnp.exp(
        -(2.0 * jnp.arange(half, dtype=jnp.float32) / HEAD_SIZE) * jnp.log(jnp.float32(1000000.0))
    )
    angles = positions[:, None] * freqs[None, :]
    cosine = jnp.cos(angles)
    sine = jnp.sin(angles)
    first = heads[..., :half]
    second = heads[..., half:]
    return jnp.concatenate(
        [first * cosine - second * sine, second * cosine + first * sine], axis=-1
    )


def attend(query_key_value, group_lengths, query_heads, key_value_heads):
    seq_count, length_rows, _ = query_key_value.shape
    query_width = query_heads * HEAD_SIZE
    key_width = key_value_heads * HEAD_SIZE
    query_rows = (
        query_key_value[..., :query_width]
        .reshape(seq_count, length_rows, query_heads, HEAD_SIZE)
        .transpose(0, 2, 1, 3)
    )
    key_rows = (
        query_key_value[..., query_width : query_width + key_width]
        .reshape(seq_count, length_rows, key_value_heads, HEAD_SIZE)
        .transpose(0, 2, 1, 3)
    )
    value_rows = (
        query_key_value[..., query_width + key_width :]
        .reshape(seq_count, length_rows, key_value_heads, HEAD_SIZE)
        .transpose(0, 2, 1, 3)
        .astype(jnp.bfloat16)
    )
    query_rows = (
        apply_rotary(query_rows, length_rows)
        .astype(jnp.bfloat16)
        .reshape(seq_count, key_value_heads, query_heads // key_value_heads, length_rows, HEAD_SIZE)
    )
    key_rows = apply_rotary(key_rows, length_rows).astype(jnp.bfloat16)
    scores = jnp.einsum(
        "bgqtd,bgsd->bgqts", query_rows, key_rows, preferred_element_type=jnp.float32
    ) / jnp.sqrt(jnp.float32(HEAD_SIZE))
    places = jnp.arange(length_rows, dtype=jnp.int32)
    causal = places[None, :] <= places[:, None]
    usable = places[None, :] < group_lengths[:, None]
    allowed = causal[None, :, :] & usable[:, None, :]
    scores = jnp.where(allowed[:, None, None, :, :], scores, jnp.float32(-1e30))
    highest = jnp.max(scores, axis=-1, keepdims=True)
    expd = jnp.exp(scores - highest)
    probs = (expd / jnp.sum(expd, axis=-1, keepdims=True)).astype(jnp.bfloat16)
    mixed = jnp.einsum("bgqts,bgsd->bgqtd", probs, value_rows, preferred_element_type=jnp.float32)
    mixed = mixed.reshape(seq_count, query_heads, length_rows, HEAD_SIZE).transpose(0, 2, 1, 3)
    return mixed.reshape(seq_count * length_rows, query_width).astype(jnp.bfloat16)


UP, DOWN, PARTNER = 0, 1, 2


def rotary_tables(length_rows):
    half = HEAD_SIZE // 2
    freqs = 1000000.0 ** (-2.0 * np.arange(half) / HEAD_SIZE)
    angles = np.arange(length_rows)[:, None] * freqs[None, :]
    cosine, sine = np.cos(angles), np.sin(angles)
    return (
        np.concatenate([cosine, cosine], axis=1).astype(np.float32),
        np.concatenate([-sine, sine], axis=1).astype(np.float32),
    )


def out_pieces(out_cols):
    big = (out_cols // 2 + HEAD_SIZE - 1) // HEAD_SIZE * HEAD_SIZE
    return big, out_cols - big


def layer_kernel(
    shards,
    groups,
    tokens,
    qkv_weight,
    out_weight,
    length_one,
    pair_weight_one,
    partner_all,
    norm_gain_flat,
    final_gain_flat,
    value_head_flat,
    qkv_bias_flat,
    cosine_table,
    sine_table,
    hidden,
    results,
    qkv_full,
    out_full,
    cross_qkv,
    cross_out,
    tok_own,
    len_tile,
    len_all,
    normed,
    qkv_rows,
    attn,
    own,
    part_out,
    part_in,
    attn_help,
    help_own,
    help_out,
    help_in,
    help_sum,
    help_done,
    stats,
    queries,
    score_rows,
    score_tile,
    score_all,
    partner_rows,
    norm_gain,
    final_gain,
    value_head,
    qkv_bias,
    cosine,
    sine,
    length,
    pair_weight,
    partner,
    local_sem,
    recv_sem,
    send_sem,
    cross_send,
    tok_send,
    tok_recv,
    len_sem,
    part_send,
    part_recv,
    attn_send,
    attn_recv,
    help_send,
    help_recv,
    done_sem,
    score_sem,
):
    line = shards // 2
    f = lax.axis_index("fsdp")
    g = lax.axis_index("dp")
    z = f // 2
    y = f % 2
    x = g // 2
    core = g % 2
    seq_rows = tokens.shape[0]
    width = tokens.shape[1]
    depth = qkv_weight.shape[0]
    out_cols = out_weight.shape[0]
    query_cols = QUERY_FEATURES // groups
    key_cols = KEY_FEATURES // groups
    heads = query_cols // HEAD_SIZE
    quarter = depth // 4
    pair = 2 * out_cols
    big, small = out_pieces(out_cols)
    is_end = (z == 0) | (z == line - 1)
    is_helper = (z == 1) | (z == line - 2)
    far = jnp.where((z == 0) | (z == 1), line - 1, 0)
    end_to_helper = {"fsdp": jnp.where(z == 0, f + 2, f - 2)}
    helper_to_end = {"fsdp": jnp.where(z == 1, f - 2, f + 2)}
    has_up = z < line - 1
    has_down = z > 0
    team = 2 * x + y
    across_team = 2 * x + 1 - y
    across = 2 * z + 1 - y
    x_peer = 2 * (1 - x) + core
    team_ids = ({"dp": x_peer}, {"fsdp": across}, {"fsdp": across, "dp": x_peer})
    way_ids = ({"fsdp": f + 2}, {"fsdp": f - 2}, {"dp": 2 * x + 1 - core})

    barrier = pltpu.get_barrier_semaphore()
    for target in (*team_ids, way_ids[PARTNER]):
        pl.semaphore_signal(barrier, inc=1, device_id=target)
    for way, ok in ((UP, has_up), (DOWN, has_down)):

        @pl.when(ok)
        def _():
            pl.semaphore_signal(barrier, inc=1, device_id=way_ids[way])

    def out_rows(side, piece, half):
        size = (big, small)[piece] // 2
        start = (side * small, (1 - side) * big)[piece]
        return start + half * size, size

    def slot(m, s, piece, half):
        if m == 0:
            start = s * depth + (2 * piece + half) * quarter
            return qkv_full.at[pl.ds(pl.multiple_of(start, 16), quarter)]
        start, size = out_rows(lax.rem(s, 2), piece, half)
        return out_full.at[pl.ds(pl.multiple_of(s * out_cols + start, 16), size)]

    count = 0

    def local(source, dest):
        nonlocal count
        copy = pltpu.make_async_copy(source, dest, local_sem.at[count])
        count += 1
        copy.start()
        return copy

    def bytes_of(ref, sem):
        return pltpu.make_async_copy(ref, ref, sem)

    def qkv_parts(piece, half, owner, dest):
        nonlocal count
        rows = pl.ds(pl.multiple_of((2 * piece + half) * quarter, 16), quarter)
        for start, size, to in (
            (owner * query_cols, query_cols, 0),
            (QUERY_FEATURES + owner * key_cols, key_cols, query_cols),
            (QUERY_FEATURES + KEY_FEATURES + owner * key_cols, key_cols, query_cols + key_cols),
        ):
            pltpu.make_async_copy(
                qkv_weight.at[rows, pl.ds(pl.multiple_of(start, 128), size)],
                dest.at[:, pl.ds(to, size)],
                local_sem.at[count],
            ).start()
        count += 1
        return bytes_of(dest, local_sem.at[count - 1])

    length_load = local(length_one, length)
    own_loads, cross_loads = [], []
    for j in range(2):
        own_loads.append(qkv_parts(j, core, team, slot(0, f, j, core)))
        cross_loads.append(qkv_parts(j, core, across_team, cross_qkv.at[j]))
    tok_local = local(tokens, tok_own)
    vectors = [
        local(flat, row.at[0, pl.ds(0, flat.shape[0])])
        for flat, row in (
            (norm_gain_flat, norm_gain),
            (final_gain_flat, final_gain),
            (value_head_flat, value_head),
            (qkv_bias_flat, qkv_bias),
        )
    ]
    late_loads = []
    for j in range(2):
        late_loads.append(qkv_parts(j, 1 - core, team, slot(0, f, j, 1 - core)))
    out_own = local(
        out_weight.at[:, pl.ds(pl.multiple_of(team * query_cols, 128), query_cols)],
        out_full.at[pl.ds(pl.multiple_of(f * out_cols, 16), out_cols)],
    )

    def cross_part(m, j):
        if m == 0:
            return cross_qkv.at[j]
        return cross_out.at[j, pl.ds(0, (small, big)[j] // 2)]

    out_cross = []
    for j in range(2):
        start, size = out_rows(y, 1 - j, core)
        out_cross.append(
            local(
                out_weight.at[
                    pl.ds(pl.multiple_of(start, 16), size),
                    pl.ds(pl.multiple_of(across_team * query_cols, 128), query_cols),
                ],
                cross_part(1, j),
            )
        )
    small_loads = [
        local(source, dest)
        for source, dest in (
            (pair_weight_one, pair_weight),
            (partner_all, partner),
            (cosine_table, cosine),
            (sine_table, sine),
        )
    ]
    everyone = shards * groups
    me = f * groups + g

    pl.semaphore_wait(barrier, 4 + has_up.astype(jnp.int32) + has_down.astype(jnp.int32))

    def way_copy(way, m, s, piece):
        return pltpu.make_async_remote_copy(
            src_ref=slot(m, s, piece, core),
            dst_ref=slot(m, s, piece, core),
            send_sem=send_sem.at[way, m],
            recv_sem=recv_sem.at[m, s, piece, core],
            device_id=way_ids[way],
        )

    def piece_of(m, o, j):
        return 1 - j if m == 1 and o == 1 else j

    def cross_copy(m, j):
        piece = piece_of(m, 1, j)
        return pltpu.make_async_remote_copy(
            src_ref=cross_part(m, j),
            dst_ref=slot(m, f, piece, core),
            send_sem=cross_send.at[m],
            recv_sem=recv_sem.at[m, f, piece, core],
            device_id=team_ids[1],
        )

    def arrived(m, s, piece, half):
        there = slot(m, s, piece, half)
        pltpu.make_async_copy(there, there, recv_sem.at[m, s, piece, half]).wait()

    def send_both(m, s, piece):
        pl.when(has_up)(way_copy(UP, m, s, piece).start)
        pl.when(has_down)(way_copy(DOWN, m, s, piece).start)

    def cross_step(m, j):
        piece = piece_of(m, 1, j)
        arrived(m, across, piece, core)
        send_both(m, across, piece)
        way_copy(PARTNER, m, across, piece).start()

    def sides(k, o):
        row = y if o == 0 else 1 - y
        below, above = z - k, z + k
        return (
            (below >= 0, 2 * jnp.maximum(below, 0) + row, UP, has_up),
            (above < line, 2 * jnp.minimum(above, line - 1) + row, DOWN, has_down),
        )

    def line_step(m, k, o, j):
        piece = piece_of(m, o, j)
        for ok, s, way, onward in sides(k, o):
            if m == 1:
                onward = onward & (k < line - 2)

            @pl.when(ok)
            def _():
                arrived(m, s, piece, core)
                pl.when(onward)(way_copy(way, m, s, piece).start)
                way_copy(PARTNER, m, s, piece).start()

    def from_partner(m, s):
        for piece in range(2):
            arrived(m, s, piece, 1 - core)

    tok_starts = (0, seq_rows // 4, seq_rows * 5 // 8, seq_rows)

    def tok_copy(way, piece):
        source = 0 if way < 2 else (1, 2, 2)[piece]
        target = team_ids[way] if way < 2 else team_ids[(1, 0, 0)[piece]]
        start, size = tok_starts[piece], tok_starts[piece + 1] - tok_starts[piece]
        return pltpu.make_async_remote_copy(
            src_ref=normed.at[pl.ds(source * seq_rows + start, size)],
            dst_ref=normed.at[pl.ds((1 + way) * seq_rows + start, size)],
            send_sem=tok_send.at[way],
            recv_sem=tok_recv.at[way, piece],
            device_id=target,
        )

    def len_copy(way):
        return pltpu.make_async_remote_copy(
            src_ref=len_tile,
            dst_ref=len_all.at[1 + way],
            send_sem=len_sem.at[0],
            recv_sem=len_sem.at[1],
            device_id=team_ids[way],
        )

    for j in range(2):
        own_loads[j].wait()
        send_both(0, f, j)
        cross_loads[j].wait()
        cross_copy(0, j).start()

    tok_local.wait()
    for copy in vectors:
        copy.wait()
    norm_rows = 16

    @pl.loop(0, seq_rows // norm_rows)
    def _(i):
        at = pl.ds(pl.multiple_of(i * norm_rows, norm_rows), norm_rows)
        rows = tok_own[at, :].astype(jnp.float32)
        scale = lax.rsqrt(jnp.mean(rows * rows, axis=-1, keepdims=True) + 1e-06)
        normed[at, :] = (rows * scale * norm_gain[...]).astype(jnp.bfloat16)

    for first, second in ((0, 1), (1, 2), (2, 0)):
        tok_copy(0, first).start()
        tok_copy(1, second).start()
    length_load.wait()
    len_tile[...] = jnp.full(len_tile.shape, length[0, 0], jnp.int32)
    len_all[0] = len_tile[...]
    for way in range(3):
        len_copy(way).start()

    bias_parts = (
        (team * query_cols, query_cols, 0),
        (QUERY_FEATURES + team * key_cols, key_cols, query_cols),
        (QUERY_FEATURES + KEY_FEATURES + team * key_cols, key_cols, query_cols + key_cols),
    )
    for start, size, to in bias_parts:
        qkv_rows[:, to : to + size] = jnp.broadcast_to(
            qkv_bias[:, pl.ds(pl.multiple_of(start, HEAD_SIZE), size)],
            (groups * seq_rows, size),
        )

    for j in range(2):
        cross_step(0, j)
        line_step(0, 1, 0, j)
    tok_copy(0, 0).wait_recv()
    tok_copy(2, 0).start()
    out_own.wait()
    for j in range(2):
        out_cross[j].wait()
        cross_copy(1, j).start()
    for j in range(2):
        line_step(0, 1, 1, j)
        tok_copy(1, 1 + j).wait_recv()
        tok_copy(2, 1 + j).start()
    steps = [(k, o, j) for k in range(2, line - 1) for o in range(2) for j in range(2)]
    for k, o, j in steps[:-1]:
        line_step(0, k, o, j)

    for way, piece in ((0, 1), (0, 2), (1, 0), (2, 0), (2, 1), (2, 2)):
        tok_copy(way, piece).wait_recv()
    bytes_of(len_all.at[pl.ds(1, 3)], len_sem.at[1]).wait()
    for copy in (*late_loads, *small_loads):
        copy.wait()

    @pl.loop(0, everyone)
    def _(i):
        partner_rows[pl.ds(i, 1), :] = jnp.full((1, HEAD_SIZE), partner[i], jnp.int32)

    def qkv_step(place):
        rows = pl.ds(pl.multiple_of(place * 2 * depth, 128), 2 * depth)

        qkv_rows[...] += jnp.dot(
            normed[:, rows], qkv_full[rows, :], preferred_element_type=jnp.float32
        )

    def qkv_places(first, last):
        @pl.loop(2 * first, 2 * last)
        def _(i):
            k = i // 2
            place = z + (2 * lax.rem(i, 2) - 1) * k

            @pl.when((place >= 0) & (place < line))
            def _():
                from_partner(0, 2 * place)
                from_partner(0, 2 * place + 1)
                qkv_step(place)

    @pl.loop(0, 1)
    def _(i):
        from_partner(0, across)
        qkv_step(z)

    qkv_places(1, 2)
    line_step(0, *steps[-1])
    for j in range(2):
        send_both(1, f, j)
    qkv_places(2, line - 1)
    for j in range(2):
        cross_step(1, j)
    for o in range(2):
        for j in range(2):
            line_step(0, line - 1, o, j)
    qkv_places(line - 1, line)

    def head_rows(j, column):
        return qkv_rows[
            pl.ds(pl.multiple_of(j * seq_rows, seq_rows), seq_rows), column : column + HEAD_SIZE
        ]

    def rotate(rows):
        return (
            rows * cosine[...] + pltpu.roll(rows, HEAD_SIZE // 2, 1) * sine[...]
        ).astype(jnp.bfloat16)

    key_heads = key_cols // HEAD_SIZE
    share = heads // key_heads

    def lanes_of(at, size):
        return pl.ds(pl.multiple_of(at, HEAD_SIZE), size)

    units = ((0, big), (big, 2 * small), (pair - big, big))

    def part_copy(way, place, at, size, unit):
        cols = lanes_of(at, size)
        return pltpu.make_async_remote_copy(
            src_ref=part_out.at[place, pl.ds((1 + way) * seq_rows, seq_rows), cols],
            dst_ref=part_in.at[way, place, :, cols],
            send_sem=part_send.at[way],
            recv_sem=part_recv.at[way, place],
            device_id=team_ids[way],
        )

    def project(place, at, size, unit):
        cols = lanes_of(at, size)
        result = lax.dot_general(
            attn[...],
            out_full[lanes_of(place * pair + at, size), :],
            (((1,), (1,)), ((), ())),
            preferred_element_type=jnp.float32,
        )
        part_out[place, :, cols] = result.astype(jnp.bfloat16)
        own[place, :, cols] = result[:seq_rows]
        for way in (2, 0, 1):
            part_copy(way, place, at, size, unit).start()

    def attn_copy(j):
        rows = pl.ds(pl.multiple_of(j * seq_rows, seq_rows), seq_rows)
        return pltpu.make_async_remote_copy(
            src_ref=attn.at[rows],
            dst_ref=attn_help.at[rows],
            send_sem=attn_send.at[0],
            recv_sem=attn_recv.at[j],
            device_id=end_to_helper,
        )

    @pl.loop(0, groups)
    def _(i):
        j = groups - 1 - i
        query_place = lax.broadcasted_iota(jnp.int32, (seq_rows, seq_rows), 0)
        key_place = lax.broadcasted_iota(jnp.int32, (seq_rows, seq_rows), 1)
        allowed = (key_place <= query_place) & (key_place < len_all[j, 0:1, :])
        at = pl.ds(pl.multiple_of(j * seq_rows, seq_rows), seq_rows)
        for kh in range(key_heads):
            offset = kh * HEAD_SIZE
            group = [slice(h * HEAD_SIZE, (h + 1) * HEAD_SIZE) for h in range(share)]
            first = kh * share * HEAD_SIZE
            key = rotate(head_rows(j, query_cols + offset))
            value = head_rows(j, query_cols + key_cols + offset).astype(jnp.bfloat16)
            for lanes in group:
                queries[lanes, :] = rotate(head_rows(j, first + lanes.start))
            score_rows[...] = lax.dot_general(
                queries[...], key, (((1,), (1,)), ((), ())), preferred_element_type=jnp.float32
            )
            for lanes in group:
                scores = score_rows[lanes, :] * np.float32(1 / np.sqrt(HEAD_SIZE))
                scores = jnp.where(allowed, scores, jnp.float32(-1e30))
                expd = jnp.exp(scores - jnp.max(scores, axis=-1, keepdims=True))
                inverse = 1.0 / jnp.sum(expd, axis=-1, keepdims=True)
                queries[lanes, :] = (expd * inverse).astype(jnp.bfloat16)
            mixed = jnp.dot(queries[...], value, preferred_element_type=jnp.float32)
            for lanes in group:
                attn[at, first + lanes.start : first + lanes.stop] = mixed[lanes].astype(
                    jnp.bfloat16
                )
        pl.when(is_end)(attn_copy(j).start)

        @pl.when(i == 0)
        def _():
            from_partner(1, across)

        result = lax.dot_general(
            attn[at, :],
            out_full[lanes_of(z * pair, pair), :],
            (((1,), (1,)), ((), ())),
            preferred_element_type=jnp.float32,
        )
        part_out[z, at, :] = result.astype(jnp.bfloat16)
        own[z] = result
        for way in range(3):
            pl.when(j == way + 1)(part_copy(way, z, 0, pair, 0).start)

    def project_pair(place):
        @pl.loop(0, 2)
        def _(i):
            project(place, i * (pair - big), big, 2 * i)

        project(place, big, 2 * small, 1)

    place = lax.broadcasted_iota(jnp.int32, len_tile.shape, 1)
    pick = (place == len_tile[...] - 1).astype(jnp.bfloat16)
    stats[...] = jnp.zeros_like(stats)

    def finish(place, sums):
        cols = lanes_of(place * pair, pair)
        hidden[:, cols] = (tok_own[:, cols].astype(jnp.float32) + sums).astype(jnp.bfloat16)
        last = jnp.dot(pick, hidden[:, cols], preferred_element_type=jnp.float32)
        weighted = last * final_gain[:, cols] * value_head[:, cols]
        squares = last * last
        for t in range(pair // HEAD_SIZE):
            lanes = slice(t * HEAD_SIZE, (t + 1) * HEAD_SIZE)
            stats[0] += squares[:, lanes]
            stats[1] += weighted[:, lanes]

    def finish_parts(place):
        for way in range(3):
            bytes_of(part_in.at[way, place], part_recv.at[way, place]).wait()
        total = own[place]
        for way in range(3):
            total += part_in[way, place].astype(jnp.float32)
        finish(place, total)

    def at_sides(k, body):
        @pl.loop(0, 2)
        def _(i):
            place = z + (2 * i - 1) * k

            @pl.when((place >= 0) & (place < line) & ((k > 0) | (i == 0)))
            def _():
                body(place)

    def own_unit(place):
        arrived(1, 2 * place + y, 0, 1 - core)
        project(place, y * (pair - big), big, 2 * y)

    def mid_unit(place):
        arrived(1, 2 * place + y, 1, 1 - core)
        arrived(1, 2 * place + 1 - y, 1, 1 - core)
        project(place, big, 2 * small, 1)

    def cross_unit(place):
        arrived(1, 2 * place + 1 - y, 0, 1 - core)
        project(place, (1 - y) * (pair - big), big, 2 * (1 - y))

    @pl.loop(1, line - 1)
    def _(k):
        mine = jnp.logical_not(is_helper) | (k < line - 2)
        line_step(1, k, 0, 0)
        line_step(1, k, 0, 1)

        @pl.when(mine)
        def _():
            at_sides(k, own_unit)

        @pl.when(jnp.logical_not(is_helper))
        def _():
            at_sides(k - 1, finish_parts)

        line_step(1, k, 1, 0)

        @pl.when(mine)
        def _():
            at_sides(k, mid_unit)

        line_step(1, k, 1, 1)

        @pl.when(mine)
        def _():
            at_sides(k, cross_unit)

    def help_part(way):
        return pltpu.make_async_remote_copy(
            src_ref=help_out.at[1 + way],
            dst_ref=help_in.at[way],
            send_sem=help_send.at[0],
            recv_sem=help_recv.at[way],
            device_id=team_ids[way],
        )

    done_copy = pltpu.make_async_remote_copy(
        src_ref=help_sum,
        dst_ref=help_done,
        send_sem=done_sem.at[0],
        recv_sem=done_sem.at[1],
        device_id=helper_to_end,
    )

    @pl.when(is_helper)
    def _():
        for o in range(2):
            from_partner(1, 2 * far + o)

        @pl.loop(0, groups)
        def _(i):
            j = groups - 1 - i
            rows = pl.ds(pl.multiple_of(j * seq_rows, seq_rows), seq_rows)
            pltpu.make_async_copy(attn_help.at[rows], attn_help.at[rows], attn_recv.at[j]).wait()
            result = lax.dot_general(
                attn_help[rows, :],
                out_full[lanes_of(far * pair, pair), :],
                (((1,), (1,)), ((), ())),
                preferred_element_type=jnp.float32,
            )
            help_own[...] = result
            help_out[j] = result.astype(jnp.bfloat16)
            for way in range(3):
                pl.when(j == way + 1)(help_part(way).start)

        project_pair(far)

        @pl.loop(0, line)
        def _(place):
            pl.when(place != far)(lambda: finish_parts(place))

        for way in range(3):
            help_part(way).wait_recv()
        total = help_own[...]
        for way in range(3):
            total += help_in[way].astype(jnp.float32)
        help_sum[...] = total.astype(jnp.bfloat16)
        done_copy.start()

    @pl.when(is_end)
    def _():
        at_sides(line - 2, finish_parts)
        done_copy.wait_recv()
        finish(far, help_done[...].astype(jnp.float32))

    @pl.when(is_helper)
    def _():
        finish_parts(far)

    mean = jnp.sum(stats[0], axis=-1, keepdims=True) / width
    score = jnp.sum(stats[1], axis=-1, keepdims=True) * lax.rsqrt(mean + 1e-06)
    first_row = lax.broadcasted_iota(jnp.int32, score_tile.shape, 0) == 0
    score_tile[...] = jnp.where(first_row, score, jnp.full(score_tile.shape, pair_weight[0, 0]))
    score_all[me] = score_tile[...]

    def score_copy(i):
        other = lax.rem(me + i, everyone)
        return pltpu.make_async_remote_copy(
            src_ref=score_tile,
            dst_ref=score_all.at[me],
            send_sem=score_sem.at[0],
            recv_sem=score_sem.at[1],
            device_id={"fsdp": other // groups, "dp": lax.rem(other, groups)},
        )

    @pl.loop(1, everyone)
    def _(i):
        score_copy(i).start()

    bytes_of(cross_qkv, cross_send.at[0]).wait()
    bytes_of(out_full.at[pl.ds(0, out_cols // 2)], cross_send.at[1]).wait()
    bytes_of(len_all.at[pl.ds(1, 3)], len_sem.at[0]).wait()
    for way in range(3):
        bytes_of(normed.at[pl.ds(0, seq_rows)], tok_send.at[way]).wait()
    for spot in range(line):
        ends = spot in (0, line - 1)
        up = 0 if spot == line - 1 else 2 * (spot + 1)
        down = 0 if spot == 0 else 2 * (line - spot)
        sent = (
            (UP, up, up - 2 * (spot == line - 2)),
            (DOWN, down, down - 2 * (spot == 1)),
            (PARTNER, shards - 1, shards - 1 - 2 * ends),
        )

        @pl.when(z == spot)
        def _():
            for way, slices, out_slices in sent:
                if slices:
                    rows = pl.ds(0, slices * depth // 2)
                    bytes_of(qkv_full.at[rows], send_sem.at[way, 0]).wait()
                    rows = pl.ds(0, out_slices * out_cols // 2)
                    bytes_of(out_full.at[rows], send_sem.at[way, 1]).wait()
            for way in range(3):
                bytes_of(part_in.at[0, pl.ds(0, line - ends)], part_send.at[way]).wait()
            if ends:
                bytes_of(attn, attn_send.at[0]).wait()

    @pl.when(is_helper)
    def _():
        bytes_of(help_in, help_send.at[0]).wait()
        done_copy.wait_send()

    bytes_of(score_all.at[pl.ds(0, everyone - 1)], score_sem.at[1]).wait()

    scores = score_all[:, 0, :]
    weights = score_all[:, 1, :]
    row = lax.broadcasted_iota(jnp.int32, scores.shape, 0)
    lane = lax.broadcasted_iota(jnp.int32, scores.shape, 1)
    partners = partner_rows[...]
    score_row = jnp.sum(jnp.where(row == lane, scores, 0.0), axis=0, keepdims=True)
    others = jnp.sum(jnp.where(partners == lane, score_row, 0.0), axis=1, keepdims=True)
    margins = jnp.where(row < partners, scores - others, others - scores)
    softplus = jnp.maximum(-margins, 0.0) + jnp.log1p(jnp.exp(-jnp.abs(margins)))
    first_lane = lane == 0
    margin = jnp.sum(jnp.where(first_lane & (row == me), margins, 0.0))
    loss = jnp.sum(jnp.where(first_lane, weights * softplus, 0.0)) / everyone
    results[...] = jnp.where(first_row, jnp.full(results.shape, margin), loss)
    bytes_of(score_all.at[pl.ds(0, everyone - 1)], score_sem.at[0]).wait()


def layer_fits(shards, groups, tokens, qkv_weight, out_weight):
    return (
        shards % 2 == 0
        and shards >= 8
        and qkv_weight.shape[0] % 64 == 0
        and groups == 4
        and KEY_VALUE_HEADS % groups == 0
        and tokens.shape[1] == HEAD_SIZE
        and shards * groups <= HEAD_SIZE
        and out_weight.shape[1] % 64 == 0
        and out_weight.shape[1] > HEAD_SIZE
    )


def layer(
    tokens,
    lengths,
    partner,
    pair_weight,
    norm_gain,
    qkv_weight,
    qkv_bias,
    out_weight,
    final_gain,
    value_head,
):
    shards, groups = lax.axis_size("fsdp"), lax.axis_size("dp")
    _, seq_rows, width = tokens.shape
    depth = qkv_weight.shape[0]
    out_cols = out_weight.shape[1]
    query_cols = QUERY_FEATURES // groups
    key_cols = KEY_FEATURES // groups
    all_cols = query_cols + 2 * key_cols
    rows = groups * seq_rows
    line, pair = shards // 2, 2 * out_cols
    cosine, sine = rotary_tables(seq_rows)
    everyone = shards * groups
    dma = pltpu.SemaphoreType.DMA
    vmem = pl.BlockSpec(memory_space=pltpu.VMEM)
    bf16, f32 = jnp.bfloat16, jnp.float32
    hidden, results = pl.pallas_call(
        functools.partial(layer_kernel, shards, groups),
        out_shape=(
            pltpu.VMEM((seq_rows, width), bf16),
            pltpu.VMEM((8, HEAD_SIZE), f32),
        ),
        in_specs=[pl.BlockSpec(memory_space=pltpu.HBM)] * 12,
        out_specs=(vmem, vmem),
        scratch_shapes=[
            pltpu.VMEM((shards * depth, all_cols), bf16),
            pltpu.VMEM((shards * out_cols, query_cols), bf16),
            pltpu.VMEM((2, depth // 4, all_cols), bf16),
            pltpu.VMEM((2, out_pieces(out_cols)[0] // 2, query_cols), bf16),
            pltpu.VMEM((seq_rows, width), bf16),
            pltpu.VMEM((8, seq_rows), jnp.int32),
            pltpu.VMEM((groups, 8, seq_rows), jnp.int32),
            pltpu.VMEM((rows, width), bf16),
            pltpu.VMEM((rows, all_cols), f32),
            pltpu.VMEM((rows, query_cols), bf16),
            pltpu.VMEM((line, seq_rows, pair), f32),
            pltpu.VMEM((line, rows, pair), bf16),
            pltpu.VMEM((groups - 1, line, seq_rows, pair), bf16),
            pltpu.VMEM((rows, query_cols), bf16),
            pltpu.VMEM((seq_rows, pair), f32),
            pltpu.VMEM((groups, seq_rows, pair), bf16),
            pltpu.VMEM((groups - 1, seq_rows, pair), bf16),
            pltpu.VMEM((seq_rows, pair), bf16),
            pltpu.VMEM((seq_rows, pair), bf16),
            pltpu.VMEM((2, 8, HEAD_SIZE), f32),
            pltpu.VMEM((query_cols * HEAD_SIZE // key_cols, HEAD_SIZE), bf16),
            pltpu.VMEM((query_cols * HEAD_SIZE // key_cols, HEAD_SIZE), f32),
            pltpu.VMEM((8, HEAD_SIZE), f32),
            pltpu.VMEM((everyone, 8, HEAD_SIZE), f32),
            pltpu.VMEM((everyone, HEAD_SIZE), jnp.int32),
            pltpu.VMEM((1, width), f32),
            pltpu.VMEM((1, width + 8 * HEAD_SIZE), f32),
            pltpu.VMEM((1, width + 8 * HEAD_SIZE), f32),
            pltpu.VMEM((1, qkv_bias.shape[0] + 8 * HEAD_SIZE), f32),
            pltpu.VMEM((seq_rows, HEAD_SIZE), f32),
            pltpu.VMEM((seq_rows, HEAD_SIZE), f32),
            pltpu.SMEM((1, 1), jnp.int32),
            pltpu.SMEM((1, 1), f32),
            pltpu.SMEM((everyone,), jnp.int32),
            dma((19,)),
            dma((2, shards, 2, 2)),
            dma((3, 2)),
            dma((2,)),
            dma((3,)),
            dma((3, 3)),
            dma((2,)),
            dma((3,)),
            dma((3, line)),
            dma((1,)),
            dma((groups,)),
            dma((1,)),
            dma((3,)),
            dma((2,)),
            dma((2,)),
        ],
        compiler_params=pltpu.CompilerParams(
            collective_id=0, has_side_effects=True, vmem_limit_bytes=56 * 1024 * 1024
        ),
    )(
        tokens[0],
        qkv_weight,
        out_weight.T,
        lengths[None],
        pair_weight[None],
        partner,
        norm_gain,
        final_gain,
        value_head,
        qkv_bias,
        jnp.asarray(cosine),
        jnp.asarray(sine),
    )
    return hidden[None], results[0, :1], results[1, 0]


def projected_by_gathers(
    tokens,
    lengths,
    norm_gain,
    qkv_weight,
    qkv_bias,
    out_weight,
):
    sequence = tokens[0]
    length_rows = sequence.shape[0]
    width = sequence.shape[1]
    normed = rms_scale(sequence.astype(jnp.float32), norm_gain).astype(jnp.bfloat16)
    query_group_count = lax.axis_size("dp")
    group_index = lax.axis_index("dp")
    query_heads = QUERY_HEADS // query_group_count
    key_value_heads = KEY_VALUE_HEADS // query_group_count
    query_cols = query_heads * HEAD_SIZE
    key_cols = key_value_heads * HEAD_SIZE
    group_normed, group_lengths = (
        lax.all_gather(normed[None], "dp", axis=0, tiled=True),
        lax.all_gather(lengths, "dp", axis=0, tiled=True),
    )
    seq_count = group_normed.shape[0]
    flat = group_normed.reshape(seq_count * length_rows, width)
    qkv_cols = jnp.concatenate(
        [
            lax.dynamic_slice_in_dim(qkv_weight, group_index * query_cols, query_cols, 1),
            lax.dynamic_slice_in_dim(
                qkv_weight, QUERY_FEATURES + group_index * key_cols, key_cols, 1
            ),
            lax.dynamic_slice_in_dim(
                qkv_weight, QUERY_FEATURES + KEY_FEATURES + group_index * key_cols, key_cols, 1
            ),
        ],
        axis=1,
    )
    bias_cols = jnp.concatenate(
        [
            lax.dynamic_slice_in_dim(qkv_bias, group_index * query_cols, query_cols, 0),
            lax.dynamic_slice_in_dim(
                qkv_bias, QUERY_FEATURES + group_index * key_cols, key_cols, 0
            ),
            lax.dynamic_slice_in_dim(
                qkv_bias, QUERY_FEATURES + KEY_FEATURES + group_index * key_cols, key_cols, 0
            ),
        ],
        axis=0,
    )
    out_rows = lax.dynamic_slice_in_dim(out_weight, group_index * query_cols, query_cols, 0)
    qkv_full, out_full = (
        lax.all_gather(qkv_cols, "fsdp", axis=0, tiled=True),
        lax.all_gather(out_rows, "fsdp", axis=1, tiled=True),
    )
    query_key_value = jnp.dot(flat, qkv_full, preferred_element_type=jnp.float32) + bias_cols
    attn = attend(
        query_key_value.reshape(seq_count, length_rows, -1),
        group_lengths,
        query_heads,
        key_value_heads,
    )
    return lax.psum_scatter(
        jnp.dot(attn, out_full, preferred_element_type=jnp.float32),
        "dp",
        scatter_dimension=0,
        tiled=True,
    )


def per_device(
    tokens,
    lengths,
    partner,
    pair_weight,
    norm_gain,
    qkv_weight,
    qkv_bias,
    out_weight,
    final_gain,
    value_head,
):
    if layer_fits(lax.axis_size("fsdp"), lax.axis_size("dp"), tokens, qkv_weight, out_weight):
        return layer(
            tokens,
            lengths,
            partner,
            pair_weight,
            norm_gain,
            qkv_weight,
            qkv_bias,
            out_weight,
            final_gain,
            value_head,
        )
    sequence = tokens[0]
    length = lengths[0]
    projected = projected_by_gathers(tokens, lengths, norm_gain, qkv_weight, qkv_bias, out_weight)
    hidden = (sequence.astype(jnp.float32) + projected).astype(jnp.bfloat16)
    last = lax.dynamic_slice_in_dim(hidden, length - 1, 1, 0)[0].astype(jnp.float32)
    score = jnp.sum(rms_scale(last, final_gain) * value_head)
    everyone, weights_all = (
        lax.all_gather(score.reshape(1), ("fsdp", "dp"), axis=0, tiled=True),
        lax.all_gather(pair_weight, ("fsdp", "dp"), axis=0, tiled=True),
    )
    total_seqs = everyone.shape[0]
    mine = lax.axis_index(("fsdp", "dp"))
    index_all = jnp.arange(total_seqs, dtype=jnp.int32)
    my_partner = jnp.sum(jnp.where(index_all == mine, partner, 0))
    other = jnp.sum(jnp.where(index_all == my_partner, everyone, jnp.float32(0.0)))
    margin = jnp.where(mine < my_partner, score - other, other - score)
    matches = partner[:, None] == index_all[None, :]
    others_all = jnp.sum(jnp.where(matches, everyone[None, :], jnp.float32(0.0)), axis=1)
    margins_all = jnp.where(index_all < partner, everyone - others_all, others_all - everyone)
    loss = jnp.sum(weights_all * jax.nn.softplus(-margins_all)) / total_seqs
    return (hidden[None], margin.reshape(1), loss)


def solution(mesh):
    return jax.shard_map(
        per_device,
        mesh=mesh,
        in_specs=(
            P(("fsdp", "dp"), None, None),
            P(("fsdp", "dp")),
            P(),
            P(("fsdp", "dp")),
            P(),
            P("fsdp", None),
            P(),
            P(None, "fsdp"),
            P(),
            P(),
        ),
        out_specs=(P(("fsdp", "dp"), None, None), P(("fsdp", "dp")), P()),
        check_vma=False,
    )
```

```python
import functools

import jax
import jax.numpy as jnp
import numpy as np
from jax import lax
from jax.experimental import pallas as pl
from jax.experimental.pallas import tpu as pltpu
from jax.sharding import PartitionSpec as P

QUERY_HEADS = 28
KEY_VALUE_HEADS = 4
HEAD_SIZE = 128
QUERY_FEATURES = 3584
KEY_FEATURES = 512


def rms_scale(value_rows, gain):
    return (
        value_rows
        * lax.rsqrt(jnp.mean(value_rows * value_rows, axis=-1, keepdims=True) + 1e-06)
        * gain
    )


def apply_rotary(heads, length_rows):
    half = HEAD_SIZE // 2
    positions = jnp.arange(length_rows, dtype=jnp.float32)
    freqs = jnp.exp(
        -(2.0 * jnp.arange(half, dtype=jnp.float32) / HEAD_SIZE) * jnp.log(jnp.float32(1000000.0))
    )
    angles = positions[:, None] * freqs[None, :]
    cosine = jnp.cos(angles)
    sine = jnp.sin(angles)
    first = heads[..., :half]
    second = heads[..., half:]
    return jnp.concatenate(
        [first * cosine - second * sine, second * cosine + first * sine], axis=-1
    )


def attend(query_key_value, group_lengths, query_heads, key_value_heads):
    seq_count, length_rows, _ = query_key_value.shape
    query_width = query_heads * HEAD_SIZE
    key_width = key_value_heads * HEAD_SIZE
    query_rows = (
        query_key_value[..., :query_width]
        .reshape(seq_count, length_rows, query_heads, HEAD_SIZE)
        .transpose(0, 2, 1, 3)
    )
    key_rows = (
        query_key_value[..., query_width : query_width + key_width]
        .reshape(seq_count, length_rows, key_value_heads, HEAD_SIZE)
        .transpose(0, 2, 1, 3)
    )
    value_rows = (
        query_key_value[..., query_width + key_width :]
        .reshape(seq_count, length_rows, key_value_heads, HEAD_SIZE)
        .transpose(0, 2, 1, 3)
        .astype(jnp.bfloat16)
    )
    query_rows = (
        apply_rotary(query_rows, length_rows)
        .astype(jnp.bfloat16)
        .reshape(seq_count, key_value_heads, query_heads // key_value_heads, length_rows, HEAD_SIZE)
    )
    key_rows = apply_rotary(key_rows, length_rows).astype(jnp.bfloat16)
    scores = jnp.einsum(
        "bgqtd,bgsd->bgqts", query_rows, key_rows, preferred_element_type=jnp.float32
    ) / jnp.sqrt(jnp.float32(HEAD_SIZE))
    places = jnp.arange(length_rows, dtype=jnp.int32)
    causal = places[None, :] <= places[:, None]
    usable = places[None, :] < group_lengths[:, None]
    allowed = causal[None, :, :] & usable[:, None, :]
    scores = jnp.where(allowed[:, None, None, :, :], scores, jnp.float32(-1e30))
    highest = jnp.max(scores, axis=-1, keepdims=True)
    expd = jnp.exp(scores - highest)
    probs = (expd / jnp.sum(expd, axis=-1, keepdims=True)).astype(jnp.bfloat16)
    mixed = jnp.einsum("bgqts,bgsd->bgqtd", probs, value_rows, preferred_element_type=jnp.float32)
    mixed = mixed.reshape(seq_count, query_heads, length_rows, HEAD_SIZE).transpose(0, 2, 1, 3)
    return mixed.reshape(seq_count * length_rows, query_width).astype(jnp.bfloat16)


UP, DOWN, PARTNER = 0, 1, 2


def rotary_tables(length_rows):
    half = HEAD_SIZE // 2
    freqs = 1000000.0 ** (-2.0 * np.arange(half) / HEAD_SIZE)
    angles = np.arange(length_rows)[:, None] * freqs[None, :]
    cosine, sine = np.cos(angles), np.sin(angles)
    return (
        np.concatenate([cosine, cosine], axis=1).astype(np.float32),
        np.concatenate([-sine, sine], axis=1).astype(np.float32),
    )


def out_pieces(out_cols):
    big = (out_cols // 2 + HEAD_SIZE - 1) // HEAD_SIZE * HEAD_SIZE
    return big, out_cols - big


def layer_kernel(
    shards,
    groups,
    tokens,
    qkv_weight,
    out_weight,
    length_one,
    pair_weight_one,
    partner_all,
    norm_gain_flat,
    final_gain_flat,
    value_head_flat,
    qkv_bias_flat,
    cosine_table,
    sine_table,
    hidden,
    results,
    qkv_full,
    out_full,
    cross_qkv,
    cross_out,
    tok_own,
    len_tile,
    len_all,
    normed,
    qkv_rows,
    attn,
    own,
    part_out,
    part_in,
    attn_help,
    help_own,
    help_out,
    help_in,
    help_sum,
    help_done,
    stats,
    queries,
    score_rows,
    score_tile,
    score_all,
    partner_rows,
    norm_gain,
    final_gain,
    value_head,
    qkv_bias,
    cosine,
    sine,
    length,
    pair_weight,
    partner,
    local_sem,
    qkv_recv,
    out_recv,
    send_sem,
    cross_send,
    tok_send,
    tok_recv,
    len_sem,
    part_send,
    part_recv,
    attn_send,
    attn_recv,
    help_send,
    help_recv,
    done_sem,
    score_sem,
):
    line = shards // 2
    f = lax.axis_index("fsdp")
    g = lax.axis_index("dp")
    z = f // 2
    y = f % 2
    x = g // 2
    core = g % 2
    seq_rows = tokens.shape[0]
    width = tokens.shape[1]
    depth = qkv_weight.shape[0]
    out_cols = out_weight.shape[0]
    query_cols = QUERY_FEATURES // groups
    key_cols = KEY_FEATURES // groups
    heads = query_cols // HEAD_SIZE
    quarter = depth // 4
    pair = 2 * out_cols
    big, small = out_pieces(out_cols)
    is_end = (z == 0) | (z == line - 1)
    is_helper = (z == 1) | (z == line - 2)
    far = jnp.where((z == 0) | (z == 1), line - 1, 0)
    end_to_helper = {"fsdp": jnp.where(z == 0, f + 2, f - 2)}
    helper_to_end = {"fsdp": jnp.where(z == 1, f - 2, f + 2)}
    has_up = z < line - 1
    has_down = z > 0
    team = 2 * x + y
    across_team = 2 * x + 1 - y
    across = 2 * z + 1 - y
    x_peer = 2 * (1 - x) + core
    team_ids = ({"dp": x_peer}, {"fsdp": across}, {"fsdp": across, "dp": x_peer})
    way_ids = ({"fsdp": f + 2}, {"fsdp": f - 2}, {"dp": 2 * x + 1 - core})

    barrier = pltpu.get_barrier_semaphore()
    for target in (*team_ids, way_ids[PARTNER]):
        pl.semaphore_signal(barrier, inc=1, device_id=target)
    for way, ok in ((UP, has_up), (DOWN, has_down)):

        @pl.when(ok)
        def _():
            pl.semaphore_signal(barrier, inc=1, device_id=way_ids[way])

    piece_sizes = (big, small, big // 2, big // 2)
    pieces = (((0, 1), (0, 1)), ((0, 1), (1, 2, 3)))

    def out_rows(side, piece, half):
        size = piece_sizes[piece] // 2
        start = (
            side * small,
            (1 - side) * big,
            (1 - side) * (big // 2) + side * small,
            side * (small + big // 2),
        )[piece]
        return start + half * size, size

    def slot(m, s, piece, half):
        if m == 0:
            start = s * depth + (2 * piece + half) * quarter
            return qkv_full.at[pl.ds(pl.multiple_of(start, 16), quarter)]
        start, size = out_rows(lax.rem(s, 2), piece, half)
        return out_full.at[pl.ds(pl.multiple_of(s * out_cols + start, 16), size)]

    def recv_of(m, s, piece, by_partner):
        if m == 0:
            return qkv_recv.at[s, 2 if by_partner else piece]
        return out_recv.at[s, (0, 1, 0, 2)[piece], by_partner]

    count = 0

    def local(source, dest):
        nonlocal count
        copy = pltpu.make_async_copy(source, dest, local_sem.at[count])
        count += 1
        copy.start()
        return copy

    def bytes_of(ref, sem):
        return pltpu.make_async_copy(ref, ref, sem)

    def qkv_parts(piece, half, owner, dest):
        nonlocal count
        rows = pl.ds(pl.multiple_of((2 * piece + half) * quarter, 16), quarter)
        for start, size, to in (
            (owner * query_cols, query_cols, 0),
            (QUERY_FEATURES + owner * key_cols, key_cols, query_cols),
            (QUERY_FEATURES + KEY_FEATURES + owner * key_cols, key_cols, query_cols + key_cols),
        ):
            pltpu.make_async_copy(
                qkv_weight.at[rows, pl.ds(pl.multiple_of(start, 128), size)],
                dest.at[:, pl.ds(to, size)],
                local_sem.at[count],
            ).start()
        count += 1
        return bytes_of(dest, local_sem.at[count - 1])

    length_load = local(length_one, length)
    own_loads, cross_loads = [], []
    for j in range(2):
        own_loads.append(qkv_parts(j, core, team, slot(0, f, j, core)))
        cross_loads.append(qkv_parts(j, core, across_team, cross_qkv.at[j]))
    tok_local = local(tokens, tok_own)
    vectors = [
        local(flat, row.at[0, pl.ds(0, flat.shape[0])])
        for flat, row in (
            (norm_gain_flat, norm_gain),
            (final_gain_flat, final_gain),
            (value_head_flat, value_head),
            (qkv_bias_flat, qkv_bias),
        )
    ]
    late_loads = []
    for j in range(2):
        late_loads.append(qkv_parts(j, 1 - core, team, slot(0, f, j, 1 - core)))
    out_own = local(
        out_weight.at[:, pl.ds(pl.multiple_of(team * query_cols, 128), query_cols)],
        out_full.at[pl.ds(pl.multiple_of(f * out_cols, 16), out_cols)],
    )

    def cross_part(m, j):
        if m == 0:
            return cross_qkv.at[j]
        return cross_out.at[j, pl.ds(0, piece_sizes[pieces[1][1][j]] // 2)]

    out_cross = []
    for j, piece in enumerate(pieces[1][1]):
        start, size = out_rows(y, piece, core)
        out_cross.append(
            local(
                out_weight.at[
                    pl.ds(pl.multiple_of(start, 16), size),
                    pl.ds(pl.multiple_of(across_team * query_cols, 128), query_cols),
                ],
                cross_part(1, j),
            )
        )
    small_loads = [
        local(source, dest)
        for source, dest in (
            (pair_weight_one, pair_weight),
            (partner_all, partner),
            (cosine_table, cosine),
            (sine_table, sine),
        )
    ]
    everyone = shards * groups
    me = f * groups + g

    pl.semaphore_wait(barrier, 4 + has_up.astype(jnp.int32) + has_down.astype(jnp.int32))

    def way_copy(way, m, s, piece):
        return pltpu.make_async_remote_copy(
            src_ref=slot(m, s, piece, core),
            dst_ref=slot(m, s, piece, core),
            send_sem=send_sem.at[way, m],
            recv_sem=recv_of(m, s, piece, int(way == PARTNER)),
            device_id=way_ids[way],
        )

    def cross_copy(m, j):
        piece = pieces[m][1][j]
        return pltpu.make_async_remote_copy(
            src_ref=cross_part(m, j),
            dst_ref=slot(m, f, piece, core),
            send_sem=cross_send.at[m],
            recv_sem=recv_of(m, f, piece, 0),
            device_id=team_ids[1],
        )

    def arrived(m, s, piece, by_partner=0):
        bytes_of(slot(m, s, piece, core), recv_of(m, s, piece, by_partner)).wait()

    def send_both(m, s, piece):
        pl.when(has_up)(way_copy(UP, m, s, piece).start)
        pl.when(has_down)(way_copy(DOWN, m, s, piece).start)

    def cross_step(m, j):
        piece = pieces[m][1][j]
        arrived(m, across, piece)
        send_both(m, across, piece)
        way_copy(PARTNER, m, across, piece).start()

    def sides(k, o):
        row = y if o == 0 else 1 - y
        below, above = z - k, z + k
        return (
            (below >= 0, 2 * jnp.maximum(below, 0) + row, UP, has_up),
            (above < line, 2 * jnp.minimum(above, line - 1) + row, DOWN, has_down),
        )

    def line_step(m, k, o, j):
        piece = pieces[m][o][j]
        for ok, s, way, onward in sides(k, o):
            if m == 1:
                onward = onward & (k < line - 2)

            @pl.when(ok)
            def _():
                arrived(m, s, piece)
                pl.when(onward)(way_copy(way, m, s, piece).start)
                way_copy(PARTNER, m, s, piece).start()

    def from_partner(m, s, o=0):
        if m == 0:
            bytes_of(qkv_full.at[pl.ds(0, 2 * quarter)], qkv_recv.at[s, 2]).wait()
        else:
            for piece in pieces[1][o]:
                arrived(1, s, piece, 1)

    tok_starts = (0, seq_rows // 4, seq_rows * 5 // 8, seq_rows)

    def tok_copy(way, piece):
        source = 0 if way < 2 else (1, 2, 2)[piece]
        target = team_ids[way] if way < 2 else team_ids[(1, 0, 0)[piece]]
        start, size = tok_starts[piece], tok_starts[piece + 1] - tok_starts[piece]
        return pltpu.make_async_remote_copy(
            src_ref=normed.at[pl.ds(source * seq_rows + start, size)],
            dst_ref=normed.at[pl.ds((1 + way) * seq_rows + start, size)],
            send_sem=tok_send.at[way],
            recv_sem=tok_recv.at[way, piece],
            device_id=target,
        )

    def len_copy(way):
        return pltpu.make_async_remote_copy(
            src_ref=len_tile,
            dst_ref=len_all.at[1 + way],
            send_sem=len_sem.at[0],
            recv_sem=len_sem.at[1],
            device_id=team_ids[way],
        )

    for j in range(2):
        own_loads[j].wait()
        send_both(0, f, j)
        cross_loads[j].wait()
        cross_copy(0, j).start()

    tok_local.wait()
    for copy in vectors:
        copy.wait()
    norm_rows = 16

    @pl.loop(0, seq_rows // norm_rows)
    def _(i):
        at = pl.ds(pl.multiple_of(i * norm_rows, norm_rows), norm_rows)
        rows = tok_own[at, :].astype(jnp.float32)
        scale = lax.rsqrt(jnp.mean(rows * rows, axis=-1, keepdims=True) + 1e-06)
        normed[at, :] = (rows * scale * norm_gain[...]).astype(jnp.bfloat16)

    for first, second in ((0, 1), (1, 2), (2, 0)):
        tok_copy(0, first).start()
        tok_copy(1, second).start()
    length_load.wait()
    len_tile[...] = jnp.full(len_tile.shape, length[0, 0], jnp.int32)
    len_all[0] = len_tile[...]
    for way in range(3):
        len_copy(way).start()

    bias_parts = (
        (team * query_cols, query_cols, 0),
        (QUERY_FEATURES + team * key_cols, key_cols, query_cols),
        (QUERY_FEATURES + KEY_FEATURES + team * key_cols, key_cols, query_cols + key_cols),
    )
    for start, size, to in bias_parts:
        qkv_rows[:, to : to + size] = jnp.broadcast_to(
            qkv_bias[:, pl.ds(pl.multiple_of(start, HEAD_SIZE), size)],
            (groups * seq_rows, size),
        )

    for j in range(2):
        cross_step(0, j)
        line_step(0, 1, 0, j)
    tok_copy(0, 0).wait_recv()
    tok_copy(2, 0).start()
    out_own.wait()
    for j in range(3):
        out_cross[j].wait()
        cross_copy(1, j).start()
    for j in range(2):
        line_step(0, 1, 1, j)
        tok_copy(1, 1 + j).wait_recv()
        tok_copy(2, 1 + j).start()
    steps = [(k, o, j) for k in range(2, line - 1) for o in range(2) for j in range(2)]
    for k, o, j in steps[:-1]:
        line_step(0, k, o, j)

    for way, piece in ((0, 1), (0, 2), (1, 0), (2, 0), (2, 1), (2, 2)):
        tok_copy(way, piece).wait_recv()
    bytes_of(len_all.at[pl.ds(1, 3)], len_sem.at[1]).wait()
    for copy in (*late_loads, *small_loads):
        copy.wait()

    @pl.loop(0, everyone)
    def _(i):
        partner_rows[pl.ds(i, 1), :] = jnp.full((1, HEAD_SIZE), partner[i], jnp.int32)

    def qkv_step(place):
        rows = pl.ds(pl.multiple_of(place * 2 * depth, 128), 2 * depth)

        qkv_rows[...] += jnp.dot(
            normed[:, rows], qkv_full[rows, :], preferred_element_type=jnp.float32
        )

    def qkv_places(first, last):
        @pl.loop(2 * first, 2 * last)
        def _(i):
            k = i // 2
            place = z + (2 * lax.rem(i, 2) - 1) * k

            @pl.when((place >= 0) & (place < line))
            def _():
                from_partner(0, 2 * place)
                from_partner(0, 2 * place + 1)
                qkv_step(place)

    @pl.loop(0, 1)
    def _(i):
        from_partner(0, across)
        qkv_step(z)

    qkv_places(1, 2)
    line_step(0, *steps[-1])
    for j in range(2):
        send_both(1, f, j)
    qkv_places(2, line - 1)
    for j in range(3):
        cross_step(1, j)
    for o in range(2):
        for j in range(2):
            line_step(0, line - 1, o, j)
    qkv_places(line - 1, line)

    def head_rows(j, column):
        return qkv_rows[
            pl.ds(pl.multiple_of(j * seq_rows, seq_rows), seq_rows), column : column + HEAD_SIZE
        ]

    def rotate(rows):
        return (
            rows * cosine[...] + pltpu.roll(rows, HEAD_SIZE // 2, 1) * sine[...]
        ).astype(jnp.bfloat16)

    key_heads = key_cols // HEAD_SIZE
    share = heads // key_heads

    def lanes_of(at, size):
        return pl.ds(pl.multiple_of(at, HEAD_SIZE), size)

    units = ((0, big), (big, 2 * small), (pair - big, big))

    def part_copy(way, place, at, size, unit):
        cols = lanes_of(at, size)
        return pltpu.make_async_remote_copy(
            src_ref=part_out.at[place, pl.ds((1 + way) * seq_rows, seq_rows), cols],
            dst_ref=part_in.at[way, place, :, cols],
            send_sem=part_send.at[way],
            recv_sem=part_recv.at[way, place],
            device_id=team_ids[way],
        )

    def project(place, at, size, unit):
        cols = lanes_of(at, size)
        result = lax.dot_general(
            attn[...],
            out_full[lanes_of(place * pair + at, size), :],
            (((1,), (1,)), ((), ())),
            preferred_element_type=jnp.float32,
        )
        part_out[place, :, cols] = result.astype(jnp.bfloat16)
        own[place, :, cols] = result[:seq_rows]
        for way in (2, 0, 1):
            part_copy(way, place, at, size, unit).start()

    def attn_copy(j):
        rows = pl.ds(pl.multiple_of(j * seq_rows, seq_rows), seq_rows)
        return pltpu.make_async_remote_copy(
            src_ref=attn.at[rows],
            dst_ref=attn_help.at[rows],
            send_sem=attn_send.at[0],
            recv_sem=attn_recv.at[j],
            device_id=end_to_helper,
        )

    @pl.loop(0, groups)
    def _(i):
        j = groups - 1 - i
        query_place = lax.broadcasted_iota(jnp.int32, (seq_rows, seq_rows), 0)
        key_place = lax.broadcasted_iota(jnp.int32, (seq_rows, seq_rows), 1)
        allowed = (key_place <= query_place) & (key_place < len_all[j, 0:1, :])
        at = pl.ds(pl.multiple_of(j * seq_rows, seq_rows), seq_rows)
        for kh in range(key_heads):
            offset = kh * HEAD_SIZE
            group = [slice(h * HEAD_SIZE, (h + 1) * HEAD_SIZE) for h in range(share)]
            first = kh * share * HEAD_SIZE
            key = rotate(head_rows(j, query_cols + offset))
            value = head_rows(j, query_cols + key_cols + offset).astype(jnp.bfloat16)
            for lanes in group:
                queries[lanes, :] = rotate(head_rows(j, first + lanes.start))
            score_rows[...] = lax.dot_general(
                queries[...], key, (((1,), (1,)), ((), ())), preferred_element_type=jnp.float32
            )
            for lanes in group:
                scores = score_rows[lanes, :] * np.float32(1 / np.sqrt(HEAD_SIZE))
                scores = jnp.where(allowed, scores, jnp.float32(-1e30))
                expd = jnp.exp(scores - jnp.max(scores, axis=-1, keepdims=True))
                inverse = 1.0 / jnp.sum(expd, axis=-1, keepdims=True)
                queries[lanes, :] = (expd * inverse).astype(jnp.bfloat16)
            mixed = jnp.dot(queries[...], value, preferred_element_type=jnp.float32)
            for lanes in group:
                attn[at, first + lanes.start : first + lanes.stop] = mixed[lanes].astype(
                    jnp.bfloat16
                )
        pl.when(is_end)(attn_copy(j).start)

        @pl.when(i == 0)
        def _():
            from_partner(1, across, 1)

        result = lax.dot_general(
            attn[at, :],
            out_full[lanes_of(z * pair, pair), :],
            (((1,), (1,)), ((), ())),
            preferred_element_type=jnp.float32,
        )
        part_out[z, at, :] = result.astype(jnp.bfloat16)
        own[z] = result
        for way in range(3):
            pl.when(j == way + 1)(part_copy(way, z, 0, pair, 0).start)

    def project_pair(place):
        @pl.loop(0, 2)
        def _(i):
            project(place, i * (pair - big), big, 2 * i)

        project(place, big, 2 * small, 1)

    place = lax.broadcasted_iota(jnp.int32, len_tile.shape, 1)
    pick = (place == len_tile[...] - 1).astype(jnp.bfloat16)
    stats[...] = jnp.zeros_like(stats)

    def finish(place, sums):
        cols = lanes_of(place * pair, pair)
        hidden[:, cols] = (tok_own[:, cols].astype(jnp.float32) + sums).astype(jnp.bfloat16)
        last = jnp.dot(pick, hidden[:, cols], preferred_element_type=jnp.float32)
        weighted = last * final_gain[:, cols] * value_head[:, cols]
        squares = last * last
        for t in range(pair // HEAD_SIZE):
            lanes = slice(t * HEAD_SIZE, (t + 1) * HEAD_SIZE)
            stats[0] += squares[:, lanes]
            stats[1] += weighted[:, lanes]

    def finish_parts(place):
        for way in range(3):
            bytes_of(part_in.at[way, place], part_recv.at[way, place]).wait()
        total = own[place]
        for way in range(3):
            total += part_in[way, place].astype(jnp.float32)
        finish(place, total)

    def at_sides(k, body):
        @pl.loop(0, 2)
        def _(i):
            place = z + (2 * i - 1) * k

            @pl.when((place >= 0) & (place < line) & ((k > 0) | (i == 0)))
            def _():
                body(place)

    def own_unit(place):
        arrived(1, 2 * place + y, 0, 1)
        project(place, y * (pair - big), big, 2 * y)

    def mid_unit(place):
        arrived(1, 2 * place + y, 1, 1)
        arrived(1, 2 * place + 1 - y, 1, 1)
        project(place, big, 2 * small, 1)

    def cross_unit(piece):
        inner = (1 - y) * (pair - big) + y * (big // 2)
        outer = (1 - y) * (pair - big // 2)

        def body(place):
            arrived(1, 2 * place + 1 - y, piece, 1)
            project(place, (inner, outer)[piece - 2], big // 2, 0)

        return body

    @pl.loop(1, line - 1)
    def _(k):
        mine = jnp.logical_not(is_helper) | (k < line - 2)
        line_step(1, k, 0, 0)
        line_step(1, k, 0, 1)

        @pl.when(mine)
        def _():
            at_sides(k, own_unit)

        @pl.when(jnp.logical_not(is_helper))
        def _():
            at_sides(k - 1, finish_parts)

        line_step(1, k, 1, 0)

        @pl.when(mine)
        def _():
            at_sides(k, mid_unit)

        for j in (1, 2):
            line_step(1, k, 1, j)

            @pl.when(mine)
            def _():
                at_sides(k, cross_unit(1 + j))

    def help_part(way):
        return pltpu.make_async_remote_copy(
            src_ref=help_out.at[1 + way],
            dst_ref=help_in.at[way],
            send_sem=help_send.at[0],
            recv_sem=help_recv.at[way],
            device_id=team_ids[way],
        )

    done_copy = pltpu.make_async_remote_copy(
        src_ref=help_sum,
        dst_ref=help_done,
        send_sem=done_sem.at[0],
        recv_sem=done_sem.at[1],
        device_id=helper_to_end,
    )

    @pl.when(is_helper)
    def _():
        from_partner(1, 2 * far + y, 0)
        from_partner(1, 2 * far + 1 - y, 1)

        @pl.loop(0, groups)
        def _(i):
            j = groups - 1 - i
            rows = pl.ds(pl.multiple_of(j * seq_rows, seq_rows), seq_rows)
            pltpu.make_async_copy(attn_help.at[rows], attn_help.at[rows], attn_recv.at[j]).wait()
            result = lax.dot_general(
                attn_help[rows, :],
                out_full[lanes_of(far * pair, pair), :],
                (((1,), (1,)), ((), ())),
                preferred_element_type=jnp.float32,
            )
            help_own[...] = result
            help_out[j] = result.astype(jnp.bfloat16)
            for way in range(3):
                pl.when(j == way + 1)(help_part(way).start)

        project_pair(far)

        @pl.loop(0, line)
        def _(place):
            pl.when(place != far)(lambda: finish_parts(place))

        for way in range(3):
            help_part(way).wait_recv()
        total = help_own[...]
        for way in range(3):
            total += help_in[way].astype(jnp.float32)
        help_sum[...] = total.astype(jnp.bfloat16)
        done_copy.start()

    @pl.when(is_end)
    def _():
        at_sides(line - 2, finish_parts)
        done_copy.wait_recv()
        finish(far, help_done[...].astype(jnp.float32))

    @pl.when(is_helper)
    def _():
        finish_parts(far)

    mean = jnp.sum(stats[0], axis=-1, keepdims=True) / width
    score = jnp.sum(stats[1], axis=-1, keepdims=True) * lax.rsqrt(mean + 1e-06)
    first_row = lax.broadcasted_iota(jnp.int32, score_tile.shape, 0) == 0
    score_tile[...] = jnp.where(first_row, score, jnp.full(score_tile.shape, pair_weight[0, 0]))
    score_all[me] = score_tile[...]

    def score_copy(i):
        other = lax.rem(me + i, everyone)
        return pltpu.make_async_remote_copy(
            src_ref=score_tile,
            dst_ref=score_all.at[me],
            send_sem=score_sem.at[0],
            recv_sem=score_sem.at[1],
            device_id={"fsdp": other // groups, "dp": lax.rem(other, groups)},
        )

    @pl.loop(1, everyone)
    def _(i):
        score_copy(i).start()

    bytes_of(cross_qkv, cross_send.at[0]).wait()
    bytes_of(out_full.at[pl.ds(0, out_cols // 2)], cross_send.at[1]).wait()
    bytes_of(len_all.at[pl.ds(1, 3)], len_sem.at[0]).wait()
    for way in range(3):
        bytes_of(normed.at[pl.ds(0, seq_rows)], tok_send.at[way]).wait()
    for spot in range(line):
        ends = spot in (0, line - 1)
        up = 0 if spot == line - 1 else 2 * (spot + 1)
        down = 0 if spot == 0 else 2 * (line - spot)
        sent = (
            (UP, up, up - 2 * (spot == line - 2)),
            (DOWN, down, down - 2 * (spot == 1)),
            (PARTNER, shards - 1, shards - 1 - 2 * ends),
        )

        @pl.when(z == spot)
        def _():
            for way, slices, out_slices in sent:
                if slices:
                    rows = pl.ds(0, slices * depth // 2)
                    bytes_of(qkv_full.at[rows], send_sem.at[way, 0]).wait()
                    rows = pl.ds(0, out_slices * out_cols // 2)
                    bytes_of(out_full.at[rows], send_sem.at[way, 1]).wait()
            for way in range(3):
                bytes_of(part_in.at[0, pl.ds(0, line - ends)], part_send.at[way]).wait()
            if ends:
                bytes_of(attn, attn_send.at[0]).wait()

    @pl.when(is_helper)
    def _():
        bytes_of(help_in, help_send.at[0]).wait()
        done_copy.wait_send()

    bytes_of(score_all.at[pl.ds(0, everyone - 1)], score_sem.at[1]).wait()

    scores = score_all[:, 0, :]
    weights = score_all[:, 1, :]
    row = lax.broadcasted_iota(jnp.int32, scores.shape, 0)
    lane = lax.broadcasted_iota(jnp.int32, scores.shape, 1)
    partners = partner_rows[...]
    score_row = jnp.sum(jnp.where(row == lane, scores, 0.0), axis=0, keepdims=True)
    others = jnp.sum(jnp.where(partners == lane, score_row, 0.0), axis=1, keepdims=True)
    margins = jnp.where(row < partners, scores - others, others - scores)
    softplus = jnp.maximum(-margins, 0.0) + jnp.log1p(jnp.exp(-jnp.abs(margins)))
    first_lane = lane == 0
    margin = jnp.sum(jnp.where(first_lane & (row == me), margins, 0.0))
    loss = jnp.sum(jnp.where(first_lane, weights * softplus, 0.0)) / everyone
    results[...] = jnp.where(first_row, jnp.full(results.shape, margin), loss)
    bytes_of(score_all.at[pl.ds(0, everyone - 1)], score_sem.at[0]).wait()


def layer_fits(shards, groups, tokens, qkv_weight, out_weight):
    return (
        shards % 2 == 0
        and shards >= 8
        and qkv_weight.shape[0] % 64 == 0
        and groups == 4
        and KEY_VALUE_HEADS % groups == 0
        and tokens.shape[1] == HEAD_SIZE
        and shards * groups <= HEAD_SIZE
        and out_weight.shape[1] % 64 == 0
        and out_weight.shape[1] > HEAD_SIZE
    )


def layer(
    tokens,
    lengths,
    partner,
    pair_weight,
    norm_gain,
    qkv_weight,
    qkv_bias,
    out_weight,
    final_gain,
    value_head,
):
    shards, groups = lax.axis_size("fsdp"), lax.axis_size("dp")
    _, seq_rows, width = tokens.shape
    depth = qkv_weight.shape[0]
    out_cols = out_weight.shape[1]
    query_cols = QUERY_FEATURES // groups
    key_cols = KEY_FEATURES // groups
    all_cols = query_cols + 2 * key_cols
    rows = groups * seq_rows
    line, pair = shards // 2, 2 * out_cols
    cosine, sine = rotary_tables(seq_rows)
    everyone = shards * groups
    dma = pltpu.SemaphoreType.DMA
    vmem = pl.BlockSpec(memory_space=pltpu.VMEM)
    bf16, f32 = jnp.bfloat16, jnp.float32
    hidden, results = pl.pallas_call(
        functools.partial(layer_kernel, shards, groups),
        out_shape=(
            pltpu.VMEM((seq_rows, width), bf16),
            pltpu.VMEM((8, HEAD_SIZE), f32),
        ),
        in_specs=[pl.BlockSpec(memory_space=pltpu.HBM)] * 12,
        out_specs=(vmem, vmem),
        scratch_shapes=[
            pltpu.VMEM((shards * depth, all_cols), bf16),
            pltpu.VMEM((shards * out_cols, query_cols), bf16),
            pltpu.VMEM((2, depth // 4, all_cols), bf16),
            pltpu.VMEM((3, max(out_pieces(out_cols)) // 2, query_cols), bf16),
            pltpu.VMEM((seq_rows, width), bf16),
            pltpu.VMEM((8, seq_rows), jnp.int32),
            pltpu.VMEM((groups, 8, seq_rows), jnp.int32),
            pltpu.VMEM((rows, width), bf16),
            pltpu.VMEM((rows, all_cols), f32),
            pltpu.VMEM((rows, query_cols), bf16),
            pltpu.VMEM((line, seq_rows, pair), f32),
            pltpu.VMEM((line, rows, pair), bf16),
            pltpu.VMEM((groups - 1, line, seq_rows, pair), bf16),
            pltpu.VMEM((rows, query_cols), bf16),
            pltpu.VMEM((seq_rows, pair), f32),
            pltpu.VMEM((groups, seq_rows, pair), bf16),
            pltpu.VMEM((groups - 1, seq_rows, pair), bf16),
            pltpu.VMEM((seq_rows, pair), bf16),
            pltpu.VMEM((seq_rows, pair), bf16),
            pltpu.VMEM((2, 8, HEAD_SIZE), f32),
            pltpu.VMEM((query_cols * HEAD_SIZE // key_cols, HEAD_SIZE), bf16),
            pltpu.VMEM((query_cols * HEAD_SIZE // key_cols, HEAD_SIZE), f32),
            pltpu.VMEM((8, HEAD_SIZE), f32),
            pltpu.VMEM((everyone, 8, HEAD_SIZE), f32),
            pltpu.VMEM((everyone, HEAD_SIZE), jnp.int32),
            pltpu.VMEM((1, width), f32),
            pltpu.VMEM((1, width + 8 * HEAD_SIZE), f32),
            pltpu.VMEM((1, width + 8 * HEAD_SIZE), f32),
            pltpu.VMEM((1, qkv_bias.shape[0] + 8 * HEAD_SIZE), f32),
            pltpu.VMEM((seq_rows, HEAD_SIZE), f32),
            pltpu.VMEM((seq_rows, HEAD_SIZE), f32),
            pltpu.SMEM((1, 1), jnp.int32),
            pltpu.SMEM((1, 1), f32),
            pltpu.SMEM((everyone,), jnp.int32),
            dma((20,)),
            dma((shards, 3)),
            dma((shards, 3, 2)),
            dma((3, 2)),
            dma((2,)),
            dma((3,)),
            dma((3, 3)),
            dma((2,)),
            dma((3,)),
            dma((3, line)),
            dma((1,)),
            dma((groups,)),
            dma((1,)),
            dma((3,)),
            dma((2,)),
            dma((2,)),
        ],
        compiler_params=pltpu.CompilerParams(
            collective_id=0, has_side_effects=True, vmem_limit_bytes=56 * 1024 * 1024
        ),
    )(
        tokens[0],
        qkv_weight,
        out_weight.T,
        lengths[None],
        pair_weight[None],
        partner,
        norm_gain,
        final_gain,
        value_head,
        qkv_bias,
        jnp.asarray(cosine),
        jnp.asarray(sine),
    )
    return hidden[None], results[0, :1], results[1, 0]


def projected_by_gathers(
    tokens,
    lengths,
    norm_gain,
    qkv_weight,
    qkv_bias,
    out_weight,
):
    sequence = tokens[0]
    length_rows = sequence.shape[0]
    width = sequence.shape[1]
    normed = rms_scale(sequence.astype(jnp.float32), norm_gain).astype(jnp.bfloat16)
    query_group_count = lax.axis_size("dp")
    group_index = lax.axis_index("dp")
    query_heads = QUERY_HEADS // query_group_count
    key_value_heads = KEY_VALUE_HEADS // query_group_count
    query_cols = query_heads * HEAD_SIZE
    key_cols = key_value_heads * HEAD_SIZE
    group_normed, group_lengths = (
        lax.all_gather(normed[None], "dp", axis=0, tiled=True),
        lax.all_gather(lengths, "dp", axis=0, tiled=True),
    )
    seq_count = group_normed.shape[0]
    flat = group_normed.reshape(seq_count * length_rows, width)
    qkv_cols = jnp.concatenate(
        [
            lax.dynamic_slice_in_dim(qkv_weight, group_index * query_cols, query_cols, 1),
            lax.dynamic_slice_in_dim(
                qkv_weight, QUERY_FEATURES + group_index * key_cols, key_cols, 1
            ),
            lax.dynamic_slice_in_dim(
                qkv_weight, QUERY_FEATURES + KEY_FEATURES + group_index * key_cols, key_cols, 1
            ),
        ],
        axis=1,
    )
    bias_cols = jnp.concatenate(
        [
            lax.dynamic_slice_in_dim(qkv_bias, group_index * query_cols, query_cols, 0),
            lax.dynamic_slice_in_dim(
                qkv_bias, QUERY_FEATURES + group_index * key_cols, key_cols, 0
            ),
            lax.dynamic_slice_in_dim(
                qkv_bias, QUERY_FEATURES + KEY_FEATURES + group_index * key_cols, key_cols, 0
            ),
        ],
        axis=0,
    )
    out_rows = lax.dynamic_slice_in_dim(out_weight, group_index * query_cols, query_cols, 0)
    qkv_full, out_full = (
        lax.all_gather(qkv_cols, "fsdp", axis=0, tiled=True),
        lax.all_gather(out_rows, "fsdp", axis=1, tiled=True),
    )
    query_key_value = jnp.dot(flat, qkv_full, preferred_element_type=jnp.float32) + bias_cols
    attn = attend(
        query_key_value.reshape(seq_count, length_rows, -1),
        group_lengths,
        query_heads,
        key_value_heads,
    )
    return lax.psum_scatter(
        jnp.dot(attn, out_full, preferred_element_type=jnp.float32),
        "dp",
        scatter_dimension=0,
        tiled=True,
    )


def per_device(
    tokens,
    lengths,
    partner,
    pair_weight,
    norm_gain,
    qkv_weight,
    qkv_bias,
    out_weight,
    final_gain,
    value_head,
):
    if layer_fits(lax.axis_size("fsdp"), lax.axis_size("dp"), tokens, qkv_weight, out_weight):
        return layer(
            tokens,
            lengths,
            partner,
            pair_weight,
            norm_gain,
            qkv_weight,
            qkv_bias,
            out_weight,
            final_gain,
            value_head,
        )
    sequence = tokens[0]
    length = lengths[0]
    projected = projected_by_gathers(tokens, lengths, norm_gain, qkv_weight, qkv_bias, out_weight)
    hidden = (sequence.astype(jnp.float32) + projected).astype(jnp.bfloat16)
    last = lax.dynamic_slice_in_dim(hidden, length - 1, 1, 0)[0].astype(jnp.float32)
    score = jnp.sum(rms_scale(last, final_gain) * value_head)
    everyone, weights_all = (
        lax.all_gather(score.reshape(1), ("fsdp", "dp"), axis=0, tiled=True),
        lax.all_gather(pair_weight, ("fsdp", "dp"), axis=0, tiled=True),
    )
    total_seqs = everyone.shape[0]
    mine = lax.axis_index(("fsdp", "dp"))
    index_all = jnp.arange(total_seqs, dtype=jnp.int32)
    my_partner = jnp.sum(jnp.where(index_all == mine, partner, 0))
    other = jnp.sum(jnp.where(index_all == my_partner, everyone, jnp.float32(0.0)))
    margin = jnp.where(mine < my_partner, score - other, other - score)
    matches = partner[:, None] == index_all[None, :]
    others_all = jnp.sum(jnp.where(matches, everyone[None, :], jnp.float32(0.0)), axis=1)
    margins_all = jnp.where(index_all < partner, everyone - others_all, others_all - everyone)
    loss = jnp.sum(weights_all * jax.nn.softplus(-margins_all)) / total_seqs
    return (hidden[None], margin.reshape(1), loss)


def solution(mesh):
    return jax.shard_map(
        per_device,
        mesh=mesh,
        in_specs=(
            P(("fsdp", "dp"), None, None),
            P(("fsdp", "dp")),
            P(),
            P(("fsdp", "dp")),
            P(),
            P("fsdp", None),
            P(),
            P(None, "fsdp"),
            P(),
            P(),
        ),
        out_specs=(P(("fsdp", "dp"), None, None), P(("fsdp", "dp")), P()),
        check_vma=False,
    )
```

```python
import functools

import jax
import jax.numpy as jnp
import numpy as np
from jax import lax
from jax.experimental import pallas as pl
from jax.experimental.pallas import tpu as pltpu
from jax.sharding import PartitionSpec as P

QUERY_HEADS = 28
KEY_VALUE_HEADS = 4
HEAD_SIZE = 128
QUERY_FEATURES = 3584
KEY_FEATURES = 512


def rms_scale(value_rows, gain):
    return (
        value_rows
        * lax.rsqrt(jnp.mean(value_rows * value_rows, axis=-1, keepdims=True) + 1e-06)
        * gain
    )


def apply_rotary(heads, length_rows):
    half = HEAD_SIZE // 2
    positions = jnp.arange(length_rows, dtype=jnp.float32)
    freqs = jnp.exp(
        -(2.0 * jnp.arange(half, dtype=jnp.float32) / HEAD_SIZE) * jnp.log(jnp.float32(1000000.0))
    )
    angles = positions[:, None] * freqs[None, :]
    cosine = jnp.cos(angles)
    sine = jnp.sin(angles)
    first = heads[..., :half]
    second = heads[..., half:]
    return jnp.concatenate(
        [first * cosine - second * sine, second * cosine + first * sine], axis=-1
    )


def attend(query_key_value, group_lengths, query_heads, key_value_heads):
    seq_count, length_rows, _ = query_key_value.shape
    query_width = query_heads * HEAD_SIZE
    key_width = key_value_heads * HEAD_SIZE
    query_rows = (
        query_key_value[..., :query_width]
        .reshape(seq_count, length_rows, query_heads, HEAD_SIZE)
        .transpose(0, 2, 1, 3)
    )
    key_rows = (
        query_key_value[..., query_width : query_width + key_width]
        .reshape(seq_count, length_rows, key_value_heads, HEAD_SIZE)
        .transpose(0, 2, 1, 3)
    )
    value_rows = (
        query_key_value[..., query_width + key_width :]
        .reshape(seq_count, length_rows, key_value_heads, HEAD_SIZE)
        .transpose(0, 2, 1, 3)
        .astype(jnp.bfloat16)
    )
    query_rows = (
        apply_rotary(query_rows, length_rows)
        .astype(jnp.bfloat16)
        .reshape(seq_count, key_value_heads, query_heads // key_value_heads, length_rows, HEAD_SIZE)
    )
    key_rows = apply_rotary(key_rows, length_rows).astype(jnp.bfloat16)
    scores = jnp.einsum(
        "bgqtd,bgsd->bgqts", query_rows, key_rows, preferred_element_type=jnp.float32
    ) / jnp.sqrt(jnp.float32(HEAD_SIZE))
    places = jnp.arange(length_rows, dtype=jnp.int32)
    causal = places[None, :] <= places[:, None]
    usable = places[None, :] < group_lengths[:, None]
    allowed = causal[None, :, :] & usable[:, None, :]
    scores = jnp.where(allowed[:, None, None, :, :], scores, jnp.float32(-1e30))
    highest = jnp.max(scores, axis=-1, keepdims=True)
    expd = jnp.exp(scores - highest)
    probs = (expd / jnp.sum(expd, axis=-1, keepdims=True)).astype(jnp.bfloat16)
    mixed = jnp.einsum("bgqts,bgsd->bgqtd", probs, value_rows, preferred_element_type=jnp.float32)
    mixed = mixed.reshape(seq_count, query_heads, length_rows, HEAD_SIZE).transpose(0, 2, 1, 3)
    return mixed.reshape(seq_count * length_rows, query_width).astype(jnp.bfloat16)


UP, DOWN, PARTNER = 0, 1, 2


def rotary_tables(length_rows):
    half = HEAD_SIZE // 2
    freqs = 1000000.0 ** (-2.0 * np.arange(half) / HEAD_SIZE)
    angles = np.arange(length_rows)[:, None] * freqs[None, :]
    cosine, sine = np.cos(angles), np.sin(angles)
    return (
        np.concatenate([cosine, cosine], axis=1).astype(np.float32),
        np.concatenate([-sine, sine], axis=1).astype(np.float32),
    )


def out_pieces(out_cols):
    small = HEAD_SIZE // 2
    return out_cols - small, small


def layer_kernel(
    shards,
    groups,
    tokens,
    qkv_weight,
    out_weight,
    length_one,
    pair_weight_one,
    partner_all,
    norm_gain_flat,
    final_gain_flat,
    value_head_flat,
    qkv_bias_flat,
    cosine_table,
    sine_table,
    hidden,
    results,
    qkv_full,
    out_full,
    cross_qkv,
    cross_out,
    tok_own,
    len_tile,
    len_all,
    normed,
    qkv_rows,
    attn,
    own,
    part_out,
    part_in,
    attn_help,
    help_own,
    help_out,
    help_in,
    help_sum,
    help_done,
    stats,
    queries,
    score_rows,
    score_tile,
    score_all,
    partner_rows,
    norm_gain,
    final_gain,
    value_head,
    qkv_bias,
    cosine,
    sine,
    length,
    pair_weight,
    partner,
    local_sem,
    qkv_recv,
    out_recv,
    send_sem,
    cross_send,
    tok_send,
    tok_recv,
    len_sem,
    part_send,
    part_recv,
    attn_send,
    attn_recv,
    help_send,
    help_recv,
    done_sem,
    score_sem,
):
    line = shards // 2
    f = lax.axis_index("fsdp")
    g = lax.axis_index("dp")
    z = f // 2
    y = f % 2
    x = g // 2
    core = g % 2
    seq_rows = tokens.shape[0]
    width = tokens.shape[1]
    depth = qkv_weight.shape[0]
    out_cols = out_weight.shape[0]
    query_cols = QUERY_FEATURES // groups
    key_cols = KEY_FEATURES // groups
    heads = query_cols // HEAD_SIZE
    quarter = depth // 4
    pair = 2 * out_cols
    big, small = out_pieces(out_cols)
    is_end = (z == 0) | (z == line - 1)
    is_helper = (z == 1) | (z == line - 2)
    far = jnp.where((z == 0) | (z == 1), line - 1, 0)
    near = jnp.where((z == 0) | (z == 1), line - 2, 1)
    end_to_helper = {"fsdp": jnp.where(z == 0, f + 2, f - 2)}
    helper_to_end = {"fsdp": jnp.where(z == 1, f - 2, f + 2)}
    has_up = z < line - 1
    has_down = z > 0
    team = 2 * x + y
    across_team = 2 * x + 1 - y
    across = 2 * z + 1 - y
    x_peer = 2 * (1 - x) + core
    team_ids = ({"dp": x_peer}, {"fsdp": across}, {"fsdp": across, "dp": x_peer})
    way_ids = ({"fsdp": f + 2}, {"fsdp": f - 2}, {"dp": 2 * x + 1 - core})

    barrier = pltpu.get_barrier_semaphore()
    for target in (*team_ids, way_ids[PARTNER]):
        pl.semaphore_signal(barrier, inc=1, device_id=target)
    for way, ok in ((UP, has_up), (DOWN, has_down)):

        @pl.when(ok)
        def _():
            pl.semaphore_signal(barrier, inc=1, device_id=way_ids[way])

    edge = HEAD_SIZE
    piece_sizes = (big, small, big - edge, edge)
    pieces = (((0, 1), (0, 1)), ((0, 1), (1, 2, 3)))

    def out_rows(side, piece, half):
        size = piece_sizes[piece] // 2
        start = (
            side * small,
            (1 - side) * big,
            (1 - side) * edge + side * small,
            side * (out_cols - edge),
        )[piece]
        return start + half * size, size

    def slot(m, s, piece, half):
        if m == 0:
            start = s * depth + (2 * piece + half) * quarter
            return qkv_full.at[pl.ds(pl.multiple_of(start, 16), quarter)]
        start, size = out_rows(lax.rem(s, 2), piece, half)
        return out_full.at[pl.ds(pl.multiple_of(s * out_cols + start, 16), size)]

    def recv_of(m, s, piece, by_partner):
        if m == 0:
            return qkv_recv.at[s, 2 if by_partner else piece]
        return out_recv.at[s, (0, 1, 0, 2)[piece], by_partner]

    count = 0

    def local(source, dest):
        nonlocal count
        copy = pltpu.make_async_copy(source, dest, local_sem.at[count])
        count += 1
        copy.start()
        return copy

    def bytes_of(ref, sem):
        return pltpu.make_async_copy(ref, ref, sem)

    def qkv_parts(piece, half, owner, dest):
        nonlocal count
        rows = pl.ds(pl.multiple_of((2 * piece + half) * quarter, 16), quarter)
        for start, size, to in (
            (owner * query_cols, query_cols, 0),
            (QUERY_FEATURES + owner * key_cols, key_cols, query_cols),
            (QUERY_FEATURES + KEY_FEATURES + owner * key_cols, key_cols, query_cols + key_cols),
        ):
            pltpu.make_async_copy(
                qkv_weight.at[rows, pl.ds(pl.multiple_of(start, 128), size)],
                dest.at[:, pl.ds(to, size)],
                local_sem.at[count],
            ).start()
        count += 1
        return bytes_of(dest, local_sem.at[count - 1])

    length_load = local(length_one, length)
    own_loads, cross_loads = [], []
    for j in range(2):
        own_loads.append(qkv_parts(j, core, team, slot(0, f, j, core)))
        cross_loads.append(qkv_parts(j, core, across_team, cross_qkv.at[j]))
    tok_local = local(tokens, tok_own)
    vectors = [
        local(flat, row.at[0, pl.ds(0, flat.shape[0])])
        for flat, row in (
            (norm_gain_flat, norm_gain),
            (final_gain_flat, final_gain),
            (value_head_flat, value_head),
            (qkv_bias_flat, qkv_bias),
        )
    ]
    late_loads = []
    for j in range(2):
        late_loads.append(qkv_parts(j, 1 - core, team, slot(0, f, j, 1 - core)))
    out_own = local(
        out_weight.at[:, pl.ds(pl.multiple_of(team * query_cols, 128), query_cols)],
        out_full.at[pl.ds(pl.multiple_of(f * out_cols, 16), out_cols)],
    )

    def cross_part(m, j):
        if m == 0:
            return cross_qkv.at[j]
        return cross_out.at[j, pl.ds(0, piece_sizes[pieces[1][1][j]] // 2)]

    out_cross = []
    for j, piece in enumerate(pieces[1][1]):
        start, size = out_rows(y, piece, core)
        out_cross.append(
            local(
                out_weight.at[
                    pl.ds(pl.multiple_of(start, 16), size),
                    pl.ds(pl.multiple_of(across_team * query_cols, 128), query_cols),
                ],
                cross_part(1, j),
            )
        )
    small_loads = [
        local(source, dest)
        for source, dest in (
            (pair_weight_one, pair_weight),
            (partner_all, partner),
            (cosine_table, cosine),
            (sine_table, sine),
        )
    ]
    everyone = shards * groups
    me = f * groups + g

    pl.semaphore_wait(barrier, 4 + has_up.astype(jnp.int32) + has_down.astype(jnp.int32))

    def way_copy(way, m, s, piece):
        return pltpu.make_async_remote_copy(
            src_ref=slot(m, s, piece, core),
            dst_ref=slot(m, s, piece, core),
            send_sem=send_sem.at[way, m],
            recv_sem=recv_of(m, s, piece, int(way == PARTNER)),
            device_id=way_ids[way],
        )

    def cross_copy(m, j):
        piece = pieces[m][1][j]
        return pltpu.make_async_remote_copy(
            src_ref=cross_part(m, j),
            dst_ref=slot(m, f, piece, core),
            send_sem=cross_send.at[m],
            recv_sem=recv_of(m, f, piece, 0),
            device_id=team_ids[1],
        )

    def arrived(m, s, piece, by_partner=0):
        bytes_of(slot(m, s, piece, core), recv_of(m, s, piece, by_partner)).wait()

    def send_both(m, s, piece):
        pl.when(has_up)(way_copy(UP, m, s, piece).start)
        pl.when(has_down)(way_copy(DOWN, m, s, piece).start)

    def cross_step(m, j):
        piece = pieces[m][1][j]
        arrived(m, across, piece)
        send_both(m, across, piece)
        way_copy(PARTNER, m, across, piece).start()

    def sides(k, o):
        row = y if o == 0 else 1 - y
        below, above = z - k, z + k
        return (
            (below >= 0, 2 * jnp.maximum(below, 0) + row, UP, has_up),
            (above < line, 2 * jnp.minimum(above, line - 1) + row, DOWN, has_down),
        )

    def line_step(m, k, o, j):
        piece = pieces[m][o][j]
        for ok, s, way, onward in sides(k, o):
            if m == 1:
                onward = onward & (k < line - 2)
            if m == 1 and piece == 1:
                spot, target = (z - line + 2, 1) if way == UP else (z - 1, line - 2)
                onward = onward & jnp.logical_not((spot == 0) & (s // 2 == target))
                ok = ok & jnp.logical_not(is_end & (k == line - 2))

            @pl.when(ok)
            def _():
                arrived(m, s, piece)
                pl.when(onward)(way_copy(way, m, s, piece).start)
                way_copy(PARTNER, m, s, piece).start()

    def from_partner(m, s, o=0):
        if m == 0:
            bytes_of(qkv_full.at[pl.ds(0, 2 * quarter)], qkv_recv.at[s, 2]).wait()
        else:
            for piece in pieces[1][o]:
                arrived(1, s, piece, 1)

    tok_starts = (0, seq_rows // 4, seq_rows * 5 // 8, seq_rows)

    def tok_copy(way, piece):
        source = 0 if way < 2 else (1, 2, 2)[piece]
        target = team_ids[way] if way < 2 else team_ids[(1, 0, 0)[piece]]
        start, size = tok_starts[piece], tok_starts[piece + 1] - tok_starts[piece]
        return pltpu.make_async_remote_copy(
            src_ref=normed.at[pl.ds(source * seq_rows + start, size)],
            dst_ref=normed.at[pl.ds((1 + way) * seq_rows + start, size)],
            send_sem=tok_send.at[way],
            recv_sem=tok_recv.at[way, piece],
            device_id=target,
        )

    def len_copy(way):
        return pltpu.make_async_remote_copy(
            src_ref=len_tile,
            dst_ref=len_all.at[1 + way],
            send_sem=len_sem.at[0],
            recv_sem=len_sem.at[1],
            device_id=team_ids[way],
        )

    for j in range(2):
        own_loads[j].wait()
        send_both(0, f, j)
        cross_loads[j].wait()
        cross_copy(0, j).start()

    tok_local.wait()
    for copy in vectors:
        copy.wait()
    norm_rows = 16

    @pl.loop(0, seq_rows // norm_rows)
    def _(i):
        at = pl.ds(pl.multiple_of(i * norm_rows, norm_rows), norm_rows)
        rows = tok_own[at, :].astype(jnp.float32)
        scale = lax.rsqrt(jnp.mean(rows * rows, axis=-1, keepdims=True) + 1e-06)
        normed[at, :] = (rows * scale * norm_gain[...]).astype(jnp.bfloat16)

    for first, second in ((0, 1), (1, 2), (2, 0)):
        tok_copy(0, first).start()
        tok_copy(1, second).start()
    length_load.wait()
    len_tile[...] = jnp.full(len_tile.shape, length[0, 0], jnp.int32)
    len_all[0] = len_tile[...]
    for way in range(3):
        len_copy(way).start()

    bias_parts = (
        (team * query_cols, query_cols, 0),
        (QUERY_FEATURES + team * key_cols, key_cols, query_cols),
        (QUERY_FEATURES + KEY_FEATURES + team * key_cols, key_cols, query_cols + key_cols),
    )
    for start, size, to in bias_parts:
        qkv_rows[:, to : to + size] = jnp.broadcast_to(
            qkv_bias[:, pl.ds(pl.multiple_of(start, HEAD_SIZE), size)],
            (groups * seq_rows, size),
        )

    for j in range(2):
        cross_step(0, j)
        line_step(0, 1, 0, j)
    tok_copy(0, 0).wait_recv()
    tok_copy(2, 0).start()
    out_own.wait()
    for j in range(3):
        out_cross[j].wait()
        cross_copy(1, j).start()
    for j in range(2):
        line_step(0, 1, 1, j)
        tok_copy(1, 1 + j).wait_recv()
        tok_copy(2, 1 + j).start()
    steps = [(k, o, j) for k in range(2, line - 1) for o in range(2) for j in range(2)]
    for k, o, j in steps[:-1]:
        line_step(0, k, o, j)

    for way, piece in ((0, 1), (0, 2), (1, 0), (2, 0), (2, 1), (2, 2)):
        tok_copy(way, piece).wait_recv()
    bytes_of(len_all.at[pl.ds(1, 3)], len_sem.at[1]).wait()
    for copy in (*late_loads, *small_loads):
        copy.wait()

    @pl.loop(0, everyone)
    def _(i):
        partner_rows[pl.ds(i, 1), :] = jnp.full((1, HEAD_SIZE), partner[i], jnp.int32)

    def qkv_step(place):
        rows = pl.ds(pl.multiple_of(place * 2 * depth, 128), 2 * depth)

        qkv_rows[...] += jnp.dot(
            normed[:, rows], qkv_full[rows, :], preferred_element_type=jnp.float32
        )

    def qkv_places(first, last):
        @pl.loop(2 * first, 2 * last)
        def _(i):
            k = i // 2
            place = z + (2 * lax.rem(i, 2) - 1) * k

            @pl.when((place >= 0) & (place < line))
            def _():
                from_partner(0, 2 * place)
                from_partner(0, 2 * place + 1)
                qkv_step(place)

    @pl.loop(0, 1)
    def _(i):
        from_partner(0, across)
        qkv_step(z)

    qkv_places(1, 2)
    line_step(0, *steps[-1])
    for j in range(2):
        send_both(1, f, j)
    qkv_places(2, line - 1)
    for j in range(3):
        cross_step(1, j)
    for o in range(2):
        for j in range(2):
            line_step(0, line - 1, o, j)
    qkv_places(line - 1, line)

    def head_rows(j, column):
        return qkv_rows[
            pl.ds(pl.multiple_of(j * seq_rows, seq_rows), seq_rows), column : column + HEAD_SIZE
        ]

    def rotate(rows):
        return (
            rows * cosine[...] + pltpu.roll(rows, HEAD_SIZE // 2, 1) * sine[...]
        ).astype(jnp.bfloat16)

    key_heads = key_cols // HEAD_SIZE
    share = heads // key_heads

    def lanes_of(at, size):
        return pl.ds(pl.multiple_of(at, HEAD_SIZE), size)

    units = ((0, big), (big, 2 * small), (pair - big, big))

    def part_copy(way, place, at, size, unit):
        cols = lanes_of(at, size)
        return pltpu.make_async_remote_copy(
            src_ref=part_out.at[place, pl.ds((1 + way) * seq_rows, seq_rows), cols],
            dst_ref=part_in.at[way, place, :, cols],
            send_sem=part_send.at[way],
            recv_sem=part_recv.at[way, place],
            device_id=team_ids[way],
        )

    def project(place, at, size, unit):
        cols = lanes_of(at, size)
        result = lax.dot_general(
            attn[...],
            out_full[lanes_of(place * pair + at, size), :],
            (((1,), (1,)), ((), ())),
            preferred_element_type=jnp.float32,
        )
        part_out[place, :, cols] = result.astype(jnp.bfloat16)
        own[place, :, cols] = result[:seq_rows]
        for way in (2, 0, 1):
            part_copy(way, place, at, size, unit).start()

    def attn_copy(j):
        rows = pl.ds(pl.multiple_of(j * seq_rows, seq_rows), seq_rows)
        return pltpu.make_async_remote_copy(
            src_ref=attn.at[rows],
            dst_ref=attn_help.at[rows],
            send_sem=attn_send.at[0],
            recv_sem=attn_recv.at[j],
            device_id=end_to_helper,
        )

    @pl.loop(0, groups)
    def _(i):
        j = groups - 1 - i
        query_place = lax.broadcasted_iota(jnp.int32, (seq_rows, seq_rows), 0)
        key_place = lax.broadcasted_iota(jnp.int32, (seq_rows, seq_rows), 1)
        allowed = (key_place <= query_place) & (key_place < len_all[j, 0:1, :])
        at = pl.ds(pl.multiple_of(j * seq_rows, seq_rows), seq_rows)
        for kh in range(key_heads):
            offset = kh * HEAD_SIZE
            group = [slice(h * HEAD_SIZE, (h + 1) * HEAD_SIZE) for h in range(share)]
            first = kh * share * HEAD_SIZE
            key = rotate(head_rows(j, query_cols + offset))
            value = head_rows(j, query_cols + key_cols + offset).astype(jnp.bfloat16)
            for lanes in group:
                queries[lanes, :] = rotate(head_rows(j, first + lanes.start))
            score_rows[...] = lax.dot_general(
                queries[...], key, (((1,), (1,)), ((), ())), preferred_element_type=jnp.float32
            )
            for lanes in group:
                scores = score_rows[lanes, :] * np.float32(1 / np.sqrt(HEAD_SIZE))
                scores = jnp.where(allowed, scores, jnp.float32(-1e30))
                expd = jnp.exp(scores - jnp.max(scores, axis=-1, keepdims=True))
                inverse = 1.0 / jnp.sum(expd, axis=-1, keepdims=True)
                queries[lanes, :] = (expd * inverse).astype(jnp.bfloat16)
            mixed = jnp.dot(queries[...], value, preferred_element_type=jnp.float32)
            for lanes in group:
                attn[at, first + lanes.start : first + lanes.stop] = mixed[lanes].astype(
                    jnp.bfloat16
                )
        pl.when(is_end)(attn_copy(j).start)

        @pl.when(i == 0)
        def _():
            from_partner(1, across, 1)

        result = lax.dot_general(
            attn[at, :],
            out_full[lanes_of(z * pair, pair), :],
            (((1,), (1,)), ((), ())),
            preferred_element_type=jnp.float32,
        )
        part_out[z, at, :] = result.astype(jnp.bfloat16)
        own[z] = result
        for way in range(3):
            pl.when(j == way + 1)(part_copy(way, z, 0, pair, 0).start)

    def project_pair(place):
        @pl.loop(0, 2)
        def _(i):
            project(place, i * (pair - big), big, 2 * i)

        project(place, big, 2 * small, 1)

    place = lax.broadcasted_iota(jnp.int32, len_tile.shape, 1)
    pick = (place == len_tile[...] - 1).astype(jnp.bfloat16)
    stats[...] = jnp.zeros_like(stats)

    def finish(place, sums):
        cols = lanes_of(place * pair, pair)
        hidden[:, cols] = (tok_own[:, cols].astype(jnp.float32) + sums).astype(jnp.bfloat16)
        last = jnp.dot(pick, hidden[:, cols], preferred_element_type=jnp.float32)
        weighted = last * final_gain[:, cols] * value_head[:, cols]
        squares = last * last
        for t in range(pair // HEAD_SIZE):
            lanes = slice(t * HEAD_SIZE, (t + 1) * HEAD_SIZE)
            stats[0] += squares[:, lanes]
            stats[1] += weighted[:, lanes]

    def finish_parts(place):
        for way in range(3):
            bytes_of(part_in.at[way, place], part_recv.at[way, place]).wait()
        total = own[place]
        for way in range(3):
            total += part_in[way, place].astype(jnp.float32)
        finish(place, total)

    def at_sides(k, body):
        @pl.loop(0, 2)
        def _(i):
            place = z + (2 * i - 1) * k

            @pl.when((place >= 0) & (place < line) & ((k > 0) | (i == 0)))
            def _():
                body(place)

    def own_unit(place):
        arrived(1, 2 * place + y, 0, 1)
        project(place, y * (pair - big), big, 2 * y)

    def mid_unit(place):
        arrived(1, 2 * place + y, 1, 1)
        arrived(1, 2 * place + 1 - y, 1, 1)
        project(place, big, 2 * small, 1)

    def cross_unit(piece):
        inner = (1 - y) * (pair - big) + y * edge
        outer = (1 - y) * (pair - edge)

        def body(place):
            arrived(1, 2 * place + 1 - y, piece, 1)
            project(place, (inner, outer)[piece - 2], piece_sizes[piece], 0)

        return body

    @pl.loop(1, line - 1)
    def _(k):
        mine = jnp.logical_not(is_helper) | (k < line - 2)
        line_step(1, k, 0, 0)
        line_step(1, k, 0, 1)

        @pl.when(mine)
        def _():
            at_sides(k, own_unit)

        @pl.when(jnp.logical_not(is_helper))
        def _():
            at_sides(k - 1, finish_parts)

        line_step(1, k, 1, 0)

        @pl.when(mine & jnp.logical_not(is_end & (k == line - 2)))
        def _():
            at_sides(k, mid_unit)

        for j in (1, 2):
            line_step(1, k, 1, j)

            @pl.when(mine)
            def _():
                at_sides(k, cross_unit(1 + j))

    def help_part(way):
        return pltpu.make_async_remote_copy(
            src_ref=help_out.at[1 + way],
            dst_ref=help_in.at[way],
            send_sem=help_send.at[0],
            recv_sem=help_recv.at[way],
            device_id=team_ids[way],
        )

    done_copy = pltpu.make_async_remote_copy(
        src_ref=help_sum,
        dst_ref=help_done,
        send_sem=done_sem.at[0],
        recv_sem=done_sem.at[1],
        device_id=helper_to_end,
    )

    @pl.when(is_helper)
    def _():
        from_partner(1, 2 * far + y, 0)
        from_partner(1, 2 * far + 1 - y, 1)

        @pl.loop(0, groups)
        def _(i):
            j = groups - 1 - i
            rows = pl.ds(pl.multiple_of(j * seq_rows, seq_rows), seq_rows)
            pltpu.make_async_copy(attn_help.at[rows], attn_help.at[rows], attn_recv.at[j]).wait()
            result = lax.dot_general(
                attn_help[rows, :],
                out_full[lanes_of(far * pair, pair), :],
                (((1,), (1,)), ((), ())),
                preferred_element_type=jnp.float32,
            )
            middle = lax.dot_general(
                attn_help[rows, :],
                out_full[lanes_of(near * pair + big, 2 * small), :],
                (((1,), (1,)), ((), ())),
                preferred_element_type=jnp.float32,
            )
            result = jnp.concatenate([result, middle], axis=1)
            help_own[...] = result
            help_out[j] = result.astype(jnp.bfloat16)
            for way in range(3):
                pl.when(j == way + 1)(help_part(way).start)

        project_pair(far)

        @pl.loop(0, line)
        def _(place):
            pl.when(place != far)(lambda: finish_parts(place))

        for way in range(3):
            help_part(way).wait_recv()
        total = help_own[...]
        for way in range(3):
            total += help_in[way].astype(jnp.float32)
        help_sum[...] = total.astype(jnp.bfloat16)
        done_copy.start()

    @pl.when(is_end)
    def _():
        for way in range(3):
            bytes_of(
                part_in.at[way, near, :, pl.ds(0, pair - 2 * small)], part_recv.at[way, near]
            ).wait()
        done_copy.wait_recv()

        def near_cols(lanes):
            total = own[near, :, lanes]
            for way in range(3):
                total += part_in[way, near, :, lanes].astype(jnp.float32)
            return total

        middle = help_done[:, pair:].astype(jnp.float32)
        finish(
            near,
            jnp.concatenate(
                [near_cols(slice(0, big)), middle, near_cols(slice(pair - big, pair))], axis=1
            ),
        )
        finish(far, help_done[:, :pair].astype(jnp.float32))

    @pl.when(is_helper)
    def _():
        finish_parts(far)

    mean = jnp.sum(stats[0], axis=-1, keepdims=True) / width
    score = jnp.sum(stats[1], axis=-1, keepdims=True) * lax.rsqrt(mean + 1e-06)
    first_row = lax.broadcasted_iota(jnp.int32, score_tile.shape, 0) == 0
    score_tile[...] = jnp.where(first_row, score, jnp.full(score_tile.shape, pair_weight[0, 0]))
    score_all[me] = score_tile[...]

    def score_copy(i):
        other = lax.rem(me + i, everyone)
        return pltpu.make_async_remote_copy(
            src_ref=score_tile,
            dst_ref=score_all.at[me],
            send_sem=score_sem.at[0],
            recv_sem=score_sem.at[1],
            device_id={"fsdp": other // groups, "dp": lax.rem(other, groups)},
        )

    @pl.loop(1, everyone)
    def _(i):
        score_copy(i).start()

    bytes_of(cross_qkv, cross_send.at[0]).wait()
    bytes_of(out_full.at[pl.ds(0, out_cols // 2)], cross_send.at[1]).wait()
    bytes_of(len_all.at[pl.ds(1, 3)], len_sem.at[0]).wait()
    for way in range(3):
        bytes_of(normed.at[pl.ds(0, seq_rows)], tok_send.at[way]).wait()
    for spot in range(line):
        ends = spot in (0, line - 1)
        up = 0 if spot == line - 1 else 2 * (spot + 1)
        down = 0 if spot == 0 else 2 * (line - spot)
        sent = (
            (UP, up, up - 2 * (spot == line - 2)),
            (DOWN, down, down - 2 * (spot == 1)),
            (PARTNER, shards - 1, shards - 1 - 2 * ends),
        )

        @pl.when(z == spot)
        def _():
            for way, slices, out_slices in sent:
                if slices:
                    rows = pl.ds(0, slices * depth // 2)
                    bytes_of(qkv_full.at[rows], send_sem.at[way, 0]).wait()
                    less = small * (spot == (line - 2, 1, spot * ends + (1 - ends) * line)[way])
                    rows = pl.ds(0, out_slices * out_cols // 2 - less)
                    bytes_of(out_full.at[rows], send_sem.at[way, 1]).wait()
            for way in range(3):
                sums = part_in.at[0]
                if ends:
                    sums = part_out.at[0, :, pl.ds(0, ((line - 1) * pair - 2 * small) // groups)]
                bytes_of(sums, part_send.at[way]).wait()
            if ends:
                bytes_of(attn, attn_send.at[0]).wait()

    @pl.when(is_helper)
    def _():
        bytes_of(help_in, help_send.at[0]).wait()
        done_copy.wait_send()

    bytes_of(score_all.at[pl.ds(0, everyone - 1)], score_sem.at[1]).wait()

    scores = score_all[:, 0, :]
    weights = score_all[:, 1, :]
    row = lax.broadcasted_iota(jnp.int32, scores.shape, 0)
    lane = lax.broadcasted_iota(jnp.int32, scores.shape, 1)
    partners = partner_rows[...]
    score_row = jnp.sum(jnp.where(row == lane, scores, 0.0), axis=0, keepdims=True)
    others = jnp.sum(jnp.where(partners == lane, score_row, 0.0), axis=1, keepdims=True)
    margins = jnp.where(row < partners, scores - others, others - scores)
    softplus = jnp.maximum(-margins, 0.0) + jnp.log1p(jnp.exp(-jnp.abs(margins)))
    first_lane = lane == 0
    margin = jnp.sum(jnp.where(first_lane & (row == me), margins, 0.0))
    loss = jnp.sum(jnp.where(first_lane, weights * softplus, 0.0)) / everyone
    results[...] = jnp.where(first_row, jnp.full(results.shape, margin), loss)
    bytes_of(score_all.at[pl.ds(0, everyone - 1)], score_sem.at[0]).wait()


def layer_fits(shards, groups, tokens, qkv_weight, out_weight):
    return (
        shards == 8
        and qkv_weight.shape[0] % 64 == 0
        and groups == 4
        and KEY_VALUE_HEADS % groups == 0
        and tokens.shape[1] == HEAD_SIZE
        and shards * groups <= HEAD_SIZE
        and out_weight.shape[1] % 64 == 0
        and out_weight.shape[1] % HEAD_SIZE == HEAD_SIZE // 2
        and out_weight.shape[1] > 2 * HEAD_SIZE
    )


def layer(
    tokens,
    lengths,
    partner,
    pair_weight,
    norm_gain,
    qkv_weight,
    qkv_bias,
    out_weight,
    final_gain,
    value_head,
):
    shards, groups = lax.axis_size("fsdp"), lax.axis_size("dp")
    _, seq_rows, width = tokens.shape
    depth = qkv_weight.shape[0]
    out_cols = out_weight.shape[1]
    query_cols = QUERY_FEATURES // groups
    key_cols = KEY_FEATURES // groups
    all_cols = query_cols + 2 * key_cols
    rows = groups * seq_rows
    line, pair = shards // 2, 2 * out_cols
    cosine, sine = rotary_tables(seq_rows)
    everyone = shards * groups
    dma = pltpu.SemaphoreType.DMA
    vmem = pl.BlockSpec(memory_space=pltpu.VMEM)
    bf16, f32 = jnp.bfloat16, jnp.float32
    hidden, results = pl.pallas_call(
        functools.partial(layer_kernel, shards, groups),
        out_shape=(
            pltpu.VMEM((seq_rows, width), bf16),
            pltpu.VMEM((8, HEAD_SIZE), f32),
        ),
        in_specs=[pl.BlockSpec(memory_space=pltpu.HBM)] * 12,
        out_specs=(vmem, vmem),
        scratch_shapes=[
            pltpu.VMEM((shards * depth, all_cols), bf16),
            pltpu.VMEM((shards * out_cols, query_cols), bf16),
            pltpu.VMEM((2, depth // 4, all_cols), bf16),
            pltpu.VMEM((3, max(out_pieces(out_cols)) // 2, query_cols), bf16),
            pltpu.VMEM((seq_rows, width), bf16),
            pltpu.VMEM((8, seq_rows), jnp.int32),
            pltpu.VMEM((groups, 8, seq_rows), jnp.int32),
            pltpu.VMEM((rows, width), bf16),
            pltpu.VMEM((rows, all_cols), f32),
            pltpu.VMEM((rows, query_cols), bf16),
            pltpu.VMEM((line, seq_rows, pair), f32),
            pltpu.VMEM((line, rows, pair), bf16),
            pltpu.VMEM((groups - 1, line, seq_rows, pair), bf16),
            pltpu.VMEM((rows, query_cols), bf16),
            pltpu.VMEM((seq_rows, pair + HEAD_SIZE), f32),
            pltpu.VMEM((groups, seq_rows, pair + HEAD_SIZE), bf16),
            pltpu.VMEM((groups - 1, seq_rows, pair + HEAD_SIZE), bf16),
            pltpu.VMEM((seq_rows, pair + HEAD_SIZE), bf16),
            pltpu.VMEM((seq_rows, pair + HEAD_SIZE), bf16),
            pltpu.VMEM((2, 8, HEAD_SIZE), f32),
            pltpu.VMEM((query_cols * HEAD_SIZE // key_cols, HEAD_SIZE), bf16),
            pltpu.VMEM((query_cols * HEAD_SIZE // key_cols, HEAD_SIZE), f32),
            pltpu.VMEM((8, HEAD_SIZE), f32),
            pltpu.VMEM((everyone, 8, HEAD_SIZE), f32),
            pltpu.VMEM((everyone, HEAD_SIZE), jnp.int32),
            pltpu.VMEM((1, width), f32),
            pltpu.VMEM((1, width + 8 * HEAD_SIZE), f32),
            pltpu.VMEM((1, width + 8 * HEAD_SIZE), f32),
            pltpu.VMEM((1, qkv_bias.shape[0] + 8 * HEAD_SIZE), f32),
            pltpu.VMEM((seq_rows, HEAD_SIZE), f32),
            pltpu.VMEM((seq_rows, HEAD_SIZE), f32),
            pltpu.SMEM((1, 1), jnp.int32),
            pltpu.SMEM((1, 1), f32),
            pltpu.SMEM((everyone,), jnp.int32),
            dma((20,)),
            dma((shards, 3)),
            dma((shards, 3, 2)),
            dma((3, 2)),
            dma((2,)),
            dma((3,)),
            dma((3, 3)),
            dma((2,)),
            dma((3,)),
            dma((3, line)),
            dma((1,)),
            dma((groups,)),
            dma((1,)),
            dma((3,)),
            dma((2,)),
            dma((2,)),
        ],
        compiler_params=pltpu.CompilerParams(
            collective_id=0, has_side_effects=True, vmem_limit_bytes=56 * 1024 * 1024
        ),
    )(
        tokens[0],
        qkv_weight,
        out_weight.T,
        lengths[None],
        pair_weight[None],
        partner,
        norm_gain,
        final_gain,
        value_head,
        qkv_bias,
        jnp.asarray(cosine),
        jnp.asarray(sine),
    )
    return hidden[None], results[0, :1], results[1, 0]


def projected_by_gathers(
    tokens,
    lengths,
    norm_gain,
    qkv_weight,
    qkv_bias,
    out_weight,
):
    sequence = tokens[0]
    length_rows = sequence.shape[0]
    width = sequence.shape[1]
    normed = rms_scale(sequence.astype(jnp.float32), norm_gain).astype(jnp.bfloat16)
    query_group_count = lax.axis_size("dp")
    group_index = lax.axis_index("dp")
    query_heads = QUERY_HEADS // query_group_count
    key_value_heads = KEY_VALUE_HEADS // query_group_count
    query_cols = query_heads * HEAD_SIZE
    key_cols = key_value_heads * HEAD_SIZE
    group_normed, group_lengths = (
        lax.all_gather(normed[None], "dp", axis=0, tiled=True),
        lax.all_gather(lengths, "dp", axis=0, tiled=True),
    )
    seq_count = group_normed.shape[0]
    flat = group_normed.reshape(seq_count * length_rows, width)
    qkv_cols = jnp.concatenate(
        [
            lax.dynamic_slice_in_dim(qkv_weight, group_index * query_cols, query_cols, 1),
            lax.dynamic_slice_in_dim(
                qkv_weight, QUERY_FEATURES + group_index * key_cols, key_cols, 1
            ),
            lax.dynamic_slice_in_dim(
                qkv_weight, QUERY_FEATURES + KEY_FEATURES + group_index * key_cols, key_cols, 1
            ),
        ],
        axis=1,
    )
    bias_cols = jnp.concatenate(
        [
            lax.dynamic_slice_in_dim(qkv_bias, group_index * query_cols, query_cols, 0),
            lax.dynamic_slice_in_dim(
                qkv_bias, QUERY_FEATURES + group_index * key_cols, key_cols, 0
            ),
            lax.dynamic_slice_in_dim(
                qkv_bias, QUERY_FEATURES + KEY_FEATURES + group_index * key_cols, key_cols, 0
            ),
        ],
        axis=0,
    )
    out_rows = lax.dynamic_slice_in_dim(out_weight, group_index * query_cols, query_cols, 0)
    qkv_full, out_full = (
        lax.all_gather(qkv_cols, "fsdp", axis=0, tiled=True),
        lax.all_gather(out_rows, "fsdp", axis=1, tiled=True),
    )
    query_key_value = jnp.dot(flat, qkv_full, preferred_element_type=jnp.float32) + bias_cols
    attn = attend(
        query_key_value.reshape(seq_count, length_rows, -1),
        group_lengths,
        query_heads,
        key_value_heads,
    )
    return lax.psum_scatter(
        jnp.dot(attn, out_full, preferred_element_type=jnp.float32),
        "dp",
        scatter_dimension=0,
        tiled=True,
    )


def per_device(
    tokens,
    lengths,
    partner,
    pair_weight,
    norm_gain,
    qkv_weight,
    qkv_bias,
    out_weight,
    final_gain,
    value_head,
):
    if layer_fits(lax.axis_size("fsdp"), lax.axis_size("dp"), tokens, qkv_weight, out_weight):
        return layer(
            tokens,
            lengths,
            partner,
            pair_weight,
            norm_gain,
            qkv_weight,
            qkv_bias,
            out_weight,
            final_gain,
            value_head,
        )
    sequence = tokens[0]
    length = lengths[0]
    projected = projected_by_gathers(tokens, lengths, norm_gain, qkv_weight, qkv_bias, out_weight)
    hidden = (sequence.astype(jnp.float32) + projected).astype(jnp.bfloat16)
    last = lax.dynamic_slice_in_dim(hidden, length - 1, 1, 0)[0].astype(jnp.float32)
    score = jnp.sum(rms_scale(last, final_gain) * value_head)
    everyone, weights_all = (
        lax.all_gather(score.reshape(1), ("fsdp", "dp"), axis=0, tiled=True),
        lax.all_gather(pair_weight, ("fsdp", "dp"), axis=0, tiled=True),
    )
    total_seqs = everyone.shape[0]
    mine = lax.axis_index(("fsdp", "dp"))
    index_all = jnp.arange(total_seqs, dtype=jnp.int32)
    my_partner = jnp.sum(jnp.where(index_all == mine, partner, 0))
    other = jnp.sum(jnp.where(index_all == my_partner, everyone, jnp.float32(0.0)))
    margin = jnp.where(mine < my_partner, score - other, other - score)
    matches = partner[:, None] == index_all[None, :]
    others_all = jnp.sum(jnp.where(matches, everyone[None, :], jnp.float32(0.0)), axis=1)
    margins_all = jnp.where(index_all < partner, everyone - others_all, others_all - everyone)
    loss = jnp.sum(weights_all * jax.nn.softplus(-margins_all)) / total_seqs
    return (hidden[None], margin.reshape(1), loss)


def solution(mesh):
    return jax.shard_map(
        per_device,
        mesh=mesh,
        in_specs=(
            P(("fsdp", "dp"), None, None),
            P(("fsdp", "dp")),
            P(),
            P(("fsdp", "dp")),
            P(),
            P("fsdp", None),
            P(),
            P(None, "fsdp"),
            P(),
            P(),
        ),
        out_specs=(P(("fsdp", "dp"), None, None), P(("fsdp", "dp")), P()),
        check_vma=False,
    )
```

```python
import functools

import jax
import jax.numpy as jnp
import numpy as np
from jax import lax
from jax.experimental import pallas as pl
from jax.experimental.pallas import tpu as pltpu
from jax.sharding import PartitionSpec as P

QUERY_HEADS = 28
KEY_VALUE_HEADS = 4
HEAD_SIZE = 128
QUERY_FEATURES = 3584
KEY_FEATURES = 512


def rms_scale(value_rows, gain):
    return (
        value_rows
        * lax.rsqrt(jnp.mean(value_rows * value_rows, axis=-1, keepdims=True) + 1e-06)
        * gain
    )


def apply_rotary(heads, length_rows):
    half = HEAD_SIZE // 2
    positions = jnp.arange(length_rows, dtype=jnp.float32)
    freqs = jnp.exp(
        -(2.0 * jnp.arange(half, dtype=jnp.float32) / HEAD_SIZE) * jnp.log(jnp.float32(1000000.0))
    )
    angles = positions[:, None] * freqs[None, :]
    cosine = jnp.cos(angles)
    sine = jnp.sin(angles)
    first = heads[..., :half]
    second = heads[..., half:]
    return jnp.concatenate(
        [first * cosine - second * sine, second * cosine + first * sine], axis=-1
    )


def attend(query_key_value, group_lengths, query_heads, key_value_heads):
    seq_count, length_rows, _ = query_key_value.shape
    query_width = query_heads * HEAD_SIZE
    key_width = key_value_heads * HEAD_SIZE
    query_rows = (
        query_key_value[..., :query_width]
        .reshape(seq_count, length_rows, query_heads, HEAD_SIZE)
        .transpose(0, 2, 1, 3)
    )
    key_rows = (
        query_key_value[..., query_width : query_width + key_width]
        .reshape(seq_count, length_rows, key_value_heads, HEAD_SIZE)
        .transpose(0, 2, 1, 3)
    )
    value_rows = (
        query_key_value[..., query_width + key_width :]
        .reshape(seq_count, length_rows, key_value_heads, HEAD_SIZE)
        .transpose(0, 2, 1, 3)
        .astype(jnp.bfloat16)
    )
    query_rows = (
        apply_rotary(query_rows, length_rows)
        .astype(jnp.bfloat16)
        .reshape(seq_count, key_value_heads, query_heads // key_value_heads, length_rows, HEAD_SIZE)
    )
    key_rows = apply_rotary(key_rows, length_rows).astype(jnp.bfloat16)
    scores = jnp.einsum(
        "bgqtd,bgsd->bgqts", query_rows, key_rows, preferred_element_type=jnp.float32
    ) / jnp.sqrt(jnp.float32(HEAD_SIZE))
    places = jnp.arange(length_rows, dtype=jnp.int32)
    causal = places[None, :] <= places[:, None]
    usable = places[None, :] < group_lengths[:, None]
    allowed = causal[None, :, :] & usable[:, None, :]
    scores = jnp.where(allowed[:, None, None, :, :], scores, jnp.float32(-1e30))
    highest = jnp.max(scores, axis=-1, keepdims=True)
    expd = jnp.exp(scores - highest)
    probs = (expd / jnp.sum(expd, axis=-1, keepdims=True)).astype(jnp.bfloat16)
    mixed = jnp.einsum("bgqts,bgsd->bgqtd", probs, value_rows, preferred_element_type=jnp.float32)
    mixed = mixed.reshape(seq_count, query_heads, length_rows, HEAD_SIZE).transpose(0, 2, 1, 3)
    return mixed.reshape(seq_count * length_rows, query_width).astype(jnp.bfloat16)


UP, DOWN, PARTNER = 0, 1, 2


def rotary_tables(length_rows):
    half = HEAD_SIZE // 2
    freqs = 1000000.0 ** (-2.0 * np.arange(half) / HEAD_SIZE)
    angles = np.arange(length_rows)[:, None] * freqs[None, :]
    cosine, sine = np.cos(angles), np.sin(angles)
    return (
        np.concatenate([cosine, cosine], axis=1).astype(np.float32),
        np.concatenate([-sine, sine], axis=1).astype(np.float32),
    )


def out_pieces(out_cols):
    small = HEAD_SIZE // 2
    return out_cols - small, small


def layer_kernel(
    shards,
    groups,
    tokens,
    qkv_weight,
    out_weight,
    length_one,
    pair_weight_one,
    partner_all,
    norm_gain_flat,
    final_gain_flat,
    value_head_flat,
    qkv_bias_flat,
    cosine_table,
    sine_table,
    hidden,
    results,
    qkv_full,
    out_full,
    cross_qkv,
    cross_out,
    tok_own,
    len_tile,
    len_all,
    normed,
    qkv_rows,
    attn,
    own,
    part_out,
    part_in,
    attn_help,
    help_own,
    help_out,
    help_in,
    help_sum,
    help_done,
    stats,
    queries,
    score_rows,
    score_tile,
    score_all,
    partner_rows,
    norm_gain,
    final_gain,
    value_head,
    qkv_bias,
    cosine,
    sine,
    length,
    pair_weight,
    partner,
    local_sem,
    qkv_recv,
    out_recv,
    send_sem,
    cross_send,
    tok_send,
    tok_recv,
    len_sem,
    part_send,
    part_recv,
    attn_send,
    attn_recv,
    help_send,
    help_recv,
    done_sem,
    score_sem,
):
    line = shards // 2
    f = lax.axis_index("fsdp")
    g = lax.axis_index("dp")
    z = f // 2
    y = f % 2
    x = g // 2
    core = g % 2
    seq_rows = tokens.shape[0]
    width = tokens.shape[1]
    depth = qkv_weight.shape[0]
    out_cols = out_weight.shape[0]
    query_cols = QUERY_FEATURES // groups
    key_cols = KEY_FEATURES // groups
    heads = query_cols // HEAD_SIZE
    quarter = depth // 4
    pair = 2 * out_cols
    big, small = out_pieces(out_cols)
    is_end = (z == 0) | (z == line - 1)
    is_helper = (z == 1) | (z == line - 2)
    far = jnp.where((z == 0) | (z == 1), line - 1, 0)
    near = jnp.where((z == 0) | (z == 1), line - 2, 1)
    end_to_helper = {"fsdp": jnp.where(z == 0, f + 2, f - 2)}
    helper_to_end = {"fsdp": jnp.where(z == 1, f - 2, f + 2)}
    has_up = z < line - 1
    has_down = z > 0
    team = 2 * x + y
    across_team = 2 * x + 1 - y
    across = 2 * z + 1 - y
    x_peer = 2 * (1 - x) + core
    team_ids = ({"dp": x_peer}, {"fsdp": across}, {"fsdp": across, "dp": x_peer})
    way_ids = ({"fsdp": f + 2}, {"fsdp": f - 2}, {"dp": 2 * x + 1 - core})

    barrier = pltpu.get_barrier_semaphore()
    for target in (*team_ids, way_ids[PARTNER]):
        pl.semaphore_signal(barrier, inc=1, device_id=target)
    for way, ok in ((UP, has_up), (DOWN, has_down)):

        @pl.when(ok)
        def _():
            pl.semaphore_signal(barrier, inc=1, device_id=way_ids[way])

    edge = HEAD_SIZE
    piece_sizes = (big, small, big - edge, edge)
    pieces = (((0, 1), (0, 1)), ((0, 1), (1, 2, 3)))

    def out_rows(side, piece, half):
        size = piece_sizes[piece] // 2
        start = (
            side * small,
            (1 - side) * big,
            (1 - side) * edge + side * small,
            side * (out_cols - edge),
        )[piece]
        return start + half * size, size

    def slot(m, s, piece, half):
        if m == 0:
            start = s * depth + (2 * piece + half) * quarter
            return qkv_full.at[pl.ds(pl.multiple_of(start, 16), quarter)]
        start, size = out_rows(lax.rem(s, 2), piece, half)
        return out_full.at[pl.ds(pl.multiple_of(s * out_cols + start, 16), size)]

    def recv_of(m, s, piece, by_partner):
        if m == 0:
            return qkv_recv.at[s, 2 if by_partner else piece]
        return out_recv.at[s, (0, 1, 0, 2)[piece], by_partner]

    count = 0

    def local(source, dest):
        nonlocal count
        copy = pltpu.make_async_copy(source, dest, local_sem.at[count])
        count += 1
        copy.start()
        return copy

    def bytes_of(ref, sem):
        return pltpu.make_async_copy(ref, ref, sem)

    def qkv_parts(piece, half, owner, dest):
        nonlocal count
        rows = pl.ds(pl.multiple_of((2 * piece + half) * quarter, 16), quarter)
        for start, size, to in (
            (owner * query_cols, query_cols, 0),
            (QUERY_FEATURES + owner * key_cols, key_cols, query_cols),
            (QUERY_FEATURES + KEY_FEATURES + owner * key_cols, key_cols, query_cols + key_cols),
        ):
            pltpu.make_async_copy(
                qkv_weight.at[rows, pl.ds(pl.multiple_of(start, 128), size)],
                dest.at[:, pl.ds(to, size)],
                local_sem.at[count],
            ).start()
        count += 1
        return bytes_of(dest, local_sem.at[count - 1])

    length_load = local(length_one, length)
    own_loads, cross_loads = [], []
    for j in range(2):
        own_loads.append(qkv_parts(j, core, team, slot(0, f, j, core)))
        cross_loads.append(qkv_parts(j, core, across_team, cross_qkv.at[j]))
    tok_local = local(tokens, tok_own)
    vectors = [
        local(flat, row.at[0, pl.ds(0, flat.shape[0])])
        for flat, row in (
            (norm_gain_flat, norm_gain),
            (final_gain_flat, final_gain),
            (value_head_flat, value_head),
            (qkv_bias_flat, qkv_bias),
        )
    ]
    late_loads = []
    for j in range(2):
        late_loads.append(qkv_parts(j, 1 - core, team, slot(0, f, j, 1 - core)))
    out_own = local(
        out_weight.at[:, pl.ds(pl.multiple_of(team * query_cols, 128), query_cols)],
        out_full.at[pl.ds(pl.multiple_of(f * out_cols, 16), out_cols)],
    )

    def cross_part(m, j):
        if m == 0:
            return cross_qkv.at[j]
        return cross_out.at[j, pl.ds(0, piece_sizes[pieces[1][1][j]] // 2)]

    out_cross = []
    for j, piece in enumerate(pieces[1][1]):
        start, size = out_rows(y, piece, core)
        out_cross.append(
            local(
                out_weight.at[
                    pl.ds(pl.multiple_of(start, 16), size),
                    pl.ds(pl.multiple_of(across_team * query_cols, 128), query_cols),
                ],
                cross_part(1, j),
            )
        )
    small_loads = [
        local(source, dest)
        for source, dest in (
            (pair_weight_one, pair_weight),
            (partner_all, partner),
            (cosine_table, cosine),
            (sine_table, sine),
        )
    ]
    everyone = shards * groups
    me = f * groups + g

    pl.semaphore_wait(barrier, 4 + has_up.astype(jnp.int32) + has_down.astype(jnp.int32))

    def way_copy(way, m, s, piece):
        return pltpu.make_async_remote_copy(
            src_ref=slot(m, s, piece, core),
            dst_ref=slot(m, s, piece, core),
            send_sem=send_sem.at[way, m],
            recv_sem=recv_of(m, s, piece, int(way == PARTNER)),
            device_id=way_ids[way],
        )

    def cross_copy(m, j):
        piece = pieces[m][1][j]
        return pltpu.make_async_remote_copy(
            src_ref=cross_part(m, j),
            dst_ref=slot(m, f, piece, core),
            send_sem=cross_send.at[m],
            recv_sem=recv_of(m, f, piece, 0),
            device_id=team_ids[1],
        )

    def arrived(m, s, piece, by_partner=0):
        bytes_of(slot(m, s, piece, core), recv_of(m, s, piece, by_partner)).wait()

    def send_both(m, s, piece):
        pl.when(has_up)(way_copy(UP, m, s, piece).start)
        pl.when(has_down)(way_copy(DOWN, m, s, piece).start)

    def cross_step(m, j):
        piece = pieces[m][1][j]
        arrived(m, across, piece)
        send_both(m, across, piece)
        way_copy(PARTNER, m, across, piece).start()

    def sides(k, o):
        row = y if o == 0 else 1 - y
        below, above = z - k, z + k
        return (
            (below >= 0, 2 * jnp.maximum(below, 0) + row, UP, has_up),
            (above < line, 2 * jnp.minimum(above, line - 1) + row, DOWN, has_down),
        )

    def line_step(m, k, o, j):
        piece = pieces[m][o][j]
        for ok, s, way, onward in sides(k, o):
            if m == 1:
                onward = onward & (k < line - 2)
            if m == 1 and piece == 1:
                spot, target = (z - line + 2, 1) if way == UP else (z - 1, line - 2)
                onward = onward & jnp.logical_not((spot == 0) & (s // 2 == target))
                ok = ok & jnp.logical_not(is_end & (k == line - 2))

            @pl.when(ok)
            def _():
                arrived(m, s, piece)
                pl.when(onward)(way_copy(way, m, s, piece).start)
                way_copy(PARTNER, m, s, piece).start()

    def from_partner(m, s, o=0):
        if m == 0:
            bytes_of(qkv_full.at[pl.ds(0, 2 * quarter)], qkv_recv.at[s, 2]).wait()
        else:
            for piece in pieces[1][o]:
                arrived(1, s, piece, 1)

    tok_starts = (0, seq_rows // 4, seq_rows * 5 // 8, seq_rows)

    def tok_copy(way, piece):
        source = 0 if way < 2 else (1, 2, 2)[piece]
        target = team_ids[way] if way < 2 else team_ids[(1, 0, 0)[piece]]
        start, size = tok_starts[piece], tok_starts[piece + 1] - tok_starts[piece]
        return pltpu.make_async_remote_copy(
            src_ref=normed.at[pl.ds(source * seq_rows + start, size)],
            dst_ref=normed.at[pl.ds((1 + way) * seq_rows + start, size)],
            send_sem=tok_send.at[0],
            recv_sem=tok_recv.at[min(3 * way + piece, 6)],
            device_id=target,
        )

    def len_copy(way):
        return pltpu.make_async_remote_copy(
            src_ref=len_tile,
            dst_ref=len_all.at[1 + way],
            send_sem=len_sem.at[0],
            recv_sem=len_sem.at[1],
            device_id=team_ids[way],
        )

    for j in range(2):
        own_loads[j].wait()
        send_both(0, f, j)
        cross_loads[j].wait()
        cross_copy(0, j).start()

    tok_local.wait()
    for copy in vectors:
        copy.wait()
    norm_rows = 16

    @pl.loop(0, seq_rows // norm_rows)
    def _(i):
        at = pl.ds(pl.multiple_of(i * norm_rows, norm_rows), norm_rows)
        rows = tok_own[at, :].astype(jnp.float32)
        scale = lax.rsqrt(jnp.mean(rows * rows, axis=-1, keepdims=True) + 1e-06)
        normed[at, :] = (rows * scale * norm_gain[...]).astype(jnp.bfloat16)

    for first, second in ((0, 1), (1, 2), (2, 0)):
        tok_copy(0, first).start()
        tok_copy(1, second).start()
    length_load.wait()
    len_tile[...] = jnp.full(len_tile.shape, length[0, 0], jnp.int32)
    len_all[0] = len_tile[...]
    for way in range(3):
        len_copy(way).start()

    bias_parts = (
        (team * query_cols, query_cols, 0),
        (QUERY_FEATURES + team * key_cols, key_cols, query_cols),
        (QUERY_FEATURES + KEY_FEATURES + team * key_cols, key_cols, query_cols + key_cols),
    )
    for start, size, to in bias_parts:
        qkv_rows[:, to : to + size] = jnp.broadcast_to(
            qkv_bias[:, pl.ds(pl.multiple_of(start, HEAD_SIZE), size)],
            (groups * seq_rows, size),
        )

    for j in range(2):
        cross_step(0, j)
        line_step(0, 1, 0, j)
    tok_copy(0, 0).wait_recv()
    tok_copy(2, 0).start()
    out_own.wait()
    for j in range(3):
        out_cross[j].wait()
        cross_copy(1, j).start()
    for j in range(2):
        line_step(0, 1, 1, j)
        tok_copy(1, 1 + j).wait_recv()
        tok_copy(2, 1 + j).start()
    steps = [(k, o, j) for k in range(2, line - 1) for o in range(2) for j in range(2)]
    for k, o, j in steps[:-1]:
        line_step(0, k, o, j)

    for way, piece in ((0, 1), (0, 2), (1, 0)):
        tok_copy(way, piece).wait_recv()
    bytes_of(normed.at[pl.ds(3 * seq_rows, seq_rows)], tok_recv.at[6]).wait()
    bytes_of(len_all.at[pl.ds(1, 3)], len_sem.at[1]).wait()
    for copy in (*late_loads, *small_loads):
        copy.wait()

    @pl.loop(0, everyone)
    def _(i):
        partner_rows[pl.ds(i, 1), :] = jnp.full((1, HEAD_SIZE), partner[i], jnp.int32)

    def qkv_step(place):
        rows = pl.ds(pl.multiple_of(place * 2 * depth, 128), 2 * depth)

        qkv_rows[...] += jnp.dot(
            normed[:, rows], qkv_full[rows, :], preferred_element_type=jnp.float32
        )

    def qkv_places(first, last):
        @pl.loop(2 * first, 2 * last)
        def _(i):
            k = i // 2
            place = z + (2 * lax.rem(i, 2) - 1) * k

            @pl.when((place >= 0) & (place < line))
            def _():
                from_partner(0, 2 * place)
                from_partner(0, 2 * place + 1)
                qkv_step(place)

    @pl.loop(0, 1)
    def _(i):
        from_partner(0, across)
        qkv_step(z)

    qkv_places(1, 2)
    line_step(0, *steps[-1])
    for j in range(2):
        send_both(1, f, j)
    qkv_places(2, line - 1)
    for j in range(3):
        cross_step(1, j)
    for o in range(2):
        for j in range(2):
            line_step(0, line - 1, o, j)
    qkv_places(line - 1, line)

    def head_rows(j, column):
        return qkv_rows[
            pl.ds(pl.multiple_of(j * seq_rows, seq_rows), seq_rows), column : column + HEAD_SIZE
        ]

    def rotate(rows):
        return (
            rows * cosine[...] + pltpu.roll(rows, HEAD_SIZE // 2, 1) * sine[...]
        ).astype(jnp.bfloat16)

    key_heads = key_cols // HEAD_SIZE
    share = heads // key_heads

    def lanes_of(at, size):
        return pl.ds(pl.multiple_of(at, HEAD_SIZE), size)

    units = ((0, big), (big, 2 * small), (pair - big, big))

    def part_copy(way, place, at, size, unit):
        cols = lanes_of(at, size)
        return pltpu.make_async_remote_copy(
            src_ref=part_out.at[place, pl.ds((1 + way) * seq_rows, seq_rows), cols],
            dst_ref=part_in.at[way, place, :, cols],
            send_sem=part_send.at[0],
            recv_sem=part_recv.at[way, place],
            device_id=team_ids[way],
        )

    def project(place, at, size, unit):
        cols = lanes_of(at, size)
        result = lax.dot_general(
            attn[...],
            out_full[lanes_of(place * pair + at, size), :],
            (((1,), (1,)), ((), ())),
            preferred_element_type=jnp.float32,
        )
        part_out[place, :, cols] = result.astype(jnp.bfloat16)
        own[place, :, cols] = result[:seq_rows]
        for way in (2, 0, 1):
            part_copy(way, place, at, size, unit).start()

    def attn_copy(j):
        rows = pl.ds(pl.multiple_of(j * seq_rows, seq_rows), seq_rows)
        return pltpu.make_async_remote_copy(
            src_ref=attn.at[rows],
            dst_ref=attn_help.at[rows],
            send_sem=attn_send.at[0],
            recv_sem=attn_recv.at[j],
            device_id=end_to_helper,
        )

    @pl.loop(0, groups)
    def _(i):
        j = groups - 1 - i
        query_place = lax.broadcasted_iota(jnp.int32, (seq_rows, seq_rows), 0)
        key_place = lax.broadcasted_iota(jnp.int32, (seq_rows, seq_rows), 1)
        allowed = (key_place <= query_place) & (key_place < len_all[j, 0:1, :])
        at = pl.ds(pl.multiple_of(j * seq_rows, seq_rows), seq_rows)
        for kh in range(key_heads):
            offset = kh * HEAD_SIZE
            group = [slice(h * HEAD_SIZE, (h + 1) * HEAD_SIZE) for h in range(share)]
            first = kh * share * HEAD_SIZE
            key = rotate(head_rows(j, query_cols + offset))
            value = head_rows(j, query_cols + key_cols + offset).astype(jnp.bfloat16)
            for lanes in group:
                queries[lanes, :] = rotate(head_rows(j, first + lanes.start))
            score_rows[...] = lax.dot_general(
                queries[...], key, (((1,), (1,)), ((), ())), preferred_element_type=jnp.float32
            )
            for lanes in group:
                scores = score_rows[lanes, :] * np.float32(1 / np.sqrt(HEAD_SIZE))
                scores = jnp.where(allowed, scores, jnp.float32(-1e30))
                expd = jnp.exp(scores - jnp.max(scores, axis=-1, keepdims=True))
                inverse = 1.0 / jnp.sum(expd, axis=-1, keepdims=True)
                queries[lanes, :] = (expd * inverse).astype(jnp.bfloat16)
            mixed = jnp.dot(queries[...], value, preferred_element_type=jnp.float32)
            for lanes in group:
                attn[at, first + lanes.start : first + lanes.stop] = mixed[lanes].astype(
                    jnp.bfloat16
                )
        pl.when(is_end)(attn_copy(j).start)

        @pl.when(i == 0)
        def _():
            from_partner(1, across, 1)

        result = lax.dot_general(
            attn[at, :],
            out_full[lanes_of(z * pair, pair), :],
            (((1,), (1,)), ((), ())),
            preferred_element_type=jnp.float32,
        )
        part_out[z, at, :] = result.astype(jnp.bfloat16)
        own[z] = result
        for way in range(3):
            pl.when(j == way + 1)(part_copy(way, z, 0, pair, 0).start)

    def project_pair(place):
        @pl.loop(0, 2)
        def _(i):
            project(place, i * (pair - big), big, 2 * i)

        project(place, big, 2 * small, 1)

    place = lax.broadcasted_iota(jnp.int32, len_tile.shape, 1)
    pick = (place == len_tile[...] - 1).astype(jnp.bfloat16)
    stats[...] = jnp.zeros_like(stats)

    def finish(place, sums):
        cols = lanes_of(place * pair, pair)
        hidden[:, cols] = (tok_own[:, cols].astype(jnp.float32) + sums).astype(jnp.bfloat16)
        last = jnp.dot(pick, hidden[:, cols], preferred_element_type=jnp.float32)
        weighted = last * final_gain[:, cols] * value_head[:, cols]
        squares = last * last
        for t in range(pair // HEAD_SIZE):
            lanes = slice(t * HEAD_SIZE, (t + 1) * HEAD_SIZE)
            stats[0] += squares[:, lanes]
            stats[1] += weighted[:, lanes]

    def finish_parts(place):
        for way in range(3):
            bytes_of(part_in.at[way, place], part_recv.at[way, place]).wait()
        total = own[place]
        for way in range(3):
            total += part_in[way, place].astype(jnp.float32)
        finish(place, total)

    def at_sides(k, body):
        @pl.loop(0, 2)
        def _(i):
            place = z + (2 * i - 1) * k

            @pl.when((place >= 0) & (place < line) & ((k > 0) | (i == 0)))
            def _():
                body(place)

    def own_unit(place):
        arrived(1, 2 * place + y, 0, 1)
        project(place, y * (pair - big), big, 2 * y)

    def mid_unit(place):
        arrived(1, 2 * place + y, 1, 1)
        arrived(1, 2 * place + 1 - y, 1, 1)
        project(place, big, 2 * small, 1)

    def cross_unit(piece):
        inner = (1 - y) * (pair - big) + y * edge
        outer = (1 - y) * (pair - edge)

        def body(place):
            arrived(1, 2 * place + 1 - y, piece, 1)
            project(place, (inner, outer)[piece - 2], piece_sizes[piece], 0)

        return body

    @pl.loop(1, line - 1)
    def _(k):
        mine = jnp.logical_not(is_helper) | (k < line - 2)
        line_step(1, k, 0, 0)
        line_step(1, k, 0, 1)

        @pl.when(mine)
        def _():
            at_sides(k, own_unit)

        @pl.when(jnp.logical_not(is_helper))
        def _():
            at_sides(k - 1, finish_parts)

        line_step(1, k, 1, 0)

        @pl.when(mine & jnp.logical_not(is_end & (k == line - 2)))
        def _():
            at_sides(k, mid_unit)

        for j in (1, 2):
            line_step(1, k, 1, j)

            @pl.when(mine)
            def _():
                at_sides(k, cross_unit(1 + j))

    def help_part(way):
        return pltpu.make_async_remote_copy(
            src_ref=help_out.at[1 + way],
            dst_ref=help_in.at[way],
            send_sem=help_send.at[0],
            recv_sem=help_recv.at[0],
            device_id=team_ids[way],
        )

    done_copy = pltpu.make_async_remote_copy(
        src_ref=help_sum,
        dst_ref=help_done,
        send_sem=done_sem.at[0],
        recv_sem=done_sem.at[1],
        device_id=helper_to_end,
    )

    @pl.when(is_helper)
    def _():
        from_partner(1, 2 * far + y, 0)
        from_partner(1, 2 * far + 1 - y, 1)

        @pl.loop(0, groups)
        def _(i):
            j = groups - 1 - i
            rows = pl.ds(pl.multiple_of(j * seq_rows, seq_rows), seq_rows)
            pltpu.make_async_copy(attn_help.at[rows], attn_help.at[rows], attn_recv.at[j]).wait()
            result = lax.dot_general(
                attn_help[rows, :],
                out_full[lanes_of(far * pair, pair), :],
                (((1,), (1,)), ((), ())),
                preferred_element_type=jnp.float32,
            )
            middle = lax.dot_general(
                attn_help[rows, :],
                out_full[lanes_of(near * pair + big, 2 * small), :],
                (((1,), (1,)), ((), ())),
                preferred_element_type=jnp.float32,
            )
            result = jnp.concatenate([result, middle], axis=1)
            help_own[...] = result
            help_out[j] = result.astype(jnp.bfloat16)
            for way in range(3):
                pl.when(j == way + 1)(help_part(way).start)

        project_pair(far)

        @pl.loop(0, line)
        def _(place):
            pl.when(place != far)(lambda: finish_parts(place))

        bytes_of(help_in, help_recv.at[0]).wait()
        total = help_own[...]
        for way in range(3):
            total += help_in[way].astype(jnp.float32)
        help_sum[...] = total.astype(jnp.bfloat16)
        done_copy.start()

    @pl.when(is_end)
    def _():
        for way in range(3):
            bytes_of(
                part_in.at[way, near, :, pl.ds(0, pair - 2 * small)], part_recv.at[way, near]
            ).wait()
        done_copy.wait_recv()

        def near_cols(lanes):
            total = own[near, :, lanes]
            for way in range(3):
                total += part_in[way, near, :, lanes].astype(jnp.float32)
            return total

        middle = help_done[:, pair:].astype(jnp.float32)
        finish(
            near,
            jnp.concatenate(
                [near_cols(slice(0, big)), middle, near_cols(slice(pair - big, pair))], axis=1
            ),
        )
        finish(far, help_done[:, :pair].astype(jnp.float32))

    @pl.when(is_helper)
    def _():
        finish_parts(far)

    mean = jnp.sum(stats[0], axis=-1, keepdims=True) / width
    score = jnp.sum(stats[1], axis=-1, keepdims=True) * lax.rsqrt(mean + 1e-06)
    first_row = lax.broadcasted_iota(jnp.int32, score_tile.shape, 0) == 0
    score_tile[...] = jnp.where(first_row, score, jnp.full(score_tile.shape, pair_weight[0, 0]))
    score_all[me] = score_tile[...]

    def score_copy(i):
        other = lax.rem(me + i, everyone)
        return pltpu.make_async_remote_copy(
            src_ref=score_tile,
            dst_ref=score_all.at[me],
            send_sem=score_sem.at[0],
            recv_sem=score_sem.at[1],
            device_id={"fsdp": other // groups, "dp": lax.rem(other, groups)},
        )

    @pl.loop(1, everyone)
    def _(i):
        score_copy(i).start()

    bytes_of(cross_qkv, cross_send.at[0]).wait()
    bytes_of(out_full.at[pl.ds(0, out_cols // 2)], cross_send.at[1]).wait()
    bytes_of(len_all.at[pl.ds(1, 3)], len_sem.at[0]).wait()
    bytes_of(normed.at[pl.ds(0, 3 * seq_rows)], tok_send.at[0]).wait()
    for spot in range(line):
        ends = spot in (0, line - 1)
        up = 0 if spot == line - 1 else 2 * (spot + 1)
        down = 0 if spot == 0 else 2 * (line - spot)
        sent = (
            (UP, up, up - 2 * (spot == line - 2)),
            (DOWN, down, down - 2 * (spot == 1)),
            (PARTNER, shards - 1, shards - 1 - 2 * ends),
        )

        @pl.when(z == spot)
        def _():
            for way, slices, out_slices in sent:
                if slices:
                    rows = pl.ds(0, slices * depth // 2)
                    bytes_of(qkv_full.at[rows], send_sem.at[way, 0]).wait()
                    less = small * (spot == (line - 2, 1, spot * ends + (1 - ends) * line)[way])
                    rows = pl.ds(0, out_slices * out_cols // 2 - less)
                    bytes_of(out_full.at[rows], send_sem.at[way, 1]).wait()
            sums = part_in
            if ends:
                cols = pl.ds(0, ((line - 1) * pair - 2 * small) // groups)
                sums = part_out.at[pl.ds(0, 3), :, cols]
            bytes_of(sums, part_send.at[0]).wait()
            if ends:
                bytes_of(attn, attn_send.at[0]).wait()

    @pl.when(is_helper)
    def _():
        bytes_of(help_in, help_send.at[0]).wait()
        done_copy.wait_send()

    bytes_of(score_all.at[pl.ds(0, everyone - 1)], score_sem.at[1]).wait()

    scores = score_all[:, 0, :]
    weights = score_all[:, 1, :]
    row = lax.broadcasted_iota(jnp.int32, scores.shape, 0)
    lane = lax.broadcasted_iota(jnp.int32, scores.shape, 1)
    partners = partner_rows[...]
    score_row = jnp.sum(jnp.where(row == lane, scores, 0.0), axis=0, keepdims=True)
    others = jnp.sum(jnp.where(partners == lane, score_row, 0.0), axis=1, keepdims=True)
    margins = jnp.where(row < partners, scores - others, others - scores)
    softplus = jnp.maximum(-margins, 0.0) + jnp.log1p(jnp.exp(-jnp.abs(margins)))
    first_lane = lane == 0
    margin = jnp.sum(jnp.where(first_lane & (row == me), margins, 0.0))
    loss = jnp.sum(jnp.where(first_lane, weights * softplus, 0.0)) / everyone
    results[...] = jnp.where(first_row, jnp.full(results.shape, margin), loss)
    bytes_of(score_all.at[pl.ds(0, everyone - 1)], score_sem.at[0]).wait()


def layer_fits(shards, groups, tokens, qkv_weight, out_weight):
    return (
        shards == 8
        and qkv_weight.shape[0] % 64 == 0
        and groups == 4
        and KEY_VALUE_HEADS % groups == 0
        and tokens.shape[1] == HEAD_SIZE
        and shards * groups <= HEAD_SIZE
        and out_weight.shape[1] % 64 == 0
        and out_weight.shape[1] % HEAD_SIZE == HEAD_SIZE // 2
        and out_weight.shape[1] > 2 * HEAD_SIZE
    )


def layer(
    tokens,
    lengths,
    partner,
    pair_weight,
    norm_gain,
    qkv_weight,
    qkv_bias,
    out_weight,
    final_gain,
    value_head,
):
    shards, groups = lax.axis_size("fsdp"), lax.axis_size("dp")
    _, seq_rows, width = tokens.shape
    depth = qkv_weight.shape[0]
    out_cols = out_weight.shape[1]
    query_cols = QUERY_FEATURES // groups
    key_cols = KEY_FEATURES // groups
    all_cols = query_cols + 2 * key_cols
    rows = groups * seq_rows
    line, pair = shards // 2, 2 * out_cols
    cosine, sine = rotary_tables(seq_rows)
    everyone = shards * groups
    dma = pltpu.SemaphoreType.DMA
    vmem = pl.BlockSpec(memory_space=pltpu.VMEM)
    bf16, f32 = jnp.bfloat16, jnp.float32
    hidden, results = pl.pallas_call(
        functools.partial(layer_kernel, shards, groups),
        out_shape=(
            pltpu.VMEM((seq_rows, width), bf16),
            pltpu.VMEM((8, HEAD_SIZE), f32),
        ),
        in_specs=[pl.BlockSpec(memory_space=pltpu.HBM)] * 12,
        out_specs=(vmem, vmem),
        scratch_shapes=[
            pltpu.VMEM((shards * depth, all_cols), bf16),
            pltpu.VMEM((shards * out_cols, query_cols), bf16),
            pltpu.VMEM((2, depth // 4, all_cols), bf16),
            pltpu.VMEM((3, max(out_pieces(out_cols)) // 2, query_cols), bf16),
            pltpu.VMEM((seq_rows, width), bf16),
            pltpu.VMEM((8, seq_rows), jnp.int32),
            pltpu.VMEM((groups, 8, seq_rows), jnp.int32),
            pltpu.VMEM((rows, width), bf16),
            pltpu.VMEM((rows, all_cols), f32),
            pltpu.VMEM((rows, query_cols), bf16),
            pltpu.VMEM((line, seq_rows, pair), f32),
            pltpu.VMEM((line, rows, pair), bf16),
            pltpu.VMEM((groups - 1, line, seq_rows, pair), bf16),
            pltpu.VMEM((rows, query_cols), bf16),
            pltpu.VMEM((seq_rows, pair + HEAD_SIZE), f32),
            pltpu.VMEM((groups, seq_rows, pair + HEAD_SIZE), bf16),
            pltpu.VMEM((groups - 1, seq_rows, pair + HEAD_SIZE), bf16),
            pltpu.VMEM((seq_rows, pair + HEAD_SIZE), bf16),
            pltpu.VMEM((seq_rows, pair + HEAD_SIZE), bf16),
            pltpu.VMEM((2, 8, HEAD_SIZE), f32),
            pltpu.VMEM((query_cols * HEAD_SIZE // key_cols, HEAD_SIZE), bf16),
            pltpu.VMEM((query_cols * HEAD_SIZE // key_cols, HEAD_SIZE), f32),
            pltpu.VMEM((8, HEAD_SIZE), f32),
            pltpu.VMEM((everyone, 8, HEAD_SIZE), f32),
            pltpu.VMEM((everyone, HEAD_SIZE), jnp.int32),
            pltpu.VMEM((1, width), f32),
            pltpu.VMEM((1, width + 8 * HEAD_SIZE), f32),
            pltpu.VMEM((1, width + 8 * HEAD_SIZE), f32),
            pltpu.VMEM((1, qkv_bias.shape[0] + 8 * HEAD_SIZE), f32),
            pltpu.VMEM((seq_rows, HEAD_SIZE), f32),
            pltpu.VMEM((seq_rows, HEAD_SIZE), f32),
            pltpu.SMEM((1, 1), jnp.int32),
            pltpu.SMEM((1, 1), f32),
            pltpu.SMEM((everyone,), jnp.int32),
            dma((20,)),
            dma((shards, 3)),
            dma((shards, 3, 2)),
            dma((3, 2)),
            dma((2,)),
            dma((1,)),
            dma((7,)),
            dma((2,)),
            dma((1,)),
            dma((3, line)),
            dma((1,)),
            dma((groups,)),
            dma((1,)),
            dma((1,)),
            dma((2,)),
            dma((2,)),
        ],
        compiler_params=pltpu.CompilerParams(
            collective_id=0, has_side_effects=True, vmem_limit_bytes=56 * 1024 * 1024
        ),
    )(
        tokens[0],
        qkv_weight,
        out_weight.T,
        lengths[None],
        pair_weight[None],
        partner,
        norm_gain,
        final_gain,
        value_head,
        qkv_bias,
        jnp.asarray(cosine),
        jnp.asarray(sine),
    )
    return hidden[None], results[0, :1], results[1, 0]


def projected_by_gathers(
    tokens,
    lengths,
    norm_gain,
    qkv_weight,
    qkv_bias,
    out_weight,
):
    sequence = tokens[0]
    length_rows = sequence.shape[0]
    width = sequence.shape[1]
    normed = rms_scale(sequence.astype(jnp.float32), norm_gain).astype(jnp.bfloat16)
    query_group_count = lax.axis_size("dp")
    group_index = lax.axis_index("dp")
    query_heads = QUERY_HEADS // query_group_count
    key_value_heads = KEY_VALUE_HEADS // query_group_count
    query_cols = query_heads * HEAD_SIZE
    key_cols = key_value_heads * HEAD_SIZE
    group_normed, group_lengths = (
        lax.all_gather(normed[None], "dp", axis=0, tiled=True),
        lax.all_gather(lengths, "dp", axis=0, tiled=True),
    )
    seq_count = group_normed.shape[0]
    flat = group_normed.reshape(seq_count * length_rows, width)
    qkv_cols = jnp.concatenate(
        [
            lax.dynamic_slice_in_dim(qkv_weight, group_index * query_cols, query_cols, 1),
            lax.dynamic_slice_in_dim(
                qkv_weight, QUERY_FEATURES + group_index * key_cols, key_cols, 1
            ),
            lax.dynamic_slice_in_dim(
                qkv_weight, QUERY_FEATURES + KEY_FEATURES + group_index * key_cols, key_cols, 1
            ),
        ],
        axis=1,
    )
    bias_cols = jnp.concatenate(
        [
            lax.dynamic_slice_in_dim(qkv_bias, group_index * query_cols, query_cols, 0),
            lax.dynamic_slice_in_dim(
                qkv_bias, QUERY_FEATURES + group_index * key_cols, key_cols, 0
            ),
            lax.dynamic_slice_in_dim(
                qkv_bias, QUERY_FEATURES + KEY_FEATURES + group_index * key_cols, key_cols, 0
            ),
        ],
        axis=0,
    )
    out_rows = lax.dynamic_slice_in_dim(out_weight, group_index * query_cols, query_cols, 0)
    qkv_full, out_full = (
        lax.all_gather(qkv_cols, "fsdp", axis=0, tiled=True),
        lax.all_gather(out_rows, "fsdp", axis=1, tiled=True),
    )
    query_key_value = jnp.dot(flat, qkv_full, preferred_element_type=jnp.float32) + bias_cols
    attn = attend(
        query_key_value.reshape(seq_count, length_rows, -1),
        group_lengths,
        query_heads,
        key_value_heads,
    )
    return lax.psum_scatter(
        jnp.dot(attn, out_full, preferred_element_type=jnp.float32),
        "dp",
        scatter_dimension=0,
        tiled=True,
    )


def per_device(
    tokens,
    lengths,
    partner,
    pair_weight,
    norm_gain,
    qkv_weight,
    qkv_bias,
    out_weight,
    final_gain,
    value_head,
):
    if layer_fits(lax.axis_size("fsdp"), lax.axis_size("dp"), tokens, qkv_weight, out_weight):
        return layer(
            tokens,
            lengths,
            partner,
            pair_weight,
            norm_gain,
            qkv_weight,
            qkv_bias,
            out_weight,
            final_gain,
            value_head,
        )
    sequence = tokens[0]
    length = lengths[0]
    projected = projected_by_gathers(tokens, lengths, norm_gain, qkv_weight, qkv_bias, out_weight)
    hidden = (sequence.astype(jnp.float32) + projected).astype(jnp.bfloat16)
    last = lax.dynamic_slice_in_dim(hidden, length - 1, 1, 0)[0].astype(jnp.float32)
    score = jnp.sum(rms_scale(last, final_gain) * value_head)
    everyone, weights_all = (
        lax.all_gather(score.reshape(1), ("fsdp", "dp"), axis=0, tiled=True),
        lax.all_gather(pair_weight, ("fsdp", "dp"), axis=0, tiled=True),
    )
    total_seqs = everyone.shape[0]
    mine = lax.axis_index(("fsdp", "dp"))
    index_all = jnp.arange(total_seqs, dtype=jnp.int32)
    my_partner = jnp.sum(jnp.where(index_all == mine, partner, 0))
    other = jnp.sum(jnp.where(index_all == my_partner, everyone, jnp.float32(0.0)))
    margin = jnp.where(mine < my_partner, score - other, other - score)
    matches = partner[:, None] == index_all[None, :]
    others_all = jnp.sum(jnp.where(matches, everyone[None, :], jnp.float32(0.0)), axis=1)
    margins_all = jnp.where(index_all < partner, everyone - others_all, others_all - everyone)
    loss = jnp.sum(weights_all * jax.nn.softplus(-margins_all)) / total_seqs
    return (hidden[None], margin.reshape(1), loss)


def solution(mesh):
    return jax.shard_map(
        per_device,
        mesh=mesh,
        in_specs=(
            P(("fsdp", "dp"), None, None),
            P(("fsdp", "dp")),
            P(),
            P(("fsdp", "dp")),
            P(),
            P("fsdp", None),
            P(),
            P(None, "fsdp"),
            P(),
            P(),
        ),
        out_specs=(P(("fsdp", "dp"), None, None), P(("fsdp", "dp")), P()),
        check_vma=False,
    )
```
